256 devices in a mesh: row: 16 (over y_hi, x, core), col: 16 (over z, y_lo).
Axes of the slice: x: 4, y: 4 (y_hi: 2, y_lo: 2; y = y_hi * 2 + y_lo), z: 8, core: 2. Of those that a mesh axis runs over, the one named last changes fastest.
Arguments:
- rho_real: float32 [8192, 8192], P('row', 'col'), may hold values from -6 to 12, as said below
- rho_imag: float32 [8192, 8192], P('row', 'col'), may hold values from -6 to 6, as said below
- gate_real_matrix: float32 [16, 16], replicated, may hold values from -1 to 1, as said below
- gate_imaginary: float32 [16, 16], replicated, may hold values from -1 to 1, as said below
- angles: float32 [8, 3], replicated, may hold values from -3.140625 to 3.140625
- targets: int32 [8], replicated, may hold values from 0 to 4
- gate_order: int32 [8], replicated, may hold values from 0 to 7, each once
Outputs:
- mixed_real: float32 [8192, 8192], P('row', 'col')
- depolarized_quadrature: float32 [8192, 8192], P('row', 'col')
- purity: float32 [], replicated
The draws below stay inside these ranges and needn't reach their ends.
Inputs may be any that keep to these rules, and one draw needn't show every extreme that they name: rho_real is symmetric: entries of order one off the diagonal, each diagonal entry raised by 2 to 6. rho_imag is antisymmetric with a zero diagonal, so that rho_real + i rho_imag is Hermitian. gate_real_matrix + i gate_imaginary is a unitary matrix. gate_real_matrix + i gate_imaginary is a unitary matrix. `targets`: each gate acts on one of the 5 low qubits. `gate_order`: each gate appears once.
All inputs are finite; a program needn't handle non-finite values.
Results may differ from the reference program's by a relative error of at most 0.0001.
Values sent between devices are 32-bit elements; how exact they have to be, the bound alone decides.
A program may use at most 64 MiB of HBM per device.

```python
import jax
import jax.numpy as jnp
from jax import lax

LQ = 5
GATE = 16
GATES = 8
DIM = 8192


def mirrored_weights(key):
    return jnp.ones((DIM,), jnp.float32)


def raw_noise(key):
    return jnp.clip(jax.random.normal(key, (DIM, DIM), jnp.float32), -6.0, 6.0)


def draw_rho_real(key, part):
    noise_key = jax.random.fold_in(key, 11)
    scale_key = jax.random.fold_in(key, 12)
    raise_key = jax.random.fold_in(key, 13)
    values = raw_noise(noise_key)
    values = 0.5 * (values + values.T)
    scales = mirrored_weights(scale_key)
    values = values * scales[:, None] * scales[None, :]
    raises = jax.random.uniform(raise_key, (DIM,), jnp.float32, 2.0, 6.0)
    on_diag = lax.broadcasted_iota(jnp.int32, (DIM, DIM), 0) == lax.broadcasted_iota(jnp.int32, (DIM, DIM), 1)
    return values + jnp.where(on_diag, raises[None, :], jnp.zeros_like(values))


def draw_rho_imag(key, part):
    noise_key = jax.random.fold_in(key, 21)
    scale_key = jax.random.fold_in(key, 22)
    values = raw_noise(noise_key)
    values = 0.5 * (values - values.T)
    scales = mirrored_weights(scale_key)
    return values * scales[:, None] * scales[None, :]


def unitary_parts(key):
    shared = jax.random.fold_in(key, 31)
    real_key = jax.random.fold_in(shared, 1)
    imag_key = jax.random.fold_in(shared, 2)
    first = jax.random.normal(real_key, (GATE, GATE), jnp.float32)
    second = jax.random.normal(imag_key, (GATE, GATE), jnp.float32)
    whole = lax.complex(first, second)
    factor_q, factor_r = jnp.linalg.qr(whole)
    diag_r = jnp.diagonal(factor_r)
    phases = diag_r / jnp.maximum(jnp.abs(diag_r), 0.001)
    unitary = factor_q * phases[None, :]
    return (jnp.real(unitary).astype(jnp.float32), jnp.imag(unitary).astype(jnp.float32))


def draw_gate_real_matrix(key, part):
    return unitary_parts(key)[0]


def draw_gate_imaginary(key, part):
    return unitary_parts(key)[1]


def place_ends(array, stream_key, low, largest):
    shape = array.shape
    spot = [jax.random.randint(jax.random.fold_in(stream_key, axis), (), 0, shape[axis]) for axis in range(len(shape))]
    array = array.at[tuple(spot)].set(low)
    longest = shape.index(max(shape))
    spot[longest] = (spot[longest] + 1) % shape[longest]
    return array.at[tuple(spot)].set(largest)


def setup_inputs(seed: int = 0) -> dict:
    splits = jax.random.split(jax.random.key(seed), 8)
    rho_real = draw_rho_real(jax.random.fold_in(splits[7], 71), 0)
    rho_imag = draw_rho_imag(jax.random.fold_in(splits[7], 71), 0)
    gate_real_matrix = draw_gate_real_matrix(jax.random.fold_in(splits[7], 71), 0)
    gate_imaginary = draw_gate_imaginary(jax.random.fold_in(splits[7], 71), 0)
    angles = jnp.clip(jax.random.uniform(splits[4], (GATES, 3), jnp.float32, -3.140625, 3.140625), -3.140625, 3.140625)
    targets = place_ends(jax.random.randint(splits[5], (GATES,), 0, LQ), jax.random.fold_in(splits[5], 1), 0, LQ - 1).astype(jnp.int32)
    gate_order = jax.random.permutation(splits[6], GATES).astype(jnp.int32)
    return dict(rho_real=rho_real, rho_imag=rho_imag, gate_real_matrix=gate_real_matrix, gate_imaginary=gate_imaginary, angles=angles, targets=targets, gate_order=gate_order)


highest = lax.Precision.HIGHEST
mixing = 0.25

def complex_blend(pattern, left_real, left_imag, right_real, right_imag):
    real_part = jnp.einsum(pattern, left_real, right_real, precision=highest) - jnp.einsum(pattern, left_imag, right_imag, precision=highest)
    imag_part = jnp.einsum(pattern, left_real, right_imag, precision=highest) + jnp.einsum(pattern, left_imag, right_real, precision=highest)
    return (real_part, imag_part)

def embed_gate(angle_row, target, low_width):
    half_turn = angle_row[0] / 2
    cosine_half = jnp.cos(half_turn)
    sine_half = jnp.sin(half_turn)
    phase_first = angle_row[1]
    phase_second = angle_row[2]
    element_count = ((cosine_half, cosine_half * 0.0), (-jnp.cos(phase_second) * sine_half, -jnp.sin(phase_second) * sine_half), (jnp.cos(phase_first) * sine_half, jnp.sin(phase_first) * sine_half), (jnp.cos(phase_first + phase_second) * cosine_half, jnp.sin(phase_first + phase_second) * cosine_half))
    left_index = lax.broadcasted_iota(jnp.int32, (low_width, low_width), 0)
    right_index = lax.broadcasted_iota(jnp.int32, (low_width, low_width), 1)
    target_bit = jnp.left_shift(jnp.ones((), jnp.int32), target.astype(jnp.int32))
    same_rest = jnp.bitwise_or(jnp.bitwise_xor(left_index, right_index), target_bit) == target_bit
    left_high = jnp.bitwise_and(left_index, target_bit) > 0
    right_high = jnp.bitwise_and(right_index, target_bit) > 0
    result = []
    for member in range(2):
        chosen = jnp.where(left_high, jnp.where(right_high, element_count[3][member], element_count[2][member]), jnp.where(right_high, element_count[1][member], element_count[0][member]))
        result.append(jnp.where(same_rest, chosen, jnp.zeros_like(chosen)))
    return (result[0], result[1])

def joined_gate(angles, targets, gate_order, low_width):
    gate_count = angles.shape[0]
    slot_ids = jnp.arange(gate_count, dtype=jnp.int32)
    total_real = jnp.eye(low_width, dtype=jnp.float32)
    total_imag = jnp.zeros((low_width, low_width), jnp.float32)
    for position in range(gate_count):
        picked = slot_ids == gate_order[position].astype(jnp.int32)
        angle_row = jnp.sum(jnp.where(picked[:, None], angles, jnp.zeros_like(angles)), axis=0)
        target = jnp.sum(jnp.where(picked, targets, jnp.zeros_like(targets))).astype(jnp.int32)
        step_real, step_imag = embed_gate(angle_row, target, low_width)
        total_real, total_imag = complex_blend('ab,bc->ac', step_real, step_imag, total_real, total_imag)
    return (total_real, total_imag)

def reference(rho_real, rho_imag, gate_real_matrix, gate_imaginary, angles, targets, gate_order):
    low_width = 2 ** LQ
    block_inphase_component, block_quadrature = joined_gate(angles, targets, gate_order, low_width)

    def row_block(segment_list):
        center_divide = complex_blend('xi,ifo->xfo', gate_real_matrix, gate_imaginary, segment_list[0], segment_list[1])
        return complex_blend('hf,ofg->ohg', block_inphase_component, block_quadrature, center_divide[0], center_divide[1])
    split_real = jnp.transpose(rho_real.reshape(GATE, GATE, low_width, DIM), (1, 0, 2, 3))
    split_imag = jnp.transpose(rho_imag.reshape(GATE, GATE, low_width, DIM), (1, 0, 2, 3))
    rows_real, rows_imag = lax.map(row_block, (split_real, split_imag))

    def col_block(segment_list):
        center_divide = complex_blend('rghl,Gg->rhGl', segment_list[0], segment_list[1], gate_real_matrix, -gate_imaginary)
        return complex_blend('rhGl,Ll->rhGL', center_divide[0], center_divide[1], block_inphase_component, -block_quadrature)
    block_rows = 512
    block_count = DIM // block_rows
    col_real, col_imag = lax.map(col_block, (rows_real.reshape(block_count, block_rows, GATE, GATE, low_width), rows_imag.reshape(block_count, block_rows, GATE, GATE, low_width)))
    col_real = col_real.reshape(DIM, DIM)
    col_imag = col_imag.reshape(DIM, DIM)
    trace_real = jnp.trace(col_real)
    trace_imag = jnp.trace(col_imag)
    diag_index = jnp.arange(DIM, dtype=jnp.int32)
    mixed_real = ((1 - mixing) * col_real).at[diag_index, diag_index].add(mixing * trace_real / DIM)
    depolarized_quadrature = ((1 - mixing) * col_imag).at[diag_index, diag_index].add(mixing * trace_imag / DIM)
    purity = (jnp.sum(mixed_real * mixed_real) + jnp.sum(depolarized_quadrature * depolarized_quadrature)) / (DIM * DIM)
    return (mixed_real, depolarized_quadrature, purity)
```

```python
import functools

import jax
import jax.numpy as jnp
from jax import lax
from jax.experimental import pallas as pl
from jax.experimental.pallas import tpu as pltpu
from jax.sharding import PartitionSpec as P

MESH = pl.DeviceIdType.MESH
HIGHEST = lax.Precision.HIGHEST
MIX = 0.25
KEEP = 1 - MIX
GATE = 16
LOW = 32
GATES = 8
BLOCK = (2, 8, 128)


def ring(v):
    v %= 8
    return min(v, 8 - v)


STEPS = [4, 3, -3, 2, -2, 1, -1, 0]
UNITS = []
for beta_ in range(8):
    found = []
    for dz_ in STEPS:
        if ring(beta_ - dz_) >= ring(dz_):
            found.append((dz_, 0))
        if ring(beta_ - dz_) > ring(dz_):
            found.append((dz_, 1))
    UNITS.append(found)
BETAS = [7, 1, 6, 2, 5, 3, 4, 0]
FORWARDS = [(*UNITS[b_][u_], b_) for u_ in range(1, 8) for b_ in BETAS if UNITS[b_][u_][0] != 0]
SLOT = {f_: i_ for i_, f_ in enumerate(FORWARDS)}


def wrap(v, n):
    return jnp.where(v >= n, v - n, v)


def near(v):
    return jnp.minimum(v, 8 - v)


def pick(index, values):
    out = jnp.int32(values[0])
    for i, value in enumerate(values):
        if value != values[0]:
            out = jnp.where(index == i, value, out)
    return out


def lanes(shape=(8, 128)):
    return lax.broadcasted_iota(jnp.int32, shape, 1)


def exchange(t):
    lane = lanes()
    low = lane < 64
    even = (lane // 32) % 2 == 0
    u = [None] * 4
    for k in range(2):
        a, b = t[k], t[k + 2]
        turned = pltpu.roll(jnp.where(low, b, a), 64, 1)
        u[k] = jnp.where(low, a, turned)
        u[k + 2] = jnp.where(low, turned, b)
    out = []
    for i in range(2):
        a, b = u[2 * i], u[2 * i + 1]
        out.append(jnp.where(even, a, pltpu.roll(b, 32, 1)))
        out.append(jnp.where(even, pltpu.roll(a, 96, 1), b))
    return out


def pack(src, dst):
    def row(h, _):
        for part in range(2):
            for q in range(4):
                tiles = [
                    src[part, pl.ds(pl.multiple_of(32 * h + 8 * k, 8), 8), pl.ds(128 * q, 128)]
                    for k in range(4)
                ]
                for i, tile in enumerate(exchange(tiles)):
                    dst[16 * h + 4 * q + i, part] = tile
        return 0

    lax.fori_loop(0, 16, row, 0)


def exchange_kernel(
    re_ref, im_ref, f_ref, sums_ref, own, turned, pd, pe, mu, md, me, part_sums, plane_sums, load_sem, s1, ru, r1, r1z, s2, r2, sa, ra, sb, rb
):
    r, c = lax.axis_index("row"), lax.axis_index("col")
    z, ylo = c // 2, c % 2
    rho, core = r // 2, r % 2
    x, y = rho % 4, (rho // 4) * 2 + ylo
    partner = r + 1 - 2 * core
    beta = wrap(rho + 8 - z, 8)
    xs = [wrap(x + jx, 4) for jx in range(4)]
    xb = [wrap(x + 4 - jx, 4) for jx in range(4)]
    cores = (core, 1 - core)

    def plane(fn, lo, inner):
        def step(jy, _):
            yy = wrap(y + jy, 4)
            top = yy >= 2
            yh = jnp.where(top, 8, 0)
            p = jnp.where(top, yy - 2, yy)
            for jx, jc in inner:
                fn(yh + xs[jx] * 2 + cores[jc], p, jy * 8 + jx * 2 + jc)
            return 0

        lax.fori_loop(lo, 4, step, 0)

    def others(fn):
        plane(fn, 0, [(jx, jc) for jx in (1, 2, 3) for jc in (0, 1)])
        plane(fn, 1, [(0, 0), (0, 1)])

    def copy(src, dst, send, recv, row, col):
        return pltpu.make_async_remote_copy(src, dst, send, recv, device_id=(row, col), device_id_type=MESH)

    barrier = pltpu.get_barrier_semaphore()

    def greet(h, p, j):
        pl.semaphore_signal(barrier, inc=1, device_id=(h, 2 * z + p), device_id_type=MESH)

    others(greet)
    greet(partner, ylo, 0)
    for k in range(1, 8):
        for h in (r, partner):
            pl.semaphore_signal(barrier, inc=1, device_id=(h, 2 * wrap(z + k, 8) + ylo), device_id_type=MESH)

    loads = [
        pltpu.make_async_copy(ref.at[pl.ds(128 * i, 128)], own.at[part, pl.ds(128 * i, 128)], load_sem.at[part, i])
        for i in range(4)
        for part, ref in ((0, re_ref), (1, im_ref))
    ]
    for load in loads:
        load.start()
    for load in loads:
        load.wait()
    pack(own, pd)

    def turn(i, _):
        rows = pl.ds(pl.multiple_of(128 * i, 128), 128)
        for j in range(4):
            there = pl.ds(128 * j, 128)
            turned[0, there, rows] = own[0, rows, there].T
            turned[1, there, rows] = -own[1, rows, there].T
        return 0

    lax.fori_loop(0, 4, turn, 0)
    pack(turned, pe)
    packed = (pd, pe)

    pl.semaphore_wait(barrier, 45)

    def at_step(dz):
        zz = wrap(z + dz % 8, 8)
        b = wrap(rho + 8 - zz, 8)
        return zz, b, near(b) >= ring(dz), near(b) > ring(dz)

    def final(kind, b, co, dz, yl):
        a = (-dz) % 8
        return f_ref.at[2 * b + co, 2 * a + yl] if kind == 0 else f_ref.at[2 * a + yl, 2 * b + co]

    first = pick(beta, [UNITS[b][0][0] % 8 for b in range(8)])
    zf = wrap(z + first, 8)
    others(lambda h, p, j: copy(pd.at[16 * h + 2 * zf + p], mu.at[j], s1, ru.at[j], h, 2 * z + p).start())
    for dz in STEPS[:-1]:
        zz, b, direct, also = at_step(dz)
        for kind, valid in ((0, direct), (1, also)):
            if kind == 1 and ring(dz) == 4:
                continue

            @pl.when(valid)
            def _():
                for h in (r, partner):
                    copy(packed[kind].at[16 * h + 2 * zz + ylo], final(kind, b, core, dz, ylo), s2, r2, h, 2 * zz + ylo).start()

    for i, dz in enumerate(STEPS):
        zz, b, direct, also = at_step(dz)
        for kind, valid in ((0, direct), (1, also)):
            if dz == 0:
                dst, sem = final(kind, b, core, 0, ylo), r1z
            else:
                if not any(f[:2] == (dz, kind) for f in FORWARDS):
                    continue
                dst = md.at[i, 2 * b + core, ylo] if kind == 0 else me.at[i, ylo, 2 * b + core]
                sem = r1.at[pick(beta, [SLOT.get((dz, kind, bb), 0) for bb in range(8)])]
                if kind == 0:
                    valid = valid & (first != dz % 8)

            @pl.when(valid)
            def _():
                def send(h, p, j):
                    copy(packed[kind].at[16 * h + 2 * zz + p], dst, s1, sem, h, 2 * z + p).start()

                others(send)
                if dz == 0:
                    send(partner, ylo, 0)
                    dst[...] = packed[kind][16 * r + 2 * zz + ylo]


    def arrived(sem, count):
        copy(pd.at[pl.ds(0, count)], pe.at[pl.ds(0, count)], sem, sem, r, c).wait_recv()

    def left(sem, count):
        copy(pd.at[pl.ds(0, count)], pe.at[pl.ds(0, count)], sem, sem, r, c).wait_send()

    def either(condition, wait, sem, counts):
        @pl.when(condition)
        def _():
            wait(sem, counts[0])

        @pl.when(jnp.logical_not(condition))
        def _():
            wait(sem, counts[1])

    acc = jnp.zeros((8, 128), jnp.float32)

    def squares(i, acc):
        for part in range(2):
            for q in range(4):
                v = own[part, pl.ds(pl.multiple_of(8 * i, 8), 8), pl.ds(128 * q, 128)]
                acc = acc + v * v
        return acc

    total = jnp.sum(lax.fori_loop(0, 64, squares, acc))
    on_diagonal = lanes((128, 128)) == lax.broadcasted_iota(jnp.int32, (128, 128), 0)
    traces = []
    for part in range(2):
        v = sum(own[part, pl.ds(128 * q, 128), pl.ds(128 * q, 128)] for q in range(4))
        traces.append(jnp.where(r == c, jnp.sum(jnp.where(on_diagonal, v, 0.0)), 0.0))
    lane = lanes((1, 128))
    place = (y * 4 + x) * 2 + core
    part_sums[place] = jnp.where(lane == 0, total, jnp.where(lane == 1, traces[0], jnp.where(lane == 2, traces[1], 0.0)))

    def share(h, p, j):
        copy(part_sums.at[place], part_sums.at[place], sa, ra, h, 2 * z + p).start()

    others(share)
    share(partner, ylo, 0)

    def pass_on(lo, inner):
        def step(jy, _):
            yy = wrap(y + 4 - jy, 4)
            top = yy >= 2
            yh = jnp.where(top, 4, 0)
            yl = jnp.where(top, yy - 2, yy)
            for jx, jc in inner:
                j = jy * 8 + jx * 2 + jc
                bs = wrap(wrap(yh + xb[jx] + 8 - z, 8), 8)
                dz = pick(bs, [UNITS[b][0][0] % 8 for b in range(8)])
                a, b = wrap(8 - dz, 8), wrap(bs + 8 - dz, 8)
                copy(pd.at[0], mu.at[j], s1, ru.at[j], r, c).wait_recv()
                copy(mu.at[j], f_ref.at[2 * b + cores[jc], 2 * a + yl], s2, r2, r, 2 * wrap(z + dz, 8) + ylo).start()
            return 0

        lax.fori_loop(lo, 4, step, 0)

    pass_on(0, [(jx, jc) for jx in (1, 2, 3) for jc in (0, 1)])
    pass_on(1, [(0, 0), (0, 1)])
    for n, (dz, kind, bb) in enumerate(FORWARDS):
        i = STEPS.index(dz)
        a, b = (-dz) % 8, (bb - dz) % 8
        mine = beta == bb

        def onward(yl, count):
            if kind == 0:
                src, dst = md.at[i, pl.ds(2 * b, 2), pl.ds(yl, count)], f_ref.at[pl.ds(2 * b, 2), pl.ds(2 * a + yl, count)]
            else:
                src, dst = me.at[i, pl.ds(yl, count), pl.ds(2 * b, 2)], f_ref.at[pl.ds(2 * a + yl, count), pl.ds(2 * b, 2)]
            copy(src, dst, s2, r2, r, 2 * wrap(z + dz % 8, 8) + ylo).start()

        @pl.when(mine)
        def _():
            arrived(r1.at[n], 2)
            onward(1 - ylo, 1)

        @pl.when(jnp.logical_not(mine))
        def _():
            arrived(r1.at[n], 4)
            onward(0, 2)

    copy(part_sums.at[pl.ds(0, 31)], part_sums.at[pl.ds(0, 31)], sa, ra, r, c).wait_recv()
    plane_sums[z] = jnp.sum(part_sums[...], axis=0)
    for k in range(1, 8):
        copy(plane_sums.at[z], plane_sums.at[z], sb, rb, r, 2 * wrap(z + k, 8) + ylo).start()

    either(beta == 0, arrived, r1z, (59, 58))
    either(beta == 0, left, s1, (241, 242))
    left(s2, 196)
    copy(plane_sums.at[pl.ds(0, 7)], plane_sums.at[pl.ds(0, 7)], sb, rb, r, c).wait()
    copy(part_sums.at[pl.ds(0, 31)], part_sums.at[pl.ds(0, 31)], sa, ra, r, c).wait_send()
    sums_ref[...] = jnp.sum(plane_sums[...], axis=0)
    arrived(r2, 196)


def exchange_call(re, im):
    f32 = jnp.float32
    dma = pltpu.SemaphoreType.DMA
    blocks = lambda *n: pltpu.VMEM(n + BLOCK, f32)
    return pl.pallas_call(
        exchange_kernel,
        name="exchange",
        out_shape=(jax.ShapeDtypeStruct((16, 16) + BLOCK, f32), jax.ShapeDtypeStruct((1, 128), f32)),
        in_specs=[pl.BlockSpec(memory_space=pl.ANY)] * 2,
        out_specs=(pl.BlockSpec(memory_space=pltpu.VMEM), pl.BlockSpec(memory_space=pltpu.VMEM)),
        scratch_shapes=[
            pltpu.VMEM((2, 512, 512), f32),
            pltpu.VMEM((2, 512, 512), f32),
            blocks(256),
            blocks(256),
            blocks(32),
            blocks(7, 16, 2),
            blocks(7, 2, 16),
            pltpu.VMEM((32, 1, 128), f32),
            pltpu.VMEM((8, 1, 128), f32),
            dma((2, 4)),
            dma,
            dma((32,)),
            dma((len(FORWARDS),)),
            dma,
            dma,
            dma,
            dma,
            dma,
            dma,
            dma,
        ],
        compiler_params=pltpu.CompilerParams(collective_id=0, has_side_effects=True, vmem_limit_bytes=40 * 2**20),
    )(re, im)


def iota2(n, m, dim):
    return lax.broadcasted_iota(jnp.int32, (n, m), dim)


def halves(v):
    hi = v.astype(jnp.bfloat16)
    return hi, (v - hi.astype(jnp.float32)).astype(jnp.bfloat16)


def dot(a, b):
    return jnp.dot(a, b, preferred_element_type=jnp.float32)


def dot3(a, b):
    return dot(a[0], b[0]) + dot(a[0], b[1]) + dot(a[1], b[0])


def local_gate(angles, targets, order):
    theta, alpha, beta = angles[:, 0:1], angles[:, 1:2], angles[:, 2:3]
    cos, sin = jnp.cos(theta / 2), jnp.sin(theta / 2)
    both = alpha + beta
    elements = (
        (cos, cos * 0.0),
        (-jnp.cos(beta) * sin, -jnp.sin(beta) * sin),
        (jnp.cos(alpha) * sin, jnp.sin(alpha) * sin),
        (jnp.cos(both) * cos, jnp.sin(both) * cos),
    )
    i, j = iota2(64, 64, 0), iota2(64, 64, 1)
    left, right = i % 32, j % 32
    same_part, lower = i // 32 == j // 32, i // 32 > j // 32
    gates = lax.broadcasted_iota(jnp.int32, (GATES, 1), 0)
    total = jnp.where(iota2(64, 32, 0) == iota2(64, 32, 1), 1.0, 0.0)
    for position in range(GATES):
        gate = order[position]
        bit = jnp.left_shift(jnp.int32(1), targets[gate])
        entry = [
            [jnp.sum(jnp.where(gates == gate, e, 0.0), axis=0, keepdims=True) for e in pair] for pair in elements
        ]
        left_high, right_high = (left & bit) > 0, (right & bit) > 0
        same_rest = ((left ^ right) | bit) == bit
        step = [
            jnp.where(
                same_rest,
                jnp.where(
                    left_high,
                    jnp.where(right_high, entry[3][part], entry[2][part]),
                    jnp.where(right_high, entry[1][part], entry[0][part]),
                ),
                0.0,
            )
            for part in range(2)
        ]
        step = jnp.where(same_part, step[0], jnp.where(lower, step[1], -step[1]))
        total = jnp.dot(step, total, precision=HIGHEST, preferred_element_type=jnp.float32)
    return total


def spread(rows, small, cols):
    out = []
    for half in halves(small):
        wide = dot(rows, half).astype(jnp.bfloat16)
        out.append(lax.dot_general(wide, cols, (((1,), (1,)), ((), ())), preferred_element_type=jnp.float32))
    return out


def embed(re, im, part_i, part_j, keep, sign):
    same, lower = part_i == part_j, part_i > part_j
    out = []
    for a, b in zip(re, im):
        b = jnp.where(lower, b, -b) * sign
        out.append(jnp.where(keep, jnp.where(same, a, b), 0.0).astype(jnp.bfloat16))
    return out


def one_hot(n, m, index):
    return jnp.where(index == iota2(n, m, 1), 1.0, 0.0).astype(jnp.bfloat16)


def rotate_kernel(f_ref, sums_ref, ure_ref, uim_ref, angles_ref, targets_ref, order_ref, re_ref, im_ref, purity_ref, f1, f2, nat):
    r, c = lax.axis_index("row"), lax.axis_index("col")
    z = c // 2
    i, j = iota2(256, 256, 0), iota2(256, 256, 1)
    out_g = one_hot(256, 16, iota2(256, 16, 0) // 16)
    in_g = one_hot(256, 16, (iota2(256, 16, 0) // 16 + 2 * z) % 16)
    u_re, u_im = (spread(out_g, ref[...], in_g) for ref in (ure_ref, uim_ref))
    part_i, part_j, keep = (i // 8) % 2, (j // 8) % 2, i % 8 == j % 8
    u_left = embed(u_re, u_im, part_i, part_j, keep, 1.0)
    u_right = embed(u_re, u_im, part_i, part_j, keep, -1.0)
    gate = local_gate(angles_ref[...], targets_ref, order_ref)
    low = one_hot(256, 32, iota2(256, 32, 0) % 32)
    g_re, g_im = (spread(low, gate[32 * part : 32 * part + 32], low) for part in range(2))
    part_i, part_j, keep = i // 128, j // 128, (i // 32) % 4 == (j // 32) % 4
    g_left = embed(g_re, g_im, part_i, part_j, keep, 1.0)
    gt_re, gt_im = ([m.T for m in pair] for pair in (g_re, g_im))
    g_right = embed(gt_re, gt_im, part_i, part_j, keep, 1.0)

    def first(g, _):
        v = jnp.concatenate([f_ref[g, :, part].reshape(128, 128) for part in range(2)], axis=1)
        v = dot3(halves(v), g_right)
        for part in range(2):
            f1[g, :, part] = v[:, 128 * part : 128 * part + 128].reshape(16, 8, 128)
        return 0

    lax.fori_loop(0, 16, first, 0)

    def second(n, _):
        v = jnp.concatenate([f1[2 * n + k].reshape(256, 128) for k in range(2)], axis=1)
        v = dot3(u_right, halves(v))
        for k in range(2):
            f2[2 * n + k] = v[:, 128 * k : 128 * k + 128].reshape((16,) + BLOCK)
        return 0

    lax.fori_loop(0, 8, second, 0)

    def third(n, _):
        v = jnp.concatenate([f2[:, 2 * n + k].reshape(256, 128) for k in range(2)], axis=1)
        v = dot3(u_left, halves(v))
        for k in range(2):
            f1[:, 2 * n + k] = v[:, 128 * k : 128 * k + 128].reshape((16,) + BLOCK)
        return 0

    lax.fori_loop(0, 8, third, 0)

    def fourth(g, _):
        for part in range(2):
            for q in range(4):
                for k, tile in enumerate(exchange([f1[g, 4 * q + n, part] for n in range(4)])):
                    nat[part, pl.ds(pl.multiple_of(32 * g + 8 * k, 8), 8), pl.ds(128 * q, 128)] = tile
        return 0

    lax.fori_loop(0, 16, fourth, 0)

    sums = sums_ref[...]
    lane = lanes((1, 128))
    total, trace_re, trace_im = (jnp.sum(jnp.where(lane == n, sums, 0.0)) for n in range(3))
    dim = GATE * GATE * LOW
    shifts = (jnp.where(r == c, MIX * trace_re / dim, 0.0), jnp.where(r == c, MIX * trace_im / dim, 0.0))

    def fifth(n, _):
        rows = pl.ds(pl.multiple_of(128 * n, 128), 128)
        v = jnp.concatenate([nat[part, rows, :] for part in range(2)], axis=0)
        v = dot3(g_left, halves(v))
        diagonal = lax.broadcasted_iota(jnp.int32, (128, 512), 0) + 128 * n == lanes((128, 512))
        for part, ref in ((0, re_ref), (1, im_ref)):
            ref[rows, :] = KEEP * v[128 * part : 128 * part + 128] + jnp.where(diagonal, shifts[part], 0.0)
        return 0

    lax.fori_loop(0, 4, fifth, 0)
    squared = trace_re * trace_re + trace_im * trace_im
    purity_ref[0, 0] = (KEEP * KEEP * total + (2 * KEEP * MIX + MIX * MIX) * squared / dim) / (dim * dim)


def rotate_call(f, sums, u_re, u_im, angles, targets, order):
    f32 = jnp.float32
    vmem, smem = pl.BlockSpec(memory_space=pltpu.VMEM), pl.BlockSpec(memory_space=pltpu.SMEM)
    return pl.pallas_call(
        rotate_kernel,
        name="rotate",
        out_shape=(
            jax.ShapeDtypeStruct((512, 512), f32),
            jax.ShapeDtypeStruct((512, 512), f32),
            jax.ShapeDtypeStruct((1, 1), f32),
        ),
        in_specs=[vmem, vmem, vmem, vmem, vmem, smem, smem],
        out_specs=(vmem, vmem, smem),
        scratch_shapes=[
            pltpu.VMEM((16, 16) + BLOCK, f32),
            pltpu.VMEM((16, 16) + BLOCK, f32),
            pltpu.VMEM((2, 512, 512), f32),
        ],
        compiler_params=pltpu.CompilerParams(vmem_limit_bytes=40 * 2**20),
    )(f, sums, u_re, u_im, angles, targets, order)


def on_device(rho_real, rho_imag, gate_real_matrix, gate_imaginary, angles, targets, gate_order):
    f, sums = exchange_call(rho_real, rho_imag)
    re, im, purity = rotate_call(f, sums, gate_real_matrix, gate_imaginary, angles, targets, gate_order)
    return re, im, purity.reshape(())


def solution(mesh):
    return jax.shard_map(
        on_device,
        mesh=mesh,
        in_specs=(P("row", "col"), P("row", "col"), P(), P(), P(), P(), P()),
        out_specs=(P("row", "col"), P("row", "col"), P()),
        check_vma=False,
    )
```

```python
import functools

import jax
import jax.numpy as jnp
from jax import lax
from jax.experimental import pallas as pl
from jax.experimental.pallas import tpu as pltpu
from jax.sharding import PartitionSpec as P

MESH = pl.DeviceIdType.MESH
HIGHEST = lax.Precision.HIGHEST
MIX = 0.25
KEEP = 1 - MIX
GATE = 16
LOW = 32
GATES = 8
BLOCK = (2, 8, 128)


def ring(v):
    v %= 8
    return min(v, 8 - v)


STEPS = [4, 3, -3, 2, -2, 1, -1, 0]
UNITS = []
for beta_ in range(8):
    found = []
    for dz_ in STEPS:
        if ring(beta_ - dz_) >= ring(dz_):
            found.append((dz_, 0))
        if ring(beta_ - dz_) > ring(dz_):
            found.append((dz_, 1))
    UNITS.append(found)
BETAS = [7, 1, 6, 2, 5, 3, 4, 0]
FORWARDS = [(*UNITS[b_][u_], b_) for u_ in range(1, 8) for b_ in BETAS if UNITS[b_][u_][0] != 0]
GROUP = {dz_: int(ring(dz_) == 1) for dz_ in STEPS}
SLOT = {f_: i_ for i_, f_ in enumerate(FORWARDS)}


def wrap(v, n):
    return jnp.where(v >= n, v - n, v)


def near(v):
    return jnp.minimum(v, 8 - v)


def pick(index, values):
    out = jnp.int32(values[0])
    for i, value in enumerate(values):
        if value != values[0]:
            out = jnp.where(index == i, value, out)
    return out


def lanes(shape=(8, 128)):
    return lax.broadcasted_iota(jnp.int32, shape, 1)


def exchange(t):
    lane = lanes()
    low = lane < 64
    even = (lane // 32) % 2 == 0
    u = [None] * 4
    for k in range(2):
        a, b = t[k], t[k + 2]
        turned = pltpu.roll(jnp.where(low, b, a), 64, 1)
        u[k] = jnp.where(low, a, turned)
        u[k + 2] = jnp.where(low, turned, b)
    out = []
    for i in range(2):
        a, b = u[2 * i], u[2 * i + 1]
        out.append(jnp.where(even, a, pltpu.roll(b, 32, 1)))
        out.append(jnp.where(even, pltpu.roll(a, 96, 1), b))
    return out


def pack(src, dst, i):
    for n in range(4):
        h = 4 * i + n
        for part in range(2):
            for q in range(4):
                tiles = [
                    src[part, pl.ds(pl.multiple_of(32 * h + 8 * k, 8), 8), pl.ds(128 * q, 128)]
                    for k in range(4)
                ]
                for m, tile in enumerate(exchange(tiles)):
                    dst[16 * h + 4 * q + m, part] = tile


def exchange_kernel(
    re_hbm, im_hbm, ure_hbm, uim_hbm, angles_hbm, targets_hbm, order_hbm, out_ref, left_ref, sums_ref,
    own, turned, pd, pe, mu, md, me, f_ref, part_sums, plane_sums, small, angles, targets, order, right1, right2,
    load_sem, small_sem, s1, ru, r1, r1z, s2, r2, sa, ra, sb, rb,
):
    r, c = lax.axis_index("row"), lax.axis_index("col")
    z, ylo = c // 2, c % 2
    rho, core = r // 2, r % 2
    x, y = rho % 4, (rho // 4) * 2 + ylo
    partner = r + 1 - 2 * core
    beta = wrap(rho + 8 - z, 8)
    xs = [wrap(x + jx, 4) for jx in range(4)]
    xb = [wrap(x + 4 - jx, 4) for jx in range(4)]
    cores = (core, 1 - core)

    def plane(fn, lo, inner):
        def step(jy, _):
            yy = wrap(y + jy, 4)
            top = yy >= 2
            yh = jnp.where(top, 8, 0)
            p = jnp.where(top, yy - 2, yy)
            for jx, jc in inner:
                fn(yh + xs[jx] * 2 + cores[jc], p, jy * 8 + jx * 2 + jc)
            return 0

        lax.fori_loop(lo, 4, step, 0)

    def others(fn):
        plane(fn, 0, [(jx, jc) for jx in (1, 2, 3) for jc in (0, 1)])
        plane(fn, 1, [(0, 0), (0, 1)])

    def copy(src, dst, send, recv, row, col):
        return pltpu.make_async_remote_copy(src, dst, send, recv, device_id=(row, col), device_id_type=MESH)

    loads = [
        [
            pltpu.make_async_copy(ref.at[pl.ds(128 * i, 128)], own.at[part, pl.ds(128 * i, 128)], load_sem.at[part, i])
            for part, ref in ((0, re_hbm), (1, im_hbm))
        ]
        for i in range(4)
    ]
    for pair in loads:
        for load in pair:
            load.start()
    barrier = pltpu.get_barrier_semaphore()

    def greet(h, p, j):
        pl.semaphore_signal(barrier, inc=1, device_id=(h, 2 * z + p), device_id_type=MESH)

    others(greet)
    greet(partner, ylo, 0)
    for k in range(1, 8):
        for h in (r, partner):
            pl.semaphore_signal(barrier, inc=1, device_id=(h, 2 * wrap(z + k, 8) + ylo), device_id_type=MESH)
    smalls = [
        pltpu.make_async_copy(ref, dst, small_sem.at[i])
        for i, (ref, dst) in enumerate(
            (
                (ure_hbm, small.at[0]),
                (uim_hbm, small.at[1]),
                (angles_hbm, angles),
                (targets_hbm, targets),
                (order_hbm, order),
            )
        )
    ]
    for load in smalls:
        load.start()
    for i, pair in enumerate(loads):
        for load in pair:
            load.wait()
        pack(own, pd, i)
    packed = (pd, pe)
    pl.semaphore_wait(barrier, 45)

    def at_step(dz):
        zz = wrap(z + dz % 8, 8)
        b = wrap(rho + 8 - zz, 8)
        return zz, b, near(b) >= ring(dz), near(b) > ring(dz)

    def final(kind, b, co, dz, yl):
        a = (-dz) % 8
        return f_ref.at[2 * b + co, 2 * a + yl] if kind == 0 else f_ref.at[2 * a + yl, 2 * b + co]

    first = pick(beta, [UNITS[b][0][0] % 8 for b in range(8)])
    zf = wrap(z + first, 8)
    others(lambda h, p, j: copy(pd.at[16 * h + 2 * zf + p], mu.at[j], s1, ru.at[j], h, 2 * z + p).start())
    def straight(kind):
        for dz in STEPS[:-1]:
            zz, b, direct, also = at_step(dz)
            if kind == 1 and ring(dz) == 4:
                continue

            @pl.when(also if kind else direct)
            def _():
                for h in (r, partner):
                    copy(
                        packed[kind].at[16 * h + 2 * zz + ylo],
                        final(kind, b, core, dz, ylo),
                        s2,
                        r2.at[GROUP[dz]],
                        h,
                        2 * zz + ylo,
                    ).start()

    def send_units(steps):
        for dz in steps:
            i = STEPS.index(dz)
            zz, b, direct, also = at_step(dz)
            for kind, valid in ((0, direct), (1, also)):
                if dz == 0:
                    dst, sem = final(kind, b, core, 0, ylo), r1z
                else:
                    if not any(f[:2] == (dz, kind) for f in FORWARDS):
                        continue
                    dst = md.at[i, 2 * b + core, ylo] if kind == 0 else me.at[i, ylo, 2 * b + core]
                    sem = r1.at[pick(beta, [SLOT.get((dz, kind, bb), 0) for bb in range(8)])]
                    if kind == 0:
                        valid = valid & (first != dz % 8)

                @pl.when(valid)
                def _():
                    def send(h, p, j):
                        copy(packed[kind].at[16 * h + 2 * zz + p], dst, s1, sem, h, 2 * z + p).start()

                    others(send)
                    if dz == 0:
                        send(partner, ylo, 0)
                        dst[...] = packed[kind][16 * r + 2 * zz + ylo]

    straight(0)
    for i in range(4):
        rows = pl.ds(128 * i, 128)
        for j in range(4):
            there = pl.ds(128 * j, 128)
            turned[0, there, rows] = own[0, rows, there].T
            turned[1, there, rows] = -own[1, rows, there].T

    for i in range(4):
        pack(turned, pe, i)
    straight(1)
    send_units(STEPS[:5])

    def arrived(sem, count):
        copy(pd.at[pl.ds(0, count)], pe.at[pl.ds(0, count)], sem, sem, r, c).wait_recv()

    def left(sem, count):
        copy(pd.at[pl.ds(0, count)], pe.at[pl.ds(0, count)], sem, sem, r, c).wait_send()

    def either(condition, wait, sem, counts):
        @pl.when(condition)
        def _():
            wait(sem, counts[0])

        @pl.when(jnp.logical_not(condition))
        def _():
            wait(sem, counts[1])

    def pass_on(lo, inner):
        def step(jy, _):
            yy = wrap(y + 4 - jy, 4)
            top = yy >= 2
            yh = jnp.where(top, 4, 0)
            yl = jnp.where(top, yy - 2, yy)
            for jx, jc in inner:
                j = jy * 8 + jx * 2 + jc
                bs = wrap(wrap(yh + xb[jx] + 8 - z, 8), 8)
                dz = pick(bs, [UNITS[b][0][0] % 8 for b in range(8)])
                a, b = wrap(8 - dz, 8), wrap(bs + 8 - dz, 8)
                copy(pd.at[0], mu.at[j], s1, ru.at[j], r, c).wait_recv()
                copy(mu.at[j], f_ref.at[2 * b + cores[jc], 2 * a + yl], s2, r2.at[0], r, 2 * wrap(z + dz, 8) + ylo).start()
            return 0

        lax.fori_loop(lo, 4, step, 0)

    pass_on(0, [(jx, jc) for jx in (1, 2, 3) for jc in (0, 1)])
    pass_on(1, [(0, 0), (0, 1)])
    send_units(STEPS[5:])

    acc = jnp.zeros((8, 128), jnp.float32)

    def squares(i, acc):
        for part in range(2):
            for q in range(4):
                v = own[part, pl.ds(pl.multiple_of(8 * i, 8), 8), pl.ds(128 * q, 128)]
                acc = acc + v * v
        return acc

    total = jnp.sum(lax.fori_loop(0, 64, squares, acc))
    on_diagonal = lanes((128, 128)) == lax.broadcasted_iota(jnp.int32, (128, 128), 0)
    traces = []
    for part in range(2):
        v = sum(own[part, pl.ds(128 * q, 128), pl.ds(128 * q, 128)] for q in range(4))
        traces.append(jnp.where(r == c, jnp.sum(jnp.where(on_diagonal, v, 0.0)), 0.0))
    lane = lanes((1, 128))
    place = (y * 4 + x) * 2 + core
    part_sums[place] = jnp.where(lane == 0, total, jnp.where(lane == 1, traces[0], jnp.where(lane == 2, traces[1], 0.0)))

    def share(h, p, j):
        copy(part_sums.at[place], part_sums.at[place], sa, ra, h, 2 * z + p).start()

    others(share)
    share(partner, ylo, 0)

    for n, (dz, kind, bb) in enumerate(FORWARDS):
        i = STEPS.index(dz)
        a, b = (-dz) % 8, (bb - dz) % 8
        mine = beta == bb

        def onward(yl, count):
            if kind == 0:
                src, dst = md.at[i, pl.ds(2 * b, 2), pl.ds(yl, count)], f_ref.at[pl.ds(2 * b, 2), pl.ds(2 * a + yl, count)]
            else:
                src, dst = me.at[i, pl.ds(yl, count), pl.ds(2 * b, 2)], f_ref.at[pl.ds(2 * a + yl, count), pl.ds(2 * b, 2)]
            copy(src, dst, s2, r2.at[GROUP[dz]], r, 2 * wrap(z + dz % 8, 8) + ylo).start()

        @pl.when(mine)
        def _():
            arrived(r1.at[n], 2)
            onward(1 - ylo, 1)

        @pl.when(jnp.logical_not(mine))
        def _():
            arrived(r1.at[n], 4)
            onward(0, 2)

    copy(part_sums.at[pl.ds(0, 31)], part_sums.at[pl.ds(0, 31)], sa, ra, r, c).wait_recv()
    plane_sums[z] = jnp.sum(part_sums[...], axis=0)
    for k in range(1, 8):
        copy(plane_sums.at[z], plane_sums.at[z], sb, rb, r, 2 * wrap(z + k, 8) + ylo).start()

    for load in smalls:
        load.wait()
    prepare(z, small, angles, targets, order, right1, right2, left_ref)
    either(beta == 0, arrived, r1z, (59, 58))
    on_lanes(f_ref, right1, 0, 2, 0, 16)
    on_lanes(f_ref, right1, 2, 14, 0, 2)
    arrived(r2.at[0], 100)
    for n in range(5):
        on_lanes(f_ref, right1, 4 + 2 * n, 2, 4, 10)
    either(beta == 0, left, s1, (241, 242))
    left(s2, 196)
    copy(plane_sums.at[pl.ds(0, 7)], plane_sums.at[pl.ds(0, 7)], sb, rb, r, c).wait()
    copy(part_sums.at[pl.ds(0, 31)], part_sums.at[pl.ds(0, 31)], sa, ra, r, c).wait_send()
    sums_ref[...] = jnp.sum(plane_sums[...], axis=0)
    arrived(r2.at[1], 96)
    on_lanes(f_ref, right1, 2, 2, 2, 14)
    on_lanes(f_ref, right1, 14, 2, 2, 14)
    on_lanes(f_ref, right1, 4, 10, 2, 2)
    on_lanes(f_ref, right1, 4, 10, 14, 2)
    matrix = (right2[0], right2[1])
    for n in range(8):
        v = jnp.concatenate([f_ref[2 * n + k].reshape(256, 128) for k in range(2)], axis=1)
        v = dot3(matrix, halves(v))
        for k in range(2):
            out_ref[2 * n + k] = v[:, 128 * k : 128 * k + 128].reshape((16,) + BLOCK)


def exchange_call(*args):
    f32, bf16 = jnp.float32, jnp.bfloat16
    dma = pltpu.SemaphoreType.DMA
    vmem, hbm = pl.BlockSpec(memory_space=pltpu.VMEM), pl.BlockSpec(memory_space=pltpu.HBM)
    blocks = lambda *n: pltpu.VMEM(n + BLOCK, f32)
    return pl.pallas_call(
        exchange_kernel,
        name="exchange",
        out_shape=(
            jax.ShapeDtypeStruct((16, 16) + BLOCK, f32),
            jax.ShapeDtypeStruct((2, 256, 256), bf16),
            jax.ShapeDtypeStruct((1, 128), f32),
        ),
        in_specs=[hbm] * 7,
        out_specs=(vmem, vmem, vmem),
        scratch_shapes=[
            pltpu.VMEM((2, 512, 512), f32),
            pltpu.VMEM((2, 512, 512), f32),
            blocks(256),
            blocks(256),
            blocks(32),
            blocks(7, 16, 2),
            blocks(7, 2, 16),
            blocks(16, 16),
            pltpu.VMEM((32, 1, 128), f32),
            pltpu.VMEM((8, 1, 128), f32),
            pltpu.VMEM((2, 16, 16), f32),
            pltpu.VMEM((3, 8), f32),
            pltpu.SMEM((8,), jnp.int32),
            pltpu.SMEM((8,), jnp.int32),
            pltpu.VMEM((2, 256, 256), bf16),
            pltpu.VMEM((2, 256, 256), bf16),
            dma((2, 4)),
            dma((5,)),
            dma,
            dma((32,)),
            dma((len(FORWARDS),)),
            dma,
            dma,
            dma((2,)),
            dma,
            dma,
            dma,
            dma,
        ],
        compiler_params=pltpu.CompilerParams(collective_id=0, has_side_effects=True, vmem_limit_bytes=40 * 2**20),
    )(*args)


def iota2(n, m, dim):
    return lax.broadcasted_iota(jnp.int32, (n, m), dim)


def halves(v):
    hi = v.astype(jnp.bfloat16)
    return hi, (v - hi.astype(jnp.float32)).astype(jnp.bfloat16)


def dot(a, b):
    return jnp.dot(a, b, preferred_element_type=jnp.float32)


def dot3(a, b):
    return dot(a[0], b[0]) + dot(a[0], b[1]) + dot(a[1], b[0])


def gate_factors(angles, targets, order):
    theta, alpha, beta = angles[0:1], angles[1:2], angles[2:3]
    cos, sin = jnp.cos(theta / 2), jnp.sin(theta / 2)
    both = alpha + beta
    elements = (
        (cos, cos * 0.0),
        (-jnp.cos(beta) * sin, -jnp.sin(beta) * sin),
        (jnp.cos(alpha) * sin, jnp.sin(alpha) * sin),
        (jnp.cos(both) * cos, jnp.sin(both) * cos),
    )
    i, j = iota2(32, 32, 0), iota2(32, 32, 1)
    left, right, high = i % 8, j % 8, i >= 16
    same_part, lower, same_factor = (i // 8) % 2 == (j // 8) % 2, i > j, i // 16 == j // 16
    gates = lax.broadcasted_iota(jnp.int32, (1, GATES), 1)
    total = jnp.where((iota2(32, 8, 0) % 16) == iota2(32, 8, 1), 1.0, 0.0)
    for position in range(GATES):
        gate = order[position]
        target = targets[gate]
        low_bit = jnp.where(target == 0, 1, jnp.where(target == 1, 2, jnp.where(target == 2, 4, 0)))
        high_bit = jnp.where(target == 3, 1, jnp.where(target == 4, 2, 0))
        bit = jnp.where(high, high_bit, low_bit)
        entry = [
            [jnp.sum(jnp.where(gates == gate, e, 0.0), axis=1, keepdims=True) for e in pair] for pair in elements
        ]
        left_high, right_high = (left & bit) > 0, (right & bit) > 0
        same_rest = ((left ^ right) | bit) == bit
        step = [
            jnp.where(
                left_high,
                jnp.where(right_high, entry[3][part], entry[2][part]),
                jnp.where(right_high, entry[1][part], entry[0][part]),
            )
            for part in range(2)
        ]
        step = [jnp.where(bit > 0, v, one) for v, one in zip(step, (1.0, 0.0))]
        step = jnp.where(same_part, step[0], jnp.where(lower, step[1], -step[1]))
        step = jnp.where(same_rest & same_factor, step, 0.0)
        total = jnp.dot(step, total, precision=HIGHEST, preferred_element_type=jnp.float32)
    return total


def one_hot(n, m, index):
    return jnp.where(index == iota2(n, m, 1), 1.0, 0.0)


def spread(rows, small, cols):
    wide = jnp.dot(rows, small, precision=HIGHEST, preferred_element_type=jnp.float32)
    return lax.dot_general(wide, cols, (((1,), (1,)), ((), ())), precision=HIGHEST, preferred_element_type=jnp.float32)


def times(a, b):
    return a[0] * b[0] - a[1] * b[1], a[0] * b[1] + a[1] * b[0]


def store_halves(ref, v):
    hi, lo = halves(v)
    ref[0] = hi
    ref[1] = lo


def prepare(z, small, angles, targets, order, right1, right2, left_ref):
    i, j = iota2(256, 256, 0), iota2(256, 256, 1)
    row = lambda n: iota2(256, n, 0)
    factors = gate_factors(angles[...], targets, order)
    low, high = ([factors[16 * w + 8 * part : 16 * w + 8 * part + 8] for part in range(2)] for w in range(2))
    out_g = one_hot(256, 16, row(16) // 16)
    in_g = one_hot(256, 16, (row(16) // 16 + 2 * z) % 16)
    u = [spread(out_g, small[part], in_g) for part in range(2)]
    same, lower = (i // 8) % 2 == (j // 8) % 2, (i // 8) % 2 > (j // 8) % 2
    value = jnp.where(same, u[0], jnp.where(lower, -u[1], u[1]))
    store_halves(right2, jnp.where(i % 8 == j % 8, value, 0.0))
    on_s = one_hot(256, 8, row(8) % 8)
    value = times(u, [spread(on_s, m, on_s) for m in low])
    store_halves(left_ref, jnp.where(same, value[0], jnp.where(lower, value[1], -value[1])))
    on_k = one_hot(256, 8, (row(8) // 32) % 4)
    on_top = one_hot(256, 8, (row(8) // 8) % 4)
    turn = lambda hot, m: spread(hot, m.T, hot)
    a = [turn(on_k, m) for m in high]
    b = times([turn(on_top, m) for m in high], [turn(on_s, m) for m in low])
    value = times(a, (b[0], -b[1]))
    same, lower = i // 128 == j // 128, i > j
    store_halves(right1, jnp.where(same, value[0], jnp.where(lower, -value[1], value[1])))


def on_lanes(f_ref, right1, g, n, g2, n2):
    here = (pl.ds(g, n), pl.ds(g2, n2))
    v = jnp.concatenate([f_ref[(*here, part)].reshape(n * n2 * 8, 128) for part in range(2)], axis=1)
    v = dot3(halves(v), (right1[0], right1[1]))
    for part in range(2):
        f_ref[(*here, part)] = v[:, 128 * part : 128 * part + 128].reshape(n, n2, 8, 128)


def rotate_kernel(f_ref, left_ref, sums_ref, re_ref, im_ref, purity_ref, stage, sem):
    r, c = lax.axis_index("row"), lax.axis_index("col")
    sums = sums_ref[...]
    lane = lanes((1, 128))
    total, trace_re, trace_im = (jnp.sum(jnp.where(lane == n, sums, 0.0)) for n in range(3))
    dim = GATE * GATE * LOW
    shifts = (jnp.where(r == c, MIX * trace_re / dim, 0.0), jnp.where(r == c, MIX * trace_im / dim, 0.0))
    squared = trace_re * trace_re + trace_im * trace_im
    purity_ref[0, 0] = (KEEP * KEEP * total + (2 * KEEP * MIX + MIX * MIX) * squared / dim) / (dim * dim)
    matrix = (left_ref[0], left_ref[1])
    sublane = lax.broadcasted_iota(jnp.int32, (8, 128), 0)
    copies = []
    for q in range(4):
        v = jnp.concatenate([f_ref[:, 4 * q + n].reshape(256, 128) for n in range(4)], axis=1)
        v = dot3(matrix, halves(v))
        for g in range(16):
            for part in range(2):
                row = 16 * g + 8 * part
                tiles = exchange([v[row : row + 8, 128 * n : 128 * n + 128] for n in range(4)])
                for k, tile in enumerate(tiles):
                    tile = KEEP * tile
                    if g // 4 == q:
                        tile = tile + jnp.where(lanes() == sublane + (32 * (g % 4) + 8 * k), shifts[part], 0.0)
                    stage[part, q, 32 * g + 8 * k : 32 * g + 8 * k + 8] = tile
        for part, ref in ((0, re_ref), (1, im_ref)):
            copies.append(pltpu.make_async_copy(stage.at[part, q], ref.at[:, pl.ds(128 * q, 128)], sem.at[part, q]))
            copies[-1].start()
    for copy in copies:
        copy.wait()


def rotate_call(f, left, sums):
    f32 = jnp.float32
    vmem, hbm = pl.BlockSpec(memory_space=pltpu.VMEM), pl.BlockSpec(memory_space=pltpu.HBM)
    return pl.pallas_call(
        rotate_kernel,
        name="rotate",
        out_shape=(
            jax.ShapeDtypeStruct((512, 512), f32),
            jax.ShapeDtypeStruct((512, 512), f32),
            jax.ShapeDtypeStruct((1, 1), f32),
        ),
        in_specs=[vmem, vmem, vmem],
        out_specs=(hbm, hbm, pl.BlockSpec(memory_space=pltpu.SMEM)),
        scratch_shapes=[pltpu.VMEM((2, 4, 512, 128), f32), pltpu.SemaphoreType.DMA((2, 4))],
        compiler_params=pltpu.CompilerParams(vmem_limit_bytes=20 * 2**20),
    )(f, left, sums)


def on_device(rho_real, rho_imag, gate_real_matrix, gate_imaginary, angles, targets, gate_order):
    args = (rho_real, rho_imag, gate_real_matrix, gate_imaginary, angles.T, targets, gate_order)
    f, left, sums = exchange_call(*(pltpu.with_memory_space_constraint(v, pltpu.HBM) for v in args))
    re, im, purity = rotate_call(f, left, sums)
    return re, im, purity.reshape(())


def solution(mesh):
    return jax.shard_map(
        on_device,
        mesh=mesh,
        in_specs=(P("row", "col"), P("row", "col"), P(), P(), P(), P(), P()),
        out_specs=(P("row", "col"), P("row", "col"), P()),
        check_vma=False,
    )
```

```python
import functools

import jax
import jax.numpy as jnp
from jax import lax
from jax.experimental import pallas as pl
from jax.experimental.pallas import tpu as pltpu
from jax.sharding import PartitionSpec as P

MESH = pl.DeviceIdType.MESH
HIGHEST = lax.Precision.HIGHEST
MIX = 0.25
KEEP = 1 - MIX
GATE = 16
LOW = 32
GATES = 8
BLOCK = (2, 8, 128)


def ring(v):
    v %= 8
    return min(v, 8 - v)


STEPS = [4, 3, -3, 2, -2, 1, -1, 0]
UNITS = []
for beta_ in range(8):
    found = []
    for dz_ in STEPS:
        if ring(beta_ - dz_) >= ring(dz_):
            found.append((dz_, 0))
        if ring(beta_ - dz_) > ring(dz_):
            found.append((dz_, 1))
    UNITS.append(found)
CHIPS = sorted(((jx, jy) for jx in range(4) for jy in range(4) if jx or jy), key=lambda j: (min(j[0], 4 - j[0]) + min(j[1], 4 - j[1]), j))
OTHERS = [(jx, jy, jc) for jx, jy in CHIPS for jc in range(2)]
BETAS = [7, 1, 6, 2, 5, 3, 4, 0]
FORWARDS = [[(*UNITS[b_][u_], b_) for b_ in BETAS if UNITS[b_][u_][0] != 0] for u_ in range(8)]
SLOT = {f_: i_ for i_, f_ in enumerate(f_ for fs_ in FORWARDS[1:] for f_ in fs_)}
GROUP = {dz_: int(ring(dz_) == 1) for dz_ in STEPS}


def wrap(v, n):
    return jnp.where(v >= n, v - n, v)


def near(v):
    return jnp.minimum(v, 8 - v)


def pick(index, values):
    out = jnp.int32(values[0])
    for i, value in enumerate(values):
        if value != values[0]:
            out = jnp.where(index == i, value, out)
    return out


def lanes(shape=(8, 128)):
    return lax.broadcasted_iota(jnp.int32, shape, 1)


def halve(a, b, mask, shift):
    turned = pltpu.roll(jnp.where(mask, b, a), shift, 1)
    return jnp.where(mask, a, turned), jnp.where(mask, turned, b)


def pack(src, dst, tmp, i):
    low = lanes() < 64
    even = (lanes() // 32) % 2 == 0
    groups = [(4 * i + n, part, q) for n in range(4) for part in range(2) for q in range(4)]
    for n, (h, part, q) in enumerate(groups):
        tiles = [src[part, 32 * h + 8 * k : 32 * h + 8 * k + 8, 128 * q : 128 * q + 128] for k in range(4)]
        for k in range(2):
            tmp[n, k], tmp[n, k + 2] = halve(tiles[k], tiles[k + 2], low, 64)
    for n, (h, part, q) in enumerate(groups):
        for m in range(2):
            at = 16 * h + 4 * q + 2 * m
            dst[at, part], dst[at + 1, part] = halve(tmp[n, 2 * m], tmp[n, 2 * m + 1], even, 32)


def exchange_kernel(
    re_hbm, im_hbm, ure_hbm, uim_hbm, angles_hbm, targets_hbm, order_hbm, out_ref, left_ref, sums_ref,
    own, turned, packed, mu, passing, f_ref, part_sums, plane_sums, small, angles, targets, order, right1, right2, tmp,
    load_sem, small_sem, s1, ru, r1, r1z, s2, r2, sa, ra, sb, rb,
):
    r, c = lax.axis_index("row"), lax.axis_index("col")
    z, ylo = c // 2, c % 2
    rho, core = r // 2, r % 2
    x, y = rho % 4, (rho // 4) * 2 + ylo
    partner = r + 1 - 2 * core
    beta = wrap(rho + 8 - z, 8)
    cores = (core, 1 - core)
    ahead = [wrap(x + jx, 4) * 2 for jx in range(4)]
    behind = [wrap(x + 4 - jx, 4) for jx in range(4)]
    halves_of = lambda yy, top: (jnp.where(yy >= 2, top, 0), jnp.where(yy >= 2, yy - 2, yy))
    up = [halves_of(wrap(y + jy, 4), 8) for jy in range(4)]
    down = [halves_of(wrap(y + 4 - jy, 4), 4) for jy in range(4)]

    def others(fn):
        for j, (jx, jy, jc) in enumerate(OTHERS):
            fn(up[jy][0] + ahead[jx] + cores[jc], up[jy][1], j)

    def copy(src, dst, send, recv, row, col):
        return pltpu.make_async_remote_copy(src, dst, send, recv, device_id=(row, col), device_id_type=MESH)

    loads = [
        [
            pltpu.make_async_copy(ref.at[pl.ds(128 * i, 128)], own.at[part, pl.ds(128 * i, 128)], load_sem.at[part, i])
            for part, ref in ((0, re_hbm), (1, im_hbm))
        ]
        for i in range(4)
    ]
    barrier = pltpu.get_barrier_semaphore()
    for k in (4, 3, 5, 2, 6, 1, 7):
        for h in (r, partner):
            pl.semaphore_signal(barrier, inc=1, device_id=(h, 2 * wrap(z + k, 8) + ylo), device_id_type=MESH)
    for pair in loads:
        for load in pair:
            load.start()

    def greet(h, p, j):
        pl.semaphore_signal(barrier, inc=1, device_id=(h, 2 * z + p), device_id_type=MESH)

    others(greet)
    greet(partner, ylo, 0)
    smalls = [
        pltpu.make_async_copy(ref, dst, small_sem.at[i])
        for i, (ref, dst) in enumerate(
            (
                (ure_hbm, small.at[0]),
                (uim_hbm, small.at[1]),
                (angles_hbm, angles),
                (targets_hbm, targets),
                (order_hbm, order),
            )
        )
    ]
    for load in smalls:
        load.start()
    for i, pair in enumerate(loads):
        for load in pair:
            load.wait()
        pack(own, packed.at[0], tmp, i)
    for i in range(4):
        rows = pl.ds(128 * i, 128)
        for j in range(4):
            there = pl.ds(128 * j, 128)
            turned[0, there, rows] = own[0, rows, there].T
            turned[1, there, rows] = -own[1, rows, there].T

    pl.semaphore_wait(barrier, 45)

    def at_step(dz):
        zz = wrap(z + dz % 8, 8)
        b = wrap(rho + 8 - zz, 8)
        return zz, b, near(b) >= ring(dz), near(b) > ring(dz)

    def straight(kind):
        for dz in STEPS[:-1]:
            zz, b, direct, also = at_step(dz)
            if kind == 1 and ring(dz) == 4:
                continue
            a = (-dz) % 8

            @pl.when(also if kind else direct)
            def _():
                for h in (r, partner):
                    copy(
                        packed.at[kind, 16 * h + 2 * zz + ylo],
                        f_ref.at[2 * a + ylo, 2 * b + core] if kind else f_ref.at[2 * b + core, 2 * a + ylo],
                        s2,
                        r2.at[GROUP[dz]],
                        h,
                        2 * zz + ylo,
                    ).start()

    def send_unit(u):
        unit = [UNITS[b][u] for b in range(8)]
        dz = pick(beta, [d % 8 for d, _ in unit])
        kind = pick(beta, [k for _, k in unit])
        zz = wrap(z + dz, 8)
        b = wrap(beta + 8 - dz, 8)
        first, second = jnp.where(kind == 0, core, ylo), jnp.where(kind == 0, ylo, core)
        if u == 0:
            others(lambda h, p, j: copy(packed.at[0, 16 * h + 2 * zz + p], mu.at[j], s1, ru.at[j], h, 2 * z + p).start())
            return

        def passed():
            row = 112 * kind + 16 * pick(beta, [STEPS.index(d) % 7 for d, _ in unit]) + 2 * b + first
            sem = r1.at[pick(beta, [SLOT.get((*unit[bb], bb), 0) for bb in range(8)])]
            others(lambda h, p, j: copy(packed.at[kind, 16 * h + 2 * zz + p], passing.at[row, second], s1, sem, h, 2 * z + p).start())

        def kept():
            row, col = jnp.where(kind == 0, 2 * b + core, ylo), jnp.where(kind == 0, ylo, 2 * b + core)

            def send(h, p, j):
                copy(packed.at[kind, 16 * h + 2 * zz + p], f_ref.at[row, col], s1, r1z, h, 2 * z + p).start()

            others(send)
            send(partner, ylo, 0)
            f_ref[row, col] = packed[kind, 16 * r + 2 * zz + ylo]

        away = [d != 0 for d, _ in unit]
        if all(away):
            passed()
        elif not any(away):
            kept()
        else:
            pl.when(dz != 0)(passed)
            pl.when(dz == 0)(kept)

    send_unit(0)
    straight(0)
    for i in range(4):
        pack(turned, packed.at[1], tmp, i)
    straight(1)
    send_unit(1)

    def arrived(sem, count):
        copy(packed.at[0, pl.ds(0, count)], packed.at[1, pl.ds(0, count)], sem, sem, r, c).wait_recv()

    def left(sem, count):
        copy(packed.at[0, pl.ds(0, count)], packed.at[1, pl.ds(0, count)], sem, sem, r, c).wait_send()

    def either(condition, wait, sem, counts):
        @pl.when(condition)
        def _():
            wait(sem, counts[0])

        @pl.when(jnp.logical_not(condition))
        def _():
            wait(sem, counts[1])

    def share_sums():
        def squares(i, accs):
            for n in range(2):
                rows = pl.ds(pl.multiple_of(16 * i + 8 * n, 8), 8)
                tiles = [own[part, rows, pl.ds(128 * q, 128)] for part in range(2) for q in range(4)]
                accs = [acc + v * v for acc, v in zip(accs, tiles)]
            return accs

        total = jnp.sum(sum(lax.fori_loop(0, 32, squares, [jnp.zeros((8, 128), jnp.float32)] * 8)))
        on_diagonal = lanes((128, 128)) == lax.broadcasted_iota(jnp.int32, (128, 128), 0)
        traces = []
        for part in range(2):
            v = sum(own[part, pl.ds(128 * q, 128), pl.ds(128 * q, 128)] for q in range(4))
            traces.append(jnp.where(r == c, jnp.sum(jnp.where(on_diagonal, v, 0.0)), 0.0))
        lane = lanes((1, 128))
        place = (y * 4 + x) * 2 + core
        part_sums[place] = jnp.where(lane == 0, total, jnp.where(lane == 1, traces[0], jnp.where(lane == 2, traces[1], 0.0)))

        def share(h, p, j):
            copy(part_sums.at[place], part_sums.at[place], sa, ra, h, 2 * z + p).start()

        others(share)
        share(partner, ylo, 0)

    def pass_on():
        for j, (jx, jy, jc) in enumerate(OTHERS):
            bs = wrap(wrap(down[jy][0] + behind[jx] + 8 - z, 8), 8)
            dz = pick(bs, [UNITS[b][0][0] % 8 for b in range(8)])
            a, b = wrap(8 - dz, 8), wrap(bs + 8 - dz, 8)
            copy(mu.at[j], mu.at[j], s1, ru.at[j], r, c).wait_recv()
            dst = f_ref.at[2 * b + cores[jc], 2 * a + down[jy][1]]
            copy(mu.at[j], dst, s2, r2.at[0], r, 2 * wrap(z + dz, 8) + ylo).start()

    def forward(u):
        for dz, kind, bb in FORWARDS[u]:
            n = SLOT[dz, kind, bb]
            a, b = (-dz) % 8, (bb - dz) % 8
            row = 112 * kind + 16 * (STEPS.index(dz) % 7) + 2 * b
            mine = beta == bb

            def onward(full):
                if kind == 0:
                    first, second = (0, 2), (0, 2) if full else (1 - ylo, 1)
                else:
                    first, second = (0, 2) if full else (1 - ylo, 1), (0, 2)
                src = passing.at[pl.ds(row + first[0], first[1]), pl.ds(*second)]
                at = (2 * b, 2 * a) if kind == 0 else (2 * a, 2 * b)
                dst = f_ref.at[pl.ds(at[0] + first[0], first[1]), pl.ds(at[1] + second[0], second[1])]
                copy(src, dst, s2, r2.at[GROUP[dz]], r, 2 * wrap(z + dz % 8, 8) + ylo).start()

            @pl.when(mine)
            def _():
                arrived(r1.at[n], 2)
                onward(False)

            @pl.when(jnp.logical_not(mine))
            def _():
                arrived(r1.at[n], 4)
                onward(True)

    pass_on()
    for u in range(1, 7):
        send_unit(u + 1)
        if u == 3:
            share_sums()
        forward(u)

    copy(part_sums.at[pl.ds(0, 31)], part_sums.at[pl.ds(0, 31)], sa, ra, r, c).wait_recv()
    plane_sums[z] = jnp.sum(part_sums[...], axis=0)
    for k in range(1, 8):
        copy(plane_sums.at[z], plane_sums.at[z], sb, rb, r, 2 * wrap(z + k, 8) + ylo).start()

    for load in smalls:
        load.wait()
    prepare(z, ylo, small, angles, targets, order, right1, right2, left_ref)
    either(beta == 0, arrived, r1z, (59, 58))
    on_lanes(f_ref, right1, 0, 2, 0, 16)
    on_lanes(f_ref, right1, 2, 14, 0, 2)
    arrived(r2.at[0], 100)
    for n in range(5):
        on_lanes(f_ref, right1, 4 + 2 * n, 2, 4, 10)
    either(beta == 0, left, s1, (241, 242))
    left(s2, 196)
    copy(plane_sums.at[pl.ds(0, 7)], plane_sums.at[pl.ds(0, 7)], sb, rb, r, c).wait()
    copy(part_sums.at[pl.ds(0, 31)], part_sums.at[pl.ds(0, 31)], sa, ra, r, c).wait_send()
    sums_ref[...] = jnp.sum(plane_sums[...], axis=0)
    arrived(r2.at[1], 96)
    on_lanes(f_ref, right1, 2, 2, 2, 14)
    on_lanes(f_ref, right1, 14, 2, 2, 14)
    on_lanes(f_ref, right1, 4, 10, 2, 2)
    on_lanes(f_ref, right1, 4, 10, 14, 2)
    matrix = (right2[0], right2[1])
    for n in range(8):
        v = jnp.concatenate([f_ref[2 * n + k].reshape(256, 128) for k in range(2)], axis=1)
        v = dot3(matrix, halves(v))
        for k in range(2):
            out_ref[2 * n + k] = v[:, 128 * k : 128 * k + 128].reshape((16,) + BLOCK)


def exchange_call(*args):
    f32, bf16 = jnp.float32, jnp.bfloat16
    dma = pltpu.SemaphoreType.DMA
    vmem, hbm = pl.BlockSpec(memory_space=pltpu.VMEM), pl.BlockSpec(memory_space=pltpu.HBM)
    blocks = lambda *n: pltpu.VMEM(n + BLOCK, f32)
    return pl.pallas_call(
        exchange_kernel,
        name="exchange",
        out_shape=(
            jax.ShapeDtypeStruct((16, 16) + BLOCK, f32),
            jax.ShapeDtypeStruct((2, 256, 256), bf16),
            jax.ShapeDtypeStruct((1, 128), f32),
        ),
        in_specs=[hbm] * 7,
        out_specs=(vmem, vmem, vmem),
        scratch_shapes=[
            pltpu.VMEM((2, 512, 512), f32),
            pltpu.VMEM((2, 512, 512), f32),
            blocks(2, 256),
            blocks(32),
            blocks(224, 2),
            blocks(16, 16),
            pltpu.VMEM((32, 1, 128), f32),
            pltpu.VMEM((8, 1, 128), f32),
            pltpu.VMEM((2, 16, 16), f32),
            pltpu.VMEM((3, 8), f32),
            pltpu.SMEM((8,), jnp.int32),
            pltpu.SMEM((8,), jnp.int32),
            pltpu.VMEM((2, 256, 256), bf16),
            pltpu.VMEM((2, 256, 256), bf16),
            pltpu.VMEM((32, 4, 8, 128), f32),
            dma((2, 4)),
            dma((5,)),
            dma,
            dma((32,)),
            dma((len(SLOT),)),
            dma,
            dma,
            dma((2,)),
            dma,
            dma,
            dma,
            dma,
        ],
        compiler_params=pltpu.CompilerParams(collective_id=0, has_side_effects=True, vmem_limit_bytes=40 * 2**20),
    )(*args)


def iota2(n, m, dim):
    return lax.broadcasted_iota(jnp.int32, (n, m), dim)


def halves(v):
    hi = v.astype(jnp.bfloat16)
    return hi, (v - hi.astype(jnp.float32)).astype(jnp.bfloat16)


def dot(a, b):
    return jnp.dot(a, b, preferred_element_type=jnp.float32)


def dot3(a, b):
    return dot(a[0], b[0]) + dot(a[0], b[1]) + dot(a[1], b[0])


def gate_factors(angles, targets, order):
    theta, alpha, beta = angles[0:1], angles[1:2], angles[2:3]
    cos, sin = jnp.cos(theta / 2), jnp.sin(theta / 2)
    both = alpha + beta
    elements = (
        (cos, cos * 0.0),
        (-jnp.cos(beta) * sin, -jnp.sin(beta) * sin),
        (jnp.cos(alpha) * sin, jnp.sin(alpha) * sin),
        (jnp.cos(both) * cos, jnp.sin(both) * cos),
    )
    i, j = iota2(32, 32, 0), iota2(32, 32, 1)
    left, right, high = i % 8, j % 8, i >= 16
    same_part, lower, same_factor = (i // 8) % 2 == (j // 8) % 2, i > j, i // 16 == j // 16
    gates = lax.broadcasted_iota(jnp.int32, (1, GATES), 1)
    total = jnp.where((iota2(32, 8, 0) % 16) == iota2(32, 8, 1), 1.0, 0.0)
    for position in range(GATES):
        gate = order[position]
        target = targets[gate]
        low_bit = jnp.where(target == 0, 1, jnp.where(target == 1, 2, jnp.where(target == 2, 4, 0)))
        high_bit = jnp.where(target == 3, 1, jnp.where(target == 4, 2, 0))
        bit = jnp.where(high, high_bit, low_bit)
        entry = [
            [jnp.sum(jnp.where(gates == gate, e, 0.0), axis=1, keepdims=True) for e in pair] for pair in elements
        ]
        left_high, right_high = (left & bit) > 0, (right & bit) > 0
        same_rest = ((left ^ right) | bit) == bit
        step = [
            jnp.where(
                left_high,
                jnp.where(right_high, entry[3][part], entry[2][part]),
                jnp.where(right_high, entry[1][part], entry[0][part]),
            )
            for part in range(2)
        ]
        step = [jnp.where(bit > 0, v, one) for v, one in zip(step, (1.0, 0.0))]
        step = jnp.where(same_part, step[0], jnp.where(lower, step[1], -step[1]))
        step = jnp.where(same_rest & same_factor, step, 0.0)
        total = jnp.dot(step, total, precision=HIGHEST, preferred_element_type=jnp.float32)
    return total


def one_hot(n, m, index):
    return jnp.where(index == iota2(n, m, 1), 1.0, 0.0)


def spread(rows, small, cols):
    wide = jnp.dot(rows, small, precision=HIGHEST, preferred_element_type=jnp.float32)
    return lax.dot_general(wide, cols, (((1,), (1,)), ((), ())), precision=HIGHEST, preferred_element_type=jnp.float32)


def times(a, b):
    return a[0] * b[0] - a[1] * b[1], a[0] * b[1] + a[1] * b[0]


def store_halves(ref, v):
    hi, lo = halves(v)
    ref[0] = hi
    ref[1] = lo


def prepare(z, ylo, small, angles, targets, order, right1, right2, left_ref):
    i, j = iota2(256, 256, 0), iota2(256, 256, 1)
    row = lambda n: iota2(256, n, 0)
    factors = gate_factors(angles[...], targets, order)
    low, high = ([factors[16 * w + 8 * part : 16 * w + 8 * part + 8] for part in range(2)] for w in range(2))
    out_g = one_hot(256, 16, row(16) // 16)
    in_g = one_hot(256, 16, (row(16) // 16 + 2 * z) % 16)
    u = [spread(out_g, small[part], in_g) for part in range(2)]
    same, lower = (i // 8) % 2 == (j // 8) % 2, (i // 8) % 2 > (j // 8) % 2
    value = jnp.where(same, u[0], jnp.where(lower, -u[1], u[1]))
    store_halves(right2, jnp.where(i % 8 == j % 8, value, 0.0))
    on_s = one_hot(256, 8, row(8) % 8)
    value = times(u, [spread(on_s, m, on_s) for m in low])
    store_halves(left_ref, jnp.where(same, value[0], jnp.where(lower, value[1], -value[1])))
    k = (row(8) // 32) % 4
    on_k = one_hot(256, 8, k)
    from_k = one_hot(256, 8, jnp.where((ylo == 1) & (k % 2 == 0), 2 - k, k))
    on_top = one_hot(256, 8, (row(8) // 8) % 4)
    turn = lambda hot, m, to: spread(hot, m.T, to)
    a = [turn(from_k, m, on_k) for m in high]
    b = times([turn(on_top, m, on_top) for m in high], [turn(on_s, m, on_s) for m in low])
    value = times(a, (b[0], -b[1]))
    same, lower = i // 128 == j // 128, i > j
    store_halves(right1, jnp.where(same, value[0], jnp.where(lower, -value[1], value[1])))


def on_lanes(f_ref, right1, g, n, g2, n2):
    here = (pl.ds(g, n), pl.ds(g2, n2))
    v = jnp.concatenate([f_ref[(*here, part)].reshape(n * n2 * 8, 128) for part in range(2)], axis=1)
    v = dot3(halves(v), (right1[0], right1[1]))
    for part in range(2):
        f_ref[(*here, part)] = v[:, 128 * part : 128 * part + 128].reshape(n, n2, 8, 128)


def rotate_kernel(f_ref, left_ref, sums_ref, re_ref, im_ref, purity_ref, stage, tmp, sem):
    r, c = lax.axis_index("row"), lax.axis_index("col")
    sums = sums_ref[...]
    lane = lanes((1, 128))
    total, trace_re, trace_im = (jnp.sum(jnp.where(lane == n, sums, 0.0)) for n in range(3))
    dim = GATE * GATE * LOW
    shifts = (jnp.where(r == c, MIX * trace_re / dim, 0.0), jnp.where(r == c, MIX * trace_im / dim, 0.0))
    squared = trace_re * trace_re + trace_im * trace_im
    purity_ref[0, 0] = (KEEP * KEEP * total + (2 * KEEP * MIX + MIX * MIX) * squared / dim) / (dim * dim)
    matrix = (left_ref[0], left_ref[1])
    sublane = lax.broadcasted_iota(jnp.int32, (8, 128), 0)
    copies = []
    low = lanes() < 64
    even = (lanes() // 32) % 2 == 0
    for q in range(4):
        v = jnp.concatenate([f_ref[:, 4 * q + n].reshape(256, 128) for n in range(4)], axis=1)
        v = dot3(matrix, halves(v))
        for n in range(32):
            tiles = [v[8 * n : 8 * n + 8, 128 * m : 128 * m + 128] for m in range(4)]
            for m in range(2):
                tmp[n, m], tmp[n, m + 2] = halve(tiles[m], tiles[m + 2], low, 64)
        for n in range(32):
            g, part = n // 2, n % 2
            for m in range(2):
                a, b = KEEP * tmp[n, 2 * m], KEEP * tmp[n, 2 * m + 1]
                pair = (jnp.where(even, a, pltpu.roll(b, 32, 1)), jnp.where(even, pltpu.roll(a, 96, 1), b))
                for k, tile in zip((2 * m, 2 * m + 1), pair):
                    if g // 4 == q:
                        tile = tile + jnp.where(lanes() == sublane + (32 * (g % 4) + 8 * k), shifts[part], 0.0)
                    stage[part, q, 32 * g + 8 * k : 32 * g + 8 * k + 8] = tile
        for part, ref in ((0, re_ref), (1, im_ref)):
            copies.append(pltpu.make_async_copy(stage.at[part, q], ref.at[:, pl.ds(128 * q, 128)], sem.at[part, q]))
            copies[-1].start()
    for copy in copies:
        copy.wait()


def rotate_call(f, left, sums):
    f32 = jnp.float32
    vmem, hbm = pl.BlockSpec(memory_space=pltpu.VMEM), pl.BlockSpec(memory_space=pltpu.HBM)
    return pl.pallas_call(
        rotate_kernel,
        name="rotate",
        out_shape=(
            jax.ShapeDtypeStruct((512, 512), f32),
            jax.ShapeDtypeStruct((512, 512), f32),
            jax.ShapeDtypeStruct((1, 1), f32),
        ),
        in_specs=[vmem, vmem, vmem],
        out_specs=(hbm, hbm, pl.BlockSpec(memory_space=pltpu.SMEM)),
        scratch_shapes=[
            pltpu.VMEM((2, 4, 512, 128), f32),
            pltpu.VMEM((32, 4, 8, 128), f32),
            pltpu.SemaphoreType.DMA((2, 4)),
        ],
        compiler_params=pltpu.CompilerParams(vmem_limit_bytes=20 * 2**20),
    )(f, left, sums)


def on_device(rho_real, rho_imag, gate_real_matrix, gate_imaginary, angles, targets, gate_order):
    args = (rho_real, rho_imag, gate_real_matrix, gate_imaginary, angles.T, targets, gate_order)
    f, left, sums = exchange_call(*(pltpu.with_memory_space_constraint(v, pltpu.HBM) for v in args))
    re, im, purity = rotate_call(f, left, sums)
    return re, im, purity.reshape(())


def solution(mesh):
    return jax.shard_map(
        on_device,
        mesh=mesh,
        in_specs=(P("row", "col"), P("row", "col"), P(), P(), P(), P(), P()),
        out_specs=(P("row", "col"), P("row", "col"), P()),
        check_vma=False,
    )
```

```python
import functools

import jax
import jax.numpy as jnp
from jax import lax
from jax.experimental import pallas as pl
from jax.experimental.pallas import tpu as pltpu
from jax.sharding import PartitionSpec as P

MESH = pl.DeviceIdType.MESH
HIGHEST = lax.Precision.HIGHEST
MIX = 0.25
KEEP = 1 - MIX
GATE = 16
LOW = 32
GATES = 8
BLOCK = (2, 8, 128)


def ring(v):
    v %= 8
    return min(v, 8 - v)


STEPS = [4, 3, -3, 2, -2, 1, -1, 0]
ORDER = [(d_, k_) for d_ in STEPS[:5] for k_ in (0, 1)] + [(d_, k_) for k_ in (0, 1) for d_ in (1, -1)] + [(0, 0), (0, 1)]
UNITS = [
    [(d_, k_) for d_, k_ in ORDER if ring(b_ - d_) >= ring(d_) + k_] for b_ in range(8)
]
BESIDE = {2: (1, 0), 3: (-1, 0)}
UNITS[0] = [u_ for u_ in UNITS[0] if u_ not in BESIDE.values()] + [None, None]
CHIPS = sorted(((jx, jy) for jx in range(4) for jy in range(4) if jx or jy), key=lambda j: (min(j[0], 4 - j[0]) + min(j[1], 4 - j[1]), j))
OTHERS = [(jx, jy, jc) for jx, jy in CHIPS for jc in range(2)]
BETAS = [7, 1, 6, 2, 5, 3, 4, 0]
FORWARDS = [
    [(*UNITS[b_][u_], b_) for b_ in BETAS if UNITS[b_][u_] and UNITS[b_][u_][0] != 0] + ([(*BESIDE[u_], 0)] if u_ in BESIDE else [])
    for u_ in range(8)
]
SLOT = {f_: i_ for i_, f_ in enumerate(f_ for fs_ in FORWARDS[1:] for f_ in fs_)}
AHEAD = {1:[2,3],2:[4],3:[5,6],4:[7],5:[]}


def group(dz, kind):
    return 1 + kind if ring(dz) == 1 else 0


def wrap(v, n):
    return jnp.where(v >= n, v - n, v)


def near(v):
    return jnp.minimum(v, 8 - v)


def pick(index, values):
    out = jnp.int32(values[0])
    for i, value in enumerate(values):
        if value != values[0]:
            out = jnp.where(index == i, value, out)
    return out


def lanes(shape=(8, 128)):
    return lax.broadcasted_iota(jnp.int32, shape, 1)


def halve(a, b, mask, shift):
    turned = pltpu.roll(jnp.where(mask, b, a), shift, 1)
    return jnp.where(mask, a, turned), jnp.where(mask, turned, b)


def pack(src, dst, tmp, i):
    low = lanes() < 64
    even = (lanes() // 32) % 2 == 0
    groups = [(4 * i + n, part, q) for n in range(4) for part in range(2) for q in range(4)]
    for n, (h, part, q) in enumerate(groups):
        tiles = [src[part, 32 * h + 8 * k : 32 * h + 8 * k + 8, 128 * q : 128 * q + 128] for k in range(4)]
        for k in range(2):
            tmp[n, k], tmp[n, k + 2] = halve(tiles[k], tiles[k + 2], low, 64)
    for n, (h, part, q) in enumerate(groups):
        for m in range(2):
            at = 16 * h + 4 * q + 2 * m
            dst[at, part], dst[at + 1, part] = halve(tmp[n, 2 * m], tmp[n, 2 * m + 1], even, 32)


def exchange_kernel(
    re_hbm, im_hbm, ure_hbm, uim_hbm, angles_hbm, targets_hbm, order_hbm, early_ref, late_ref, matrix_ref, sums_ref,
    own, turned, packed, mu, passing, f_ref, part_sums, plane_sums, small, angles, targets, order, factors, right1, right2, left, turned2, tmp,
    load_sem, small_sem, s1, ru, r1, r1z, s2, r2, sa, ra, sb, rb,
):
    r, c = lax.axis_index("row"), lax.axis_index("col")
    z, ylo = c // 2, c % 2
    rho, core = r // 2, r % 2
    x, y = rho % 4, (rho // 4) * 2 + ylo
    partner = r + 1 - 2 * core
    beta = wrap(rho + 8 - z, 8)
    cores = (core, 1 - core)
    ahead = [wrap(x + jx, 4) * 2 for jx in range(4)]
    behind = [wrap(x + 4 - jx, 4) for jx in range(4)]
    halves_of = lambda yy, top: (jnp.where(yy >= 2, top, 0), jnp.where(yy >= 2, yy - 2, yy))
    up = [halves_of(wrap(y + jy, 4), 8) for jy in range(4)]
    down = [halves_of(wrap(y + 4 - jy, 4), 4) for jy in range(4)]

    def others(fn):
        for j, (jx, jy, jc) in enumerate(OTHERS):
            fn(up[jy][0] + ahead[jx] + cores[jc], up[jy][1], j)

    def copy(src, dst, send, recv, row, col):
        return pltpu.make_async_remote_copy(src, dst, send, recv, device_id=(row, col), device_id_type=MESH)

    loads = [
        [
            pltpu.make_async_copy(ref.at[pl.ds(128 * i, 128)], own.at[part, pl.ds(128 * i, 128)], load_sem.at[part, i])
            for part, ref in ((0, re_hbm), (1, im_hbm))
        ]
        for i in range(4)
    ]
    barrier = pltpu.get_barrier_semaphore()
    for k in (4, 3, 5, 2, 6, 1, 7):
        for h in (r, partner):
            pl.semaphore_signal(barrier, inc=1, device_id=(h, 2 * wrap(z + k, 8) + ylo), device_id_type=MESH)
    for pair in loads:
        for load in pair:
            load.start()

    def greet(h, p, j):
        pl.semaphore_signal(barrier, inc=1, device_id=(h, 2 * z + p), device_id_type=MESH)

    others(greet)
    greet(partner, ylo, 0)
    smalls = [
        pltpu.make_async_copy(ref, dst, small_sem.at[i])
        for i, (ref, dst) in enumerate(
            (
                (ure_hbm, small.at[0]),
                (uim_hbm, small.at[1]),
                (angles_hbm, angles),
                (targets_hbm, targets),
                (order_hbm, order),
            )
        )
    ]
    for load in smalls:
        load.start()
    for i, pair in enumerate(loads):
        for load in pair:
            load.wait()
        pack(own, packed.at[0], tmp, i)
    for i in range(4):
        rows = pl.ds(128 * i, 128)
        for j in range(4):
            there = pl.ds(128 * j, 128)
            turned[0, there, rows] = own[0, rows, there].T
            turned[1, there, rows] = -own[1, rows, there].T

    pl.semaphore_wait(barrier, 45)

    def at_step(dz):
        zz = wrap(z + dz % 8, 8)
        b = wrap(rho + 8 - zz, 8)
        return zz, b, near(b) >= ring(dz), near(b) > ring(dz)

    def straight(kind):
        for dz in STEPS[:-1]:
            zz, b, direct, also = at_step(dz)
            if kind == 1 and ring(dz) == 4:
                continue
            a = (-dz) % 8

            @pl.when(also if kind else direct)
            def _():
                for h in (r, partner):
                    copy(
                        packed.at[kind, 16 * h + 2 * zz + ylo],
                        f_ref.at[2 * a + ylo, 2 * b + core] if kind else f_ref.at[2 * b + core, 2 * a + ylo],
                        s2,
                        r2.at[group(dz, kind)],
                        h,
                        2 * zz + ylo,
                    ).start()

    def send_unit(u):
        unit = [UNITS[b][u] or (0, 0) for b in range(8)]
        dz = pick(beta, [d % 8 for d, _ in unit])
        kind = pick(beta, [k for _, k in unit])
        zz = wrap(z + dz, 8)
        b = wrap(beta + 8 - dz, 8)
        first, second = jnp.where(kind == 0, core, ylo), jnp.where(kind == 0, ylo, core)
        if u == 0:
            others(lambda h, p, j: copy(packed.at[0, 16 * h + 2 * zz + p], mu.at[j], s1, ru.at[j], h, 2 * z + p).start())
            return

        def passed():
            row = 112 * kind + 16 * pick(beta, [STEPS.index(d) % 7 for d, _ in unit]) + 2 * b + first
            sem = r1.at[pick(beta, [SLOT.get((*unit[bb], bb), 0) for bb in range(8)])]
            others(lambda h, p, j: copy(packed.at[kind, 16 * h + 2 * zz + p], passing.at[row, second], s1, sem, h, 2 * z + p).start())

        def kept():
            row, col = jnp.where(kind == 0, 2 * b + core, ylo), jnp.where(kind == 0, ylo, 2 * b + core)

            def send(h, p, j):
                copy(packed.at[kind, 16 * h + 2 * zz + p], f_ref.at[row, col], s1, r1z, h, 2 * z + p).start()

            others(send)
            send(partner, ylo, 0)
            f_ref[row, col] = packed[kind, 16 * r + 2 * zz + ylo]

        here = [UNITS[bb][u] is not None and UNITS[bb][u][0] == 0 for bb in range(8)]
        away = [UNITS[bb][u] is not None and UNITS[bb][u][0] != 0 for bb in range(8)]
        for which, action in ((away, passed), (here, kept)):
            if all(which):
                action()
            elif any(which):
                pl.when(pick(beta, [int(v) for v in which]) == 1)(action)

        if u in BESIDE:

            @pl.when(beta == 0)
            def _():
                d, k = BESIDE[u]
                zb = wrap(z + d % 8, 8)
                row = 112 * k + 16 * STEPS.index(d) + 2 * (-d % 8) + core
                others(
                    lambda h, p, j: copy(
                        packed.at[k, 16 * h + 2 * zb + p], passing.at[row, ylo], s1, r1.at[SLOT[d, k, 0]], h, 2 * z + p
                    ).start()
                )

    send_unit(0)
    straight(0)
    for i in range(4):
        pack(turned, packed.at[1], tmp, i)
    straight(1)

    def arrived(sem, count):
        copy(packed.at[0, pl.ds(0, count)], packed.at[1, pl.ds(0, count)], sem, sem, r, c).wait_recv()

    def left_all(sem, count):
        copy(packed.at[0, pl.ds(0, count)], packed.at[1, pl.ds(0, count)], sem, sem, r, c).wait_send()

    def either(condition, wait, sem, counts):
        @pl.when(condition)
        def _():
            wait(sem, counts[0])

        @pl.when(jnp.logical_not(condition))
        def _():
            wait(sem, counts[1])

    def share_sums():
        def squares(i, accs):
            for n in range(2):
                rows = pl.ds(pl.multiple_of(16 * i + 8 * n, 8), 8)
                tiles = [own[part, rows, pl.ds(128 * q, 128)] for part in range(2) for q in range(4)]
                accs = [acc + v * v for acc, v in zip(accs, tiles)]
            return accs

        total = jnp.sum(sum(lax.fori_loop(0, 32, squares, [jnp.zeros((8, 128), jnp.float32)] * 8)))
        on_diagonal = lanes((128, 128)) == lax.broadcasted_iota(jnp.int32, (128, 128), 0)
        traces = []
        for part in range(2):
            v = sum(own[part, pl.ds(128 * q, 128), pl.ds(128 * q, 128)] for q in range(4))
            traces.append(jnp.where(r == c, jnp.sum(jnp.where(on_diagonal, v, 0.0)), 0.0))
        lane = lanes((1, 128))
        place = (y * 4 + x) * 2 + core
        part_sums[place] = jnp.where(lane == 0, total, jnp.where(lane == 1, traces[0], jnp.where(lane == 2, traces[1], 0.0)))

        def share(h, p, j):
            copy(part_sums.at[place], part_sums.at[place], sa, ra, h, 2 * z + p).start()

        others(share)
        share(partner, ylo, 0)

    def pass_on():
        for j, (jx, jy, jc) in enumerate(OTHERS):
            if j == 8:
                send_unit(1)
            bs = wrap(wrap(down[jy][0] + behind[jx] + 8 - z, 8), 8)
            dz = pick(bs, [UNITS[b][0][0] % 8 for b in range(8)])
            a, b = wrap(8 - dz, 8), wrap(bs + 8 - dz, 8)
            copy(mu.at[j], mu.at[j], s1, ru.at[j], r, c).wait_recv()
            dst = f_ref.at[2 * b + cores[jc], 2 * a + down[jy][1]]
            copy(mu.at[j], dst, s2, r2.at[0], r, 2 * wrap(z + dz, 8) + ylo).start()

    def forward(u):
        for dz, kind, bb in FORWARDS[u]:
            n = SLOT[dz, kind, bb]
            a, b = (-dz) % 8, (bb - dz) % 8
            row = 112 * kind + 16 * (STEPS.index(dz) % 7) + 2 * b
            mine = beta == bb

            def onward(full):
                if kind == 0:
                    first, second = (0, 2), (0, 2) if full else (1 - ylo, 1)
                else:
                    first, second = (0, 2) if full else (1 - ylo, 1), (0, 2)
                src = passing.at[pl.ds(row + first[0], first[1]), pl.ds(*second)]
                at = (2 * b, 2 * a) if kind == 0 else (2 * a, 2 * b)
                dst = f_ref.at[pl.ds(at[0] + first[0], first[1]), pl.ds(at[1] + second[0], second[1])]
                copy(src, dst, s2, r2.at[group(dz, kind)], r, 2 * wrap(z + dz % 8, 8) + ylo).start()

            @pl.when(mine)
            def _():
                arrived(r1.at[n], 2)
                onward(False)

            @pl.when(jnp.logical_not(mine))
            def _():
                arrived(r1.at[n], 4)
                onward(True)

    pass_on()
    for load in smalls:
        load.wait()
    for u in range(1, 6):
        for following in AHEAD[u]:
            send_unit(following)
        if u == 2:
            factors[...] = gate_factors(angles[...], targets, order)
        if u == 3:
            share_sums()
        if u == 4:
            prepare_lanes(ylo, factors[...], right1)
        if u == 5:
            prepare_rows(z, factors[...], small, right2, left, matrix_ref)
        forward(u)

    copy(part_sums.at[pl.ds(0, 31)], part_sums.at[pl.ds(0, 31)], sa, ra, r, c).wait_recv()
    plane_sums[z] = jnp.sum(part_sums[...], axis=0)
    for k in range(1, 8):
        copy(plane_sums.at[z], plane_sums.at[z], sb, rb, r, 2 * wrap(z + k, 8) + ylo).start()

    def over_g2(g, out):
        v = jnp.concatenate([f_ref[g + n].reshape(256, 128) for n in range(2)], axis=1)
        v = dot3((right2[0], right2[1]), halves(v))
        for n in range(2):
            out[n] = v[:, 128 * n : 128 * n + 128].reshape((16,) + BLOCK)

    either(beta == 0, arrived, r1z, (59, 58))
    on_lanes(f_ref, right1, 0, 2, 0, 16)
    on_lanes(f_ref, right1, 2, 14, 0, 2)
    turned2[pl.ds(2, 2)] = jnp.zeros((2, 16) + BLOCK, jnp.float32)
    turned2[pl.ds(14, 2)] = jnp.zeros((2, 16) + BLOCK, jnp.float32)
    arrived(r2.at[0], 100)
    for n in range(5):
        on_lanes(f_ref, right1, 4 + 2 * n, 2, 4, 10)
    arrived(r2.at[1], 56)
    on_lanes(f_ref, right1, 2, 14, 2, 2)
    on_lanes(f_ref, right1, 2, 14, 14, 2)
    for g in (0, 4, 6, 8, 10, 12):
        over_g2(g, turned2.at[pl.ds(g, 2)])
    for n in range(8):
        v = jnp.concatenate([turned2[:, 2 * n + m].reshape(256, 128) for m in range(2)], axis=1)
        early_ref[n // 2, :, 256 * (n % 2) : 256 * (n % 2) + 256] = dot3((left[0], left[1]), halves(v))
    either(beta == 0, left_all, s1, (241, 242))
    left_all(s2, 196)
    copy(plane_sums.at[pl.ds(0, 7)], plane_sums.at[pl.ds(0, 7)], sb, rb, r, c).wait()
    copy(part_sums.at[pl.ds(0, 31)], part_sums.at[pl.ds(0, 31)], sa, ra, r, c).wait_send()
    sums_ref[...] = jnp.sum(plane_sums[...], axis=0)
    arrived(r2.at[2], 40)
    on_lanes(f_ref, right1, 2, 2, 4, 10)
    on_lanes(f_ref, right1, 14, 2, 4, 10)
    over_g2(2, late_ref.at[pl.ds(0, 2)])
    over_g2(14, late_ref.at[pl.ds(2, 2)])


def exchange_call(*args):
    f32, bf16 = jnp.float32, jnp.bfloat16
    dma = pltpu.SemaphoreType.DMA
    vmem, hbm = pl.BlockSpec(memory_space=pltpu.VMEM), pl.BlockSpec(memory_space=pltpu.HBM)
    blocks = lambda *n: pltpu.VMEM(n + BLOCK, f32)
    return pl.pallas_call(
        exchange_kernel,
        name="exchange",
        out_shape=(
            jax.ShapeDtypeStruct((4, 256, 512), f32),
            jax.ShapeDtypeStruct((4, 16) + BLOCK, f32),
            jax.ShapeDtypeStruct((256, 256), bf16),
            jax.ShapeDtypeStruct((1, 128), f32),
        ),
        in_specs=[hbm] * 7,
        out_specs=(vmem, vmem, vmem, vmem),
        scratch_shapes=[
            pltpu.VMEM((2, 512, 512), f32),
            pltpu.VMEM((2, 512, 512), f32),
            blocks(2, 256),
            blocks(32),
            blocks(224, 2),
            blocks(16, 16),
            pltpu.VMEM((32, 1, 128), f32),
            pltpu.VMEM((8, 1, 128), f32),
            pltpu.VMEM((2, 16, 16), f32),
            pltpu.VMEM((3, 8), f32),
            pltpu.SMEM((8,), jnp.int32),
            pltpu.SMEM((8,), jnp.int32),
            pltpu.VMEM((32, 8), f32),
            pltpu.VMEM((2, 256, 256), bf16),
            pltpu.VMEM((2, 256, 256), bf16),
            pltpu.VMEM((2, 256, 256), bf16),
            blocks(16, 16),
            pltpu.VMEM((32, 4, 8, 128), f32),
            dma((2, 4)),
            dma((5,)),
            dma,
            dma((32,)),
            dma((len(SLOT),)),
            dma,
            dma,
            dma((3,)),
            dma,
            dma,
            dma,
            dma,
        ],
        compiler_params=pltpu.CompilerParams(collective_id=0, has_side_effects=True, vmem_limit_bytes=40 * 2**20),
    )(*args)


def iota2(n, m, dim):
    return lax.broadcasted_iota(jnp.int32, (n, m), dim)


def halves(v):
    hi = v.astype(jnp.bfloat16)
    return hi, (v - hi.astype(jnp.float32)).astype(jnp.bfloat16)


def dot(a, b):
    return jnp.dot(a, b, preferred_element_type=jnp.float32)


def dot3(a, b):
    return dot(a[0], b[0]) + dot(a[0], b[1]) + dot(a[1], b[0])


def gate_factors(angles, targets, order):
    theta, alpha, beta = angles[0:1], angles[1:2], angles[2:3]
    cos, sin = jnp.cos(theta / 2), jnp.sin(theta / 2)
    both = alpha + beta
    elements = (
        (cos, cos * 0.0),
        (-jnp.cos(beta) * sin, -jnp.sin(beta) * sin),
        (jnp.cos(alpha) * sin, jnp.sin(alpha) * sin),
        (jnp.cos(both) * cos, jnp.sin(both) * cos),
    )
    i, j = iota2(32, 32, 0), iota2(32, 32, 1)
    left, right, high = i % 8, j % 8, i >= 16
    same_part, lower, same_factor = (i // 8) % 2 == (j // 8) % 2, i > j, i // 16 == j // 16
    gates = lax.broadcasted_iota(jnp.int32, (1, GATES), 1)
    total = jnp.where((iota2(32, 8, 0) % 16) == iota2(32, 8, 1), 1.0, 0.0)
    for position in range(GATES):
        gate = order[position]
        target = targets[gate]
        low_bit = jnp.where(target == 0, 1, jnp.where(target == 1, 2, jnp.where(target == 2, 4, 0)))
        high_bit = jnp.where(target == 3, 1, jnp.where(target == 4, 2, 0))
        bit = jnp.where(high, high_bit, low_bit)
        entry = [
            [jnp.sum(jnp.where(gates == gate, e, 0.0), axis=1, keepdims=True) for e in pair] for pair in elements
        ]
        left_high, right_high = (left & bit) > 0, (right & bit) > 0
        same_rest = ((left ^ right) | bit) == bit
        step = [
            jnp.where(
                left_high,
                jnp.where(right_high, entry[3][part], entry[2][part]),
                jnp.where(right_high, entry[1][part], entry[0][part]),
            )
            for part in range(2)
        ]
        step = [jnp.where(bit > 0, v, one) for v, one in zip(step, (1.0, 0.0))]
        step = jnp.where(same_part, step[0], jnp.where(lower, step[1], -step[1]))
        step = jnp.where(same_rest & same_factor, step, 0.0)
        total = jnp.dot(step, total, precision=HIGHEST, preferred_element_type=jnp.float32)
    return total


def one_hot(n, m, index):
    return jnp.where(index == iota2(n, m, 1), 1.0, 0.0)


def spread(rows, small, cols):
    wide = jnp.dot(rows, small, precision=HIGHEST, preferred_element_type=jnp.float32)
    return lax.dot_general(wide, cols, (((1,), (1,)), ((), ())), precision=HIGHEST, preferred_element_type=jnp.float32)


def times(a, b):
    return a[0] * b[0] - a[1] * b[1], a[0] * b[1] + a[1] * b[0]


def store_halves(ref, v):
    hi, lo = halves(v)
    ref[0] = hi
    ref[1] = lo


def of(factors, which):
    return [factors[16 * which + 8 * part : 16 * which + 8 * part + 8] for part in range(2)]


def by_row(n):
    return iota2(256, n, 0)


def prepare_lanes(ylo, factors, right1):
    i, j = iota2(256, 256, 0), iota2(256, 256, 1)
    low, high = of(factors, 0), of(factors, 1)
    k = (by_row(8) // 32) % 4
    on_k = one_hot(256, 8, k)
    from_k = one_hot(256, 8, jnp.where((ylo == 1) & (k % 2 == 0), 2 - k, k))
    on_top = one_hot(256, 8, (by_row(8) // 8) % 4)
    on_s = one_hot(256, 8, by_row(8) % 8)
    turn = lambda hot, m, to: spread(hot, m.T, to)
    a = [turn(from_k, m, on_k) for m in high]
    b = times([turn(on_top, m, on_top) for m in high], [turn(on_s, m, on_s) for m in low])
    value = times(a, (b[0], -b[1]))
    same, lower = i // 128 == j // 128, i > j
    store_halves(right1, jnp.where(same, value[0], jnp.where(lower, -value[1], value[1])))


def prepare_rows(z, factors, small, right2, left, late_ref):
    i, j = iota2(256, 256, 0), iota2(256, 256, 1)
    low = of(factors, 0)
    out_g = one_hot(256, 16, by_row(16) // 16)
    in_g = one_hot(256, 16, (by_row(16) // 16 + 2 * z) % 16)
    u = [spread(out_g, small[part], in_g) for part in range(2)]
    same, lower = (i // 8) % 2 == (j // 8) % 2, (i // 8) % 2 > (j // 8) % 2
    value = jnp.where(same, u[0], jnp.where(lower, -u[1], u[1]))
    store_halves(right2, jnp.where(i % 8 == j % 8, value, 0.0))
    on_s = one_hot(256, 8, by_row(8) % 8)
    low = [spread(on_s, m, on_s) for m in low]
    real = lambda value: jnp.where(same, value[0], jnp.where(lower, value[1], -value[1]))
    store_halves(left, real(times(u, low)))
    n = (by_row(16) // 16) % 4
    in_g = one_hot(256, 16, (n + jnp.where(n < 2, 2, 12) + 2 * z) % 16)
    u = [spread(out_g, small[part], in_g) for part in range(2)]
    hi, lo = (v.astype(jnp.float32) for v in halves(real(times(u, low))))
    segment = j // 64
    late_ref[...] = jnp.where(segment == 3, 0.0, jnp.where(segment == 1, lo, hi)).astype(jnp.bfloat16)


def on_lanes(f_ref, right1, g, n, g2, n2):
    here = (pl.ds(g, n), pl.ds(g2, n2))
    v = jnp.concatenate([f_ref[(*here, part)].reshape(n * n2 * 8, 128) for part in range(2)], axis=1)
    v = dot3(halves(v), (right1[0], right1[1]))
    for part in range(2):
        f_ref[(*here, part)] = v[:, 128 * part : 128 * part + 128].reshape(n, n2, 8, 128)


def rotate_kernel(early_ref, late_ref, matrix_ref, sums_ref, re_ref, im_ref, purity_ref, stage, rotated, tmp, sem):
    r, c = lax.axis_index("row"), lax.axis_index("col")
    sums = sums_ref[...]
    lane = lanes((1, 128))
    total, trace_re, trace_im = (jnp.sum(jnp.where(lane == n, sums, 0.0)) for n in range(3))
    dim = GATE * GATE * LOW
    shifts = (jnp.where(r == c, MIX * trace_re / dim, 0.0), jnp.where(r == c, MIX * trace_im / dim, 0.0))
    squared = trace_re * trace_re + trace_im * trace_im
    purity_ref[0, 0] = (KEEP * KEEP * total + (2 * KEEP * MIX + MIX * MIX) * squared / dim) / (dim * dim)
    matrix = matrix_ref[...]
    sublane = lax.broadcasted_iota(jnp.int32, (8, 128), 0)
    low = lanes() < 64
    even = (lanes() // 32) % 2 == 0
    copies = []

    def product(q):
        v = jnp.concatenate([late_ref[:, 4 * q + m].reshape(64, 128) for m in range(4)], axis=1)
        hi, lo = halves(v)
        rotated[q] = early_ref[q] + dot(matrix, jnp.concatenate([hi, hi, lo, jnp.zeros_like(hi)], axis=0))

    product(0)
    for q in range(4):
        if q < 3:
            product(q + 1)
        for n in range(32):
            tiles = [rotated[q, 8 * n : 8 * n + 8, 128 * m : 128 * m + 128] for m in range(4)]
            for m in range(2):
                tmp[q, n, m], tmp[q, n, m + 2] = halve(tiles[m], tiles[m + 2], low, 64)
        for n in range(32):
            g, part = n // 2, n % 2
            for m in range(2):
                a, b = KEEP * tmp[q, n, 2 * m], KEEP * tmp[q, n, 2 * m + 1]
                pair = (jnp.where(even, a, pltpu.roll(b, 32, 1)), jnp.where(even, pltpu.roll(a, 96, 1), b))
                for k, tile in zip((2 * m, 2 * m + 1), pair):
                    if g // 4 == q:
                        tile = tile + jnp.where(lanes() == sublane + (32 * (g % 4) + 8 * k), shifts[part], 0.0)
                    stage[part, q, 32 * g + 8 * k : 32 * g + 8 * k + 8] = tile
        for part, ref in ((0, re_ref), (1, im_ref)):
            copies.append(pltpu.make_async_copy(stage.at[part, q], ref.at[:, pl.ds(128 * q, 128)], sem.at[part, q]))
            copies[-1].start()
    for copy in copies:
        copy.wait()


def rotate_call(*args):
    f32 = jnp.float32
    vmem, hbm = pl.BlockSpec(memory_space=pltpu.VMEM), pl.BlockSpec(memory_space=pltpu.HBM)
    return pl.pallas_call(
        rotate_kernel,
        name="rotate",
        out_shape=(
            jax.ShapeDtypeStruct((512, 512), f32),
            jax.ShapeDtypeStruct((512, 512), f32),
            jax.ShapeDtypeStruct((1, 1), f32),
        ),
        in_specs=[vmem] * 4,
        out_specs=(hbm, hbm, pl.BlockSpec(memory_space=pltpu.SMEM)),
        scratch_shapes=[
            pltpu.VMEM((2, 4, 512, 128), f32),
            pltpu.VMEM((4, 256, 512), f32),
            pltpu.VMEM((4, 32, 4, 8, 128), f32),
            pltpu.SemaphoreType.DMA((2, 4)),
        ],
        compiler_params=pltpu.CompilerParams(vmem_limit_bytes=20 * 2**20),
    )(*args)


def on_device(rho_real, rho_imag, gate_real_matrix, gate_imaginary, angles, targets, gate_order):
    args = (rho_real, rho_imag, gate_real_matrix, gate_imaginary, angles.T, targets, gate_order)
    found = exchange_call(*(pltpu.with_memory_space_constraint(v, pltpu.HBM) for v in args))
    re, im, purity = rotate_call(*found)
    return re, im, purity.reshape(())


def solution(mesh):
    return jax.shard_map(
        on_device,
        mesh=mesh,
        in_specs=(P("row", "col"), P("row", "col"), P(), P(), P(), P(), P()),
        out_specs=(P("row", "col"), P("row", "col"), P()),
        check_vma=False,
    )
```

```python
import functools

import jax
import jax.numpy as jnp
from jax import lax
from jax.experimental import pallas as pl
from jax.experimental.pallas import tpu as pltpu
from jax.sharding import PartitionSpec as P

MESH = pl.DeviceIdType.MESH
HIGHEST = lax.Precision.HIGHEST
MIX = 0.25
KEEP = 1 - MIX
GATE = 16
LOW = 32
GATES = 8
BLOCK = (2, 8, 128)


def ring(v):
    v %= 8
    return min(v, 8 - v)


STEPS = [4, 3, -3, 2, -2, 1, -1, 0]
ORDER = [(d_, k_) for d_ in STEPS[:5] for k_ in (0, 1)] + [(d_, k_) for k_ in (0, 1) for d_ in (1, -1)] + [(0, 0), (0, 1)]
UNITS = [
    [(d_, k_) for d_, k_ in ORDER if ring(b_ - d_) >= ring(d_) + k_] for b_ in range(8)
]
BESIDE = {2: (1, 0), 3: (-1, 0)}
UNITS[0] = [u_ for u_ in UNITS[0] if u_ not in BESIDE.values()] + [None, None]
CHIPS = sorted(((jx, jy) for jx in range(4) for jy in range(4) if jx or jy), key=lambda j: (min(j[0], 4 - j[0]) + min(j[1], 4 - j[1]), j))
HOPS = lambda j: min(j[0], 4 - j[0]) + min(j[1], 4 - j[1])
OTHERS = sorted(((jx, jy, jc) for jx, jy in CHIPS for jc in range(2)), key=lambda j: (HOPS(j), j[2], j))
BETAS = [7, 1, 6, 2, 5, 3, 4, 0]
FORWARDS = [
    [(*UNITS[b_][u_], b_) for b_ in BETAS if UNITS[b_][u_] and UNITS[b_][u_][0] != 0] + ([(*BESIDE[u_], 0)] if u_ in BESIDE else [])
    for u_ in range(8)
]
SLOT = {f_: i_ for i_, f_ in enumerate(f_ for fs_ in FORWARDS[1:] for f_ in fs_)}
AHEAD = {1:[2,3],2:[4],3:[5,6],4:[7],5:[]}


def group(dz, kind):
    return 1 + kind if ring(dz) == 1 else 0


def wrap(v, n):
    return jnp.where(v >= n, v - n, v)


def near(v):
    return jnp.minimum(v, 8 - v)


def pick(index, values):
    out = jnp.int32(values[0])
    for i, value in enumerate(values):
        if value != values[0]:
            out = jnp.where(index == i, value, out)
    return out


def lanes(shape=(8, 128)):
    return lax.broadcasted_iota(jnp.int32, shape, 1)


def halve(a, b, mask, shift):
    turned = pltpu.roll(jnp.where(mask, b, a), shift, 1)
    return jnp.where(mask, a, turned), jnp.where(mask, turned, b)


def pack(src, dst, tmp, i):
    low = lanes() < 64
    even = (lanes() // 32) % 2 == 0
    groups = [(4 * i + n, part, q) for n in range(4) for part in range(2) for q in range(4)]
    for n, (h, part, q) in enumerate(groups):
        tiles = [src[part, 32 * h + 8 * k : 32 * h + 8 * k + 8, 128 * q : 128 * q + 128] for k in range(4)]
        for k in range(2):
            tmp[n, k], tmp[n, k + 2] = halve(tiles[k], tiles[k + 2], low, 64)
    for n, (h, part, q) in enumerate(groups):
        for m in range(2):
            at = 16 * h + 4 * q + 2 * m
            dst[at, part], dst[at + 1, part] = halve(tmp[n, 2 * m], tmp[n, 2 * m + 1], even, 32)


def exchange_kernel(
    re_hbm, im_hbm, ure_hbm, uim_hbm, angles_hbm, targets_hbm, order_hbm, early_ref, late_ref, matrix_ref, sums_ref,
    own, turned, packed, mu, passing, f_ref, part_sums, plane_sums, small, angles, targets, order, factors, right1, right2, left, turned2, tmp,
    load_sem, small_sem, s1, ru, r1, r1z, s2, r2, sa, ra, sb, rb,
):
    r, c = lax.axis_index("row"), lax.axis_index("col")
    z, ylo = c // 2, c % 2
    rho, core = r // 2, r % 2
    x, y = rho % 4, (rho // 4) * 2 + ylo
    partner = r + 1 - 2 * core
    beta = wrap(rho + 8 - z, 8)
    cores = (core, 1 - core)
    ahead = [wrap(x + jx, 4) * 2 for jx in range(4)]
    behind = [wrap(x + 4 - jx, 4) for jx in range(4)]
    halves_of = lambda yy, top: (jnp.where(yy >= 2, top, 0), jnp.where(yy >= 2, yy - 2, yy))
    up = [halves_of(wrap(y + jy, 4), 8) for jy in range(4)]
    down = [halves_of(wrap(y + 4 - jy, 4), 4) for jy in range(4)]

    def others(fn):
        for j, (jx, jy, jc) in enumerate(OTHERS):
            fn(up[jy][0] + ahead[jx] + cores[jc], up[jy][1], j)

    def copy(src, dst, send, recv, row, col):
        return pltpu.make_async_remote_copy(src, dst, send, recv, device_id=(row, col), device_id_type=MESH)

    loads = [
        [
            pltpu.make_async_copy(ref.at[pl.ds(128 * i, 128)], own.at[part, pl.ds(128 * i, 128)], load_sem.at[part, i])
            for part, ref in ((0, re_hbm), (1, im_hbm))
        ]
        for i in range(4)
    ]
    barrier = pltpu.get_barrier_semaphore()
    for k in (4, 3, 5, 2, 6, 1, 7):
        for h in (r, partner):
            pl.semaphore_signal(barrier, inc=1, device_id=(h, 2 * wrap(z + k, 8) + ylo), device_id_type=MESH)
    for pair in loads:
        for load in pair:
            load.start()

    def greet(h, p, j):
        pl.semaphore_signal(barrier, inc=1, device_id=(h, 2 * z + p), device_id_type=MESH)

    for j, (jx, jy, jc) in reversed(list(enumerate(OTHERS))):
        greet(up[jy][0] + ahead[jx] + cores[jc], up[jy][1], j)
    greet(partner, ylo, 0)
    smalls = [
        pltpu.make_async_copy(ref, dst, small_sem.at[i])
        for i, (ref, dst) in enumerate(
            (
                (ure_hbm, small.at[0]),
                (uim_hbm, small.at[1]),
                (angles_hbm, angles),
                (targets_hbm, targets),
                (order_hbm, order),
            )
        )
    ]
    for load in smalls:
        load.start()
    for i, pair in enumerate(loads):
        for load in pair:
            load.wait()
        pack(own, packed.at[0], tmp, i)

    pl.semaphore_wait(barrier, 45)

    def at_step(dz):
        zz = wrap(z + dz % 8, 8)
        b = wrap(rho + 8 - zz, 8)
        return zz, b, near(b) >= ring(dz), near(b) > ring(dz)

    def straight(kind):
        for dz in STEPS[:-1]:
            zz, b, direct, also = at_step(dz)
            if kind == 1 and ring(dz) == 4:
                continue
            a = (-dz) % 8

            @pl.when(also if kind else direct)
            def _():
                for h in (r, partner):
                    copy(
                        packed.at[kind, 16 * h + 2 * zz + ylo],
                        f_ref.at[2 * a + ylo, 2 * b + core] if kind else f_ref.at[2 * b + core, 2 * a + ylo],
                        s2,
                        r2.at[group(dz, kind)],
                        h,
                        2 * zz + ylo,
                    ).start()

    def send_unit(u):
        unit = [UNITS[b][u] or (0, 0) for b in range(8)]
        dz = pick(beta, [d % 8 for d, _ in unit])
        kind = pick(beta, [k for _, k in unit])
        zz = wrap(z + dz, 8)
        b = wrap(beta + 8 - dz, 8)
        first, second = jnp.where(kind == 0, core, ylo), jnp.where(kind == 0, ylo, core)
        if u == 0:
            others(lambda h, p, j: copy(packed.at[0, 16 * h + 2 * zz + p], mu.at[j], s1, ru.at[j], h, 2 * z + p).start())
            return

        def passed():
            row = 112 * kind + 16 * pick(beta, [STEPS.index(d) % 7 for d, _ in unit]) + 2 * b + first
            sem = r1.at[pick(beta, [SLOT.get((*unit[bb], bb), 0) for bb in range(8)])]
            others(lambda h, p, j: copy(packed.at[kind, 16 * h + 2 * zz + p], passing.at[row, second], s1, sem, h, 2 * z + p).start())

        def kept():
            row, col = jnp.where(kind == 0, 2 * b + core, ylo), jnp.where(kind == 0, ylo, 2 * b + core)

            def send(h, p, j):
                copy(packed.at[kind, 16 * h + 2 * zz + p], f_ref.at[row, col], s1, r1z, h, 2 * z + p).start()

            others(send)
            send(partner, ylo, 0)
            f_ref[row, col] = packed[kind, 16 * r + 2 * zz + ylo]

        here = [UNITS[bb][u] is not None and UNITS[bb][u][0] == 0 for bb in range(8)]
        away = [UNITS[bb][u] is not None and UNITS[bb][u][0] != 0 for bb in range(8)]
        for which, action in ((away, passed), (here, kept)):
            if all(which):
                action()
            elif any(which):
                pl.when(pick(beta, [int(v) for v in which]) == 1)(action)

        if u in BESIDE:

            @pl.when(beta == 0)
            def _():
                d, k = BESIDE[u]
                zb = wrap(z + d % 8, 8)
                row = 112 * k + 16 * STEPS.index(d) + 2 * (-d % 8) + core
                others(
                    lambda h, p, j: copy(
                        packed.at[k, 16 * h + 2 * zb + p], passing.at[row, ylo], s1, r1.at[SLOT[d, k, 0]], h, 2 * z + p
                    ).start()
                )

    send_unit(0)
    straight(0)
    for i in range(4):
        rows = pl.ds(128 * i, 128)
        for j in range(4):
            there = pl.ds(128 * j, 128)
            turned[0, there, rows] = own[0, rows, there].T
            turned[1, there, rows] = -own[1, rows, there].T
    for i in range(4):
        pack(turned, packed.at[1], tmp, i)
    straight(1)

    def arrived(sem, count):
        copy(packed.at[0, pl.ds(0, count)], packed.at[1, pl.ds(0, count)], sem, sem, r, c).wait_recv()

    def left_all(sem, count):
        copy(packed.at[0, pl.ds(0, count)], packed.at[1, pl.ds(0, count)], sem, sem, r, c).wait_send()

    def either(condition, wait, sem, counts):
        @pl.when(condition)
        def _():
            wait(sem, counts[0])

        @pl.when(jnp.logical_not(condition))
        def _():
            wait(sem, counts[1])

    def share_sums():
        def squares(i, accs):
            for n in range(2):
                rows = pl.ds(pl.multiple_of(16 * i + 8 * n, 8), 8)
                tiles = [own[part, rows, pl.ds(128 * q, 128)] for part in range(2) for q in range(4)]
                accs = [acc + v * v for acc, v in zip(accs, tiles)]
            return accs

        total = jnp.sum(sum(lax.fori_loop(0, 32, squares, [jnp.zeros((8, 128), jnp.float32)] * 8)))
        on_diagonal = lanes((128, 128)) == lax.broadcasted_iota(jnp.int32, (128, 128), 0)
        traces = []
        for part in range(2):
            v = sum(own[part, pl.ds(128 * q, 128), pl.ds(128 * q, 128)] for q in range(4))
            traces.append(jnp.where(r == c, jnp.sum(jnp.where(on_diagonal, v, 0.0)), 0.0))
        lane = lanes((1, 128))
        place = (y * 4 + x) * 2 + core
        part_sums[place] = jnp.where(lane == 0, total, jnp.where(lane == 1, traces[0], jnp.where(lane == 2, traces[1], 0.0)))

        def share(h, p, j):
            copy(part_sums.at[place], part_sums.at[place], sa, ra, h, 2 * z + p).start()

        others(share)
        share(partner, ylo, 0)

    def pass_on():
        for j, (jx, jy, jc) in enumerate(OTHERS):
            if j == 8:
                send_unit(1)
            bs = wrap(wrap(down[jy][0] + behind[jx] + 8 - z, 8), 8)
            dz = pick(bs, [UNITS[b][0][0] % 8 for b in range(8)])
            a, b = wrap(8 - dz, 8), wrap(bs + 8 - dz, 8)
            copy(mu.at[j], mu.at[j], s1, ru.at[j], r, c).wait_recv()
            dst = f_ref.at[2 * b + cores[jc], 2 * a + down[jy][1]]
            copy(mu.at[j], dst, s2, r2.at[0], r, 2 * wrap(z + dz, 8) + ylo).start()

    def forward(u):
        for dz, kind, bb in FORWARDS[u]:
            n = SLOT[dz, kind, bb]
            a, b = (-dz) % 8, (bb - dz) % 8
            row = 112 * kind + 16 * (STEPS.index(dz) % 7) + 2 * b
            mine = beta == bb

            def onward(full):
                if kind == 0:
                    first, second = (0, 2), (0, 2) if full else (1 - ylo, 1)
                else:
                    first, second = (0, 2) if full else (1 - ylo, 1), (0, 2)
                src = passing.at[pl.ds(row + first[0], first[1]), pl.ds(*second)]
                at = (2 * b, 2 * a) if kind == 0 else (2 * a, 2 * b)
                dst = f_ref.at[pl.ds(at[0] + first[0], first[1]), pl.ds(at[1] + second[0], second[1])]
                copy(src, dst, s2, r2.at[group(dz, kind)], r, 2 * wrap(z + dz % 8, 8) + ylo).start()

            @pl.when(mine)
            def _():
                arrived(r1.at[n], 2)
                onward(False)

            @pl.when(jnp.logical_not(mine))
            def _():
                arrived(r1.at[n], 4)
                onward(True)

    pass_on()
    for load in smalls:
        load.wait()
    for u in range(1, 6):
        for following in AHEAD[u]:
            send_unit(following)
        if u == 2:
            factors[...] = gate_factors(angles[...], targets, order)
        if u == 3:
            share_sums()
        if u == 4:
            prepare_lanes(ylo, factors[...], right1)
        if u == 5:
            prepare_rows(z, factors[...], small, right2, left, matrix_ref)
        forward(u)

    copy(part_sums.at[pl.ds(0, 31)], part_sums.at[pl.ds(0, 31)], sa, ra, r, c).wait_recv()
    plane_sums[z] = jnp.sum(part_sums[...], axis=0)
    for k in range(1, 8):
        copy(plane_sums.at[z], plane_sums.at[z], sb, rb, r, 2 * wrap(z + k, 8) + ylo).start()

    def over_g2(g, out):
        v = jnp.concatenate([f_ref[g + n].reshape(256, 128) for n in range(2)], axis=1)
        v = dot3((right2[0], right2[1]), halves(v))
        for n in range(2):
            out[n] = v[:, 128 * n : 128 * n + 128].reshape((16,) + BLOCK)

    either(beta == 0, arrived, r1z, (59, 58))
    on_lanes(f_ref, right1, 0, 2, 0, 16)
    on_lanes(f_ref, right1, 2, 14, 0, 2)
    turned2[pl.ds(2, 2)] = jnp.zeros((2, 16) + BLOCK, jnp.float32)
    turned2[pl.ds(14, 2)] = jnp.zeros((2, 16) + BLOCK, jnp.float32)
    arrived(r2.at[0], 100)
    for n in range(5):
        on_lanes(f_ref, right1, 4 + 2 * n, 2, 4, 10)
    arrived(r2.at[1], 56)
    on_lanes(f_ref, right1, 2, 14, 2, 2)
    on_lanes(f_ref, right1, 2, 14, 14, 2)
    for g in (0, 4, 6, 8, 10, 12):
        over_g2(g, turned2.at[pl.ds(g, 2)])
    for n in range(8):
        v = jnp.concatenate([turned2[:, 2 * n + m].reshape(256, 128) for m in range(2)], axis=1)
        early_ref[n // 2, :, 256 * (n % 2) : 256 * (n % 2) + 256] = dot3((left[0], left[1]), halves(v))
    either(beta == 0, left_all, s1, (241, 242))
    left_all(s2, 196)
    copy(plane_sums.at[pl.ds(0, 7)], plane_sums.at[pl.ds(0, 7)], sb, rb, r, c).wait()
    copy(part_sums.at[pl.ds(0, 31)], part_sums.at[pl.ds(0, 31)], sa, ra, r, c).wait_send()
    sums_ref[...] = jnp.sum(plane_sums[...], axis=0)
    arrived(r2.at[2], 40)
    on_lanes(f_ref, right1, 2, 2, 4, 10)
    on_lanes(f_ref, right1, 14, 2, 4, 10)
    over_g2(2, late_ref.at[pl.ds(0, 2)])
    over_g2(14, late_ref.at[pl.ds(2, 2)])


def exchange_call(*args):
    f32, bf16 = jnp.float32, jnp.bfloat16
    dma = pltpu.SemaphoreType.DMA
    vmem, hbm = pl.BlockSpec(memory_space=pltpu.VMEM), pl.BlockSpec(memory_space=pltpu.HBM)
    blocks = lambda *n: pltpu.VMEM(n + BLOCK, f32)
    return pl.pallas_call(
        exchange_kernel,
        name="exchange",
        out_shape=(
            jax.ShapeDtypeStruct((4, 256, 512), f32),
            jax.ShapeDtypeStruct((4, 16) + BLOCK, f32),
            jax.ShapeDtypeStruct((256, 256), bf16),
            jax.ShapeDtypeStruct((1, 128), f32),
        ),
        in_specs=[hbm] * 7,
        out_specs=(vmem, vmem, vmem, vmem),
        scratch_shapes=[
            pltpu.VMEM((2, 512, 512), f32),
            pltpu.VMEM((2, 512, 512), f32),
            blocks(2, 256),
            blocks(32),
            blocks(224, 2),
            blocks(16, 16),
            pltpu.VMEM((32, 1, 128), f32),
            pltpu.VMEM((8, 1, 128), f32),
            pltpu.VMEM((2, 16, 16), f32),
            pltpu.VMEM((3, 8), f32),
            pltpu.SMEM((8,), jnp.int32),
            pltpu.SMEM((8,), jnp.int32),
            pltpu.VMEM((32, 8), f32),
            pltpu.VMEM((2, 256, 256), bf16),
            pltpu.VMEM((2, 256, 256), bf16),
            pltpu.VMEM((2, 256, 256), bf16),
            blocks(16, 16),
            pltpu.VMEM((32, 4, 8, 128), f32),
            dma((2, 4)),
            dma((5,)),
            dma,
            dma((32,)),
            dma((len(SLOT),)),
            dma,
            dma,
            dma((3,)),
            dma,
            dma,
            dma,
            dma,
        ],
        compiler_params=pltpu.CompilerParams(collective_id=0, has_side_effects=True, vmem_limit_bytes=40 * 2**20),
    )(*args)


def iota2(n, m, dim):
    return lax.broadcasted_iota(jnp.int32, (n, m), dim)


def halves(v):
    hi = v.astype(jnp.bfloat16)
    return hi, (v - hi.astype(jnp.float32)).astype(jnp.bfloat16)


def dot(a, b):
    return jnp.dot(a, b, preferred_element_type=jnp.float32)


def dot3(a, b):
    return dot(a[0], b[0]) + dot(a[0], b[1]) + dot(a[1], b[0])


def gate_factors(angles, targets, order):
    theta, alpha, beta = angles[0:1], angles[1:2], angles[2:3]
    cos, sin = jnp.cos(theta / 2), jnp.sin(theta / 2)
    both = alpha + beta
    elements = (
        (cos, cos * 0.0),
        (-jnp.cos(beta) * sin, -jnp.sin(beta) * sin),
        (jnp.cos(alpha) * sin, jnp.sin(alpha) * sin),
        (jnp.cos(both) * cos, jnp.sin(both) * cos),
    )
    i, j = iota2(32, 32, 0), iota2(32, 32, 1)
    left, right, high = i % 8, j % 8, i >= 16
    same_part, lower, same_factor = (i // 8) % 2 == (j // 8) % 2, i > j, i // 16 == j // 16
    gates = lax.broadcasted_iota(jnp.int32, (1, GATES), 1)
    total = jnp.where((iota2(32, 8, 0) % 16) == iota2(32, 8, 1), 1.0, 0.0)
    for position in range(GATES):
        gate = order[position]
        target = targets[gate]
        low_bit = jnp.where(target == 0, 1, jnp.where(target == 1, 2, jnp.where(target == 2, 4, 0)))
        high_bit = jnp.where(target == 3, 1, jnp.where(target == 4, 2, 0))
        bit = jnp.where(high, high_bit, low_bit)
        entry = [
            [jnp.sum(jnp.where(gates == gate, e, 0.0), axis=1, keepdims=True) for e in pair] for pair in elements
        ]
        left_high, right_high = (left & bit) > 0, (right & bit) > 0
        same_rest = ((left ^ right) | bit) == bit
        step = [
            jnp.where(
                left_high,
                jnp.where(right_high, entry[3][part], entry[2][part]),
                jnp.where(right_high, entry[1][part], entry[0][part]),
            )
            for part in range(2)
        ]
        step = [jnp.where(bit > 0, v, one) for v, one in zip(step, (1.0, 0.0))]
        step = jnp.where(same_part, step[0], jnp.where(lower, step[1], -step[1]))
        step = jnp.where(same_rest & same_factor, step, 0.0)
        total = jnp.dot(step, total, precision=HIGHEST, preferred_element_type=jnp.float32)
    return total


def one_hot(n, m, index):
    return jnp.where(index == iota2(n, m, 1), 1.0, 0.0)


def spread(rows, small, cols):
    wide = jnp.dot(rows, small, precision=HIGHEST, preferred_element_type=jnp.float32)
    return lax.dot_general(wide, cols, (((1,), (1,)), ((), ())), precision=HIGHEST, preferred_element_type=jnp.float32)


def times(a, b):
    return a[0] * b[0] - a[1] * b[1], a[0] * b[1] + a[1] * b[0]


def store_halves(ref, v):
    hi, lo = halves(v)
    ref[0] = hi
    ref[1] = lo


def of(factors, which):
    return [factors[16 * which + 8 * part : 16 * which + 8 * part + 8] for part in range(2)]


def by_row(n):
    return iota2(256, n, 0)


def prepare_lanes(ylo, factors, right1):
    i, j = iota2(256, 256, 0), iota2(256, 256, 1)
    low, high = of(factors, 0), of(factors, 1)
    k = (by_row(8) // 32) % 4
    on_k = one_hot(256, 8, k)
    from_k = one_hot(256, 8, jnp.where((ylo == 1) & (k % 2 == 0), 2 - k, k))
    on_top = one_hot(256, 8, (by_row(8) // 8) % 4)
    on_s = one_hot(256, 8, by_row(8) % 8)
    turn = lambda hot, m, to: spread(hot, m.T, to)
    a = [turn(from_k, m, on_k) for m in high]
    b = times([turn(on_top, m, on_top) for m in high], [turn(on_s, m, on_s) for m in low])
    value = times(a, (b[0], -b[1]))
    same, lower = i // 128 == j // 128, i > j
    store_halves(right1, jnp.where(same, value[0], jnp.where(lower, -value[1], value[1])))


def prepare_rows(z, factors, small, right2, left, late_ref):
    i, j = iota2(256, 256, 0), iota2(256, 256, 1)
    low = of(factors, 0)
    out_g = one_hot(256, 16, by_row(16) // 16)
    in_g = one_hot(256, 16, (by_row(16) // 16 + 2 * z) % 16)
    u = [spread(out_g, small[part], in_g) for part in range(2)]
    same, lower = (i // 8) % 2 == (j // 8) % 2, (i // 8) % 2 > (j // 8) % 2
    value = jnp.where(same, u[0], jnp.where(lower, -u[1], u[1]))
    store_halves(right2, jnp.where(i % 8 == j % 8, value, 0.0))
    on_s = one_hot(256, 8, by_row(8) % 8)
    low = [spread(on_s, m, on_s) for m in low]
    real = lambda value: jnp.where(same, value[0], jnp.where(lower, value[1], -value[1]))
    store_halves(left, real(times(u, low)))
    n = (by_row(16) // 16) % 4
    in_g = one_hot(256, 16, (n + jnp.where(n < 2, 2, 12) + 2 * z) % 16)
    u = [spread(out_g, small[part], in_g) for part in range(2)]
    hi, lo = (v.astype(jnp.float32) for v in halves(real(times(u, low))))
    segment = j // 64
    late_ref[...] = jnp.where(segment == 3, 0.0, jnp.where(segment == 1, lo, hi)).astype(jnp.bfloat16)


def on_lanes(f_ref, right1, g, n, g2, n2):
    here = (pl.ds(g, n), pl.ds(g2, n2))
    v = jnp.concatenate([f_ref[(*here, part)].reshape(n * n2 * 8, 128) for part in range(2)], axis=1)
    v = dot3(halves(v), (right1[0], right1[1]))
    for part in range(2):
        f_ref[(*here, part)] = v[:, 128 * part : 128 * part + 128].reshape(n, n2, 8, 128)


def rotate_kernel(early_ref, late_ref, matrix_ref, sums_ref, re_ref, im_ref, purity_ref, stage, rotated, tmp, sem):
    r, c = lax.axis_index("row"), lax.axis_index("col")
    sums = sums_ref[...]
    lane = lanes((1, 128))
    total, trace_re, trace_im = (jnp.sum(jnp.where(lane == n, sums, 0.0)) for n in range(3))
    dim = GATE * GATE * LOW
    shifts = (jnp.where(r == c, MIX * trace_re / dim, 0.0), jnp.where(r == c, MIX * trace_im / dim, 0.0))
    squared = trace_re * trace_re + trace_im * trace_im
    purity_ref[0, 0] = (KEEP * KEEP * total + (2 * KEEP * MIX + MIX * MIX) * squared / dim) / (dim * dim)
    matrix = matrix_ref[...]
    sublane = lax.broadcasted_iota(jnp.int32, (8, 128), 0)
    low = lanes() < 64
    even = (lanes() // 32) % 2 == 0
    copies = []

    def product(q):
        v = jnp.concatenate([late_ref[:, 4 * q + m].reshape(64, 128) for m in range(4)], axis=1)
        hi, lo = halves(v)
        rotated[q] = early_ref[q] + dot(matrix, jnp.concatenate([hi, hi, lo, jnp.zeros_like(hi)], axis=0))

    product(0)
    for q in range(4):
        if q < 3:
            product(q + 1)
        for n in range(32):
            tiles = [rotated[q, 8 * n : 8 * n + 8, 128 * m : 128 * m + 128] for m in range(4)]
            for m in range(2):
                tmp[q, n, m], tmp[q, n, m + 2] = halve(tiles[m], tiles[m + 2], low, 64)
        for n in range(32):
            g, part = n // 2, n % 2
            for m in range(2):
                a, b = KEEP * tmp[q, n, 2 * m], KEEP * tmp[q, n, 2 * m + 1]
                pair = (jnp.where(even, a, pltpu.roll(b, 32, 1)), jnp.where(even, pltpu.roll(a, 96, 1), b))
                for k, tile in zip((2 * m, 2 * m + 1), pair):
                    if g // 4 == q:
                        tile = tile + jnp.where(lanes() == sublane + (32 * (g % 4) + 8 * k), shifts[part], 0.0)
                    stage[part, q, 32 * g + 8 * k : 32 * g + 8 * k + 8] = tile
        for part, ref in ((0, re_ref), (1, im_ref)):
            copies.append(pltpu.make_async_copy(stage.at[part, q], ref.at[:, pl.ds(128 * q, 128)], sem.at[part, q]))
            copies[-1].start()
    for copy in copies:
        copy.wait()


def rotate_call(*args):
    f32 = jnp.float32
    vmem, hbm = pl.BlockSpec(memory_space=pltpu.VMEM), pl.BlockSpec(memory_space=pltpu.HBM)
    return pl.pallas_call(
        rotate_kernel,
        name="rotate",
        out_shape=(
            jax.ShapeDtypeStruct((512, 512), f32),
            jax.ShapeDtypeStruct((512, 512), f32),
            jax.ShapeDtypeStruct((1, 1), f32),
        ),
        in_specs=[vmem] * 4,
        out_specs=(hbm, hbm, pl.BlockSpec(memory_space=pltpu.SMEM)),
        scratch_shapes=[
            pltpu.VMEM((2, 4, 512, 128), f32),
            pltpu.VMEM((4, 256, 512), f32),
            pltpu.VMEM((4, 32, 4, 8, 128), f32),
            pltpu.SemaphoreType.DMA((2, 4)),
        ],
        compiler_params=pltpu.CompilerParams(vmem_limit_bytes=20 * 2**20),
    )(*args)


def on_device(rho_real, rho_imag, gate_real_matrix, gate_imaginary, angles, targets, gate_order):
    args = (rho_real, rho_imag, gate_real_matrix, gate_imaginary, angles.T, targets, gate_order)
    found = exchange_call(*(pltpu.with_memory_space_constraint(v, pltpu.HBM) for v in args))
    re, im, purity = rotate_call(*found)
    return re, im, purity.reshape(())


def solution(mesh):
    return jax.shard_map(
        on_device,
        mesh=mesh,
        in_specs=(P("row", "col"), P("row", "col"), P(), P(), P(), P(), P()),
        out_specs=(P("row", "col"), P("row", "col"), P()),
        check_vma=False,
    )
```

```python
import functools

import jax
import jax.numpy as jnp
from jax import lax
from jax.experimental import pallas as pl
from jax.experimental.pallas import tpu as pltpu
from jax.sharding import PartitionSpec as P

MESH = pl.DeviceIdType.MESH
HIGHEST = lax.Precision.HIGHEST
MIX = 0.25
KEEP = 1 - MIX
GATE = 16
LOW = 32
GATES = 8
BLOCK = (2, 8, 128)


def ring(v):
    v %= 8
    return min(v, 8 - v)


STEPS = [4, 3, -3, 2, -2, 1, -1, 0]
ORDER = [(d_, k_) for d_ in STEPS[:5] for k_ in (0, 1)] + [(d_, k_) for k_ in (0, 1) for d_ in (1, -1)] + [(0, 0), (0, 1)]
UNITS = [
    [(d_, k_) for d_, k_ in ORDER if ring(b_ - d_) >= ring(d_) + k_] for b_ in range(8)
]
BESIDE = {2: (1, 0), 3: (-1, 0)}
UNITS[0] = [u_ for u_ in UNITS[0] if u_ not in BESIDE.values()] + [None, None]
CHIPS = sorted(((jx, jy) for jx in range(4) for jy in range(4) if jx or jy), key=lambda j: (min(j[0], 4 - j[0]) + min(j[1], 4 - j[1]), j))
HOPS = lambda j: min(j[0], 4 - j[0]) + min(j[1], 4 - j[1])
OTHERS = sorted(((jx, jy, jc) for jx, jy in CHIPS for jc in range(2)), key=lambda j: (HOPS(j), j[2], j))
BETAS = [7, 1, 6, 2, 5, 3, 4, 0]
FORWARDS = [
    [(*UNITS[b_][u_], b_) for b_ in BETAS if UNITS[b_][u_] and UNITS[b_][u_][0] != 0] + ([(*BESIDE[u_], 0)] if u_ in BESIDE else [])
    for u_ in range(8)
]
SLOT = {f_: i_ for i_, f_ in enumerate(f_ for fs_ in FORWARDS[1:] for f_ in fs_)}
AHEAD = {1:[2,3],2:[4],3:[5,6],4:[7],5:[]}


def group(dz, kind):
    return 1 + kind if ring(dz) == 1 else 0


def wrap(v, n):
    return jnp.where(v >= n, v - n, v)


def near(v):
    return jnp.minimum(v, 8 - v)


def pick(index, values):
    out = jnp.int32(values[0])
    for i, value in enumerate(values):
        if value != values[0]:
            out = jnp.where(index == i, value, out)
    return out


def lanes(shape=(8, 128)):
    return lax.broadcasted_iota(jnp.int32, shape, 1)


def halve(a, b, mask, shift):
    turned = pltpu.roll(jnp.where(mask, b, a), shift, 1)
    return jnp.where(mask, a, turned), jnp.where(mask, turned, b)


def pack(src, dst, tmp, i):
    low = lanes() < 64
    even = (lanes() // 32) % 2 == 0
    groups = [(4 * i + n, part, q) for n in range(4) for part in range(2) for q in range(4)]
    for n, (h, part, q) in enumerate(groups):
        tiles = [src[part, 32 * h + 8 * k : 32 * h + 8 * k + 8, 128 * q : 128 * q + 128] for k in range(4)]
        for k in range(2):
            tmp[n, k], tmp[n, k + 2] = halve(tiles[k], tiles[k + 2], low, 64)
    for n, (h, part, q) in enumerate(groups):
        for m in range(2):
            at = 16 * h + 4 * q + 2 * m
            dst[at, part], dst[at + 1, part] = halve(tmp[n, 2 * m], tmp[n, 2 * m + 1], even, 32)


def unpack(ref, tmp, rows):
    low = lanes() < 64
    even = (lanes() // 32) % 2 == 0
    groups = [(g, part, q) for g in rows for part in range(2) for q in range(4)]
    for n, (g, part, q) in enumerate(groups):
        for m in range(2):
            tmp[n, m], tmp[n, m + 2] = halve(ref[g, 4 * q + m, part], ref[g, 4 * q + m + 2, part], low, 64)
    for n, (g, part, q) in enumerate(groups):
        for m in range(2):
            a, b = tmp[n, 2 * m], tmp[n, 2 * m + 1]
            ref[g, 4 * q + 2 * m, part] = jnp.where(even, a, pltpu.roll(b, 32, 1))
            ref[g, 4 * q + 2 * m + 1, part] = jnp.where(even, pltpu.roll(a, 96, 1), b)


def exchange_kernel(
    re_hbm, im_hbm, ure_hbm, uim_hbm, angles_hbm, targets_hbm, order_hbm, early_ref, late_ref, matrix_ref, sums_ref,
    own, turned, packed, mu, passing, f_ref, part_sums, plane_sums, small, angles, targets, order, factors, right1, right2, left, turned2, tmp,
    load_sem, small_sem, s1, ru, r1, r1z, s2, r2, sa, ra, sb, rb,
):
    r, c = lax.axis_index("row"), lax.axis_index("col")
    z, ylo = c // 2, c % 2
    rho, core = r // 2, r % 2
    x, y = rho % 4, (rho // 4) * 2 + ylo
    partner = r + 1 - 2 * core
    beta = wrap(rho + 8 - z, 8)
    cores = (core, 1 - core)
    ahead = [wrap(x + jx, 4) * 2 for jx in range(4)]
    behind = [wrap(x + 4 - jx, 4) for jx in range(4)]
    halves_of = lambda yy, top: (jnp.where(yy >= 2, top, 0), jnp.where(yy >= 2, yy - 2, yy))
    up = [halves_of(wrap(y + jy, 4), 8) for jy in range(4)]
    down = [halves_of(wrap(y + 4 - jy, 4), 4) for jy in range(4)]

    def others(fn):
        for j, (jx, jy, jc) in enumerate(OTHERS):
            fn(up[jy][0] + ahead[jx] + cores[jc], up[jy][1], j)

    def copy(src, dst, send, recv, row, col):
        return pltpu.make_async_remote_copy(src, dst, send, recv, device_id=(row, col), device_id_type=MESH)

    loads = [
        [
            pltpu.make_async_copy(ref.at[pl.ds(128 * i, 128)], own.at[part, pl.ds(128 * i, 128)], load_sem.at[part, i])
            for part, ref in ((0, re_hbm), (1, im_hbm))
        ]
        for i in range(4)
    ]
    barrier = pltpu.get_barrier_semaphore()
    for k in (4, 3, 5, 2, 6, 1, 7):
        for h in (r, partner):
            pl.semaphore_signal(barrier, inc=1, device_id=(h, 2 * wrap(z + k, 8) + ylo), device_id_type=MESH)
    for pair in loads:
        for load in pair:
            load.start()

    def greet(h, p, j):
        pl.semaphore_signal(barrier, inc=1, device_id=(h, 2 * z + p), device_id_type=MESH)

    for j, (jx, jy, jc) in reversed(list(enumerate(OTHERS))):
        greet(up[jy][0] + ahead[jx] + cores[jc], up[jy][1], j)
    greet(partner, ylo, 0)
    smalls = [
        pltpu.make_async_copy(ref, dst, small_sem.at[i])
        for i, (ref, dst) in enumerate(
            (
                (ure_hbm, small.at[0]),
                (uim_hbm, small.at[1]),
                (angles_hbm, angles),
                (targets_hbm, targets),
                (order_hbm, order),
            )
        )
    ]
    for load in smalls:
        load.start()
    for i, pair in enumerate(loads):
        for load in pair:
            load.wait()
        pack(own, packed.at[0], tmp, i)

    pl.semaphore_wait(barrier, 45)

    def at_step(dz):
        zz = wrap(z + dz % 8, 8)
        b = wrap(rho + 8 - zz, 8)
        return zz, b, near(b) >= ring(dz), near(b) > ring(dz)

    def straight(kind):
        for dz in STEPS[:-1]:
            zz, b, direct, also = at_step(dz)
            if kind == 1 and ring(dz) == 4:
                continue
            a = (-dz) % 8

            @pl.when(also if kind else direct)
            def _():
                for h in (r, partner):
                    copy(
                        packed.at[kind, 16 * h + 2 * zz + ylo],
                        f_ref.at[2 * a + ylo, 2 * b + core] if kind else f_ref.at[2 * b + core, 2 * a + ylo],
                        s2,
                        r2.at[group(dz, kind)],
                        h,
                        2 * zz + ylo,
                    ).start()

    def send_unit(u):
        unit = [UNITS[b][u] or (0, 0) for b in range(8)]
        dz = pick(beta, [d % 8 for d, _ in unit])
        kind = pick(beta, [k for _, k in unit])
        zz = wrap(z + dz, 8)
        b = wrap(beta + 8 - dz, 8)
        first, second = jnp.where(kind == 0, core, ylo), jnp.where(kind == 0, ylo, core)
        if u == 0:
            others(lambda h, p, j: copy(packed.at[0, 16 * h + 2 * zz + p], mu.at[j], s1, ru.at[j], h, 2 * z + p).start())
            return

        def passed():
            row = 112 * kind + 16 * pick(beta, [STEPS.index(d) % 7 for d, _ in unit]) + 2 * b + first
            sem = r1.at[pick(beta, [SLOT.get((*unit[bb], bb), 0) for bb in range(8)])]
            others(lambda h, p, j: copy(packed.at[kind, 16 * h + 2 * zz + p], passing.at[row, second], s1, sem, h, 2 * z + p).start())

        def kept():
            row, col = jnp.where(kind == 0, 2 * b + core, ylo), jnp.where(kind == 0, ylo, 2 * b + core)

            def send(h, p, j):
                copy(packed.at[kind, 16 * h + 2 * zz + p], f_ref.at[row, col], s1, r1z, h, 2 * z + p).start()

            others(send)
            send(partner, ylo, 0)
            f_ref[row, col] = packed[kind, 16 * r + 2 * zz + ylo]

        here = [UNITS[bb][u] is not None and UNITS[bb][u][0] == 0 for bb in range(8)]
        away = [UNITS[bb][u] is not None and UNITS[bb][u][0] != 0 for bb in range(8)]
        for which, action in ((away, passed), (here, kept)):
            if all(which):
                action()
            elif any(which):
                pl.when(pick(beta, [int(v) for v in which]) == 1)(action)

        if u in BESIDE:

            @pl.when(beta == 0)
            def _():
                d, k = BESIDE[u]
                zb = wrap(z + d % 8, 8)
                row = 112 * k + 16 * STEPS.index(d) + 2 * (-d % 8) + core
                others(
                    lambda h, p, j: copy(
                        packed.at[k, 16 * h + 2 * zb + p], passing.at[row, ylo], s1, r1.at[SLOT[d, k, 0]], h, 2 * z + p
                    ).start()
                )

    send_unit(0)
    straight(0)
    for i in range(4):
        rows = pl.ds(128 * i, 128)
        for j in range(4):
            there = pl.ds(128 * j, 128)
            turned[0, there, rows] = own[0, rows, there].T
            turned[1, there, rows] = -own[1, rows, there].T
    for i in range(4):
        pack(turned, packed.at[1], tmp, i)
    straight(1)

    def arrived(sem, count):
        copy(packed.at[0, pl.ds(0, count)], packed.at[1, pl.ds(0, count)], sem, sem, r, c).wait_recv()

    def left_all(sem, count):
        copy(packed.at[0, pl.ds(0, count)], packed.at[1, pl.ds(0, count)], sem, sem, r, c).wait_send()

    def either(condition, wait, sem, counts):
        @pl.when(condition)
        def _():
            wait(sem, counts[0])

        @pl.when(jnp.logical_not(condition))
        def _():
            wait(sem, counts[1])

    def share_sums():
        def squares(i, accs):
            for n in range(2):
                rows = pl.ds(pl.multiple_of(16 * i + 8 * n, 8), 8)
                tiles = [own[part, rows, pl.ds(128 * q, 128)] for part in range(2) for q in range(4)]
                accs = [acc + v * v for acc, v in zip(accs, tiles)]
            return accs

        total = jnp.sum(sum(lax.fori_loop(0, 32, squares, [jnp.zeros((8, 128), jnp.float32)] * 8)))
        on_diagonal = lanes((128, 128)) == lax.broadcasted_iota(jnp.int32, (128, 128), 0)
        traces = []
        for part in range(2):
            v = sum(own[part, pl.ds(128 * q, 128), pl.ds(128 * q, 128)] for q in range(4))
            traces.append(jnp.where(r == c, jnp.sum(jnp.where(on_diagonal, v, 0.0)), 0.0))
        lane = lanes((1, 128))
        place = (y * 4 + x) * 2 + core
        part_sums[place] = jnp.where(lane == 0, total, jnp.where(lane == 1, traces[0], jnp.where(lane == 2, traces[1], 0.0)))

        def share(h, p, j):
            copy(part_sums.at[place], part_sums.at[place], sa, ra, h, 2 * z + p).start()

        others(share)
        share(partner, ylo, 0)

    def pass_on():
        for j, (jx, jy, jc) in enumerate(OTHERS):
            if j == 8:
                send_unit(1)
            bs = wrap(wrap(down[jy][0] + behind[jx] + 8 - z, 8), 8)
            dz = pick(bs, [UNITS[b][0][0] % 8 for b in range(8)])
            a, b = wrap(8 - dz, 8), wrap(bs + 8 - dz, 8)
            copy(mu.at[j], mu.at[j], s1, ru.at[j], r, c).wait_recv()
            dst = f_ref.at[2 * b + cores[jc], 2 * a + down[jy][1]]
            copy(mu.at[j], dst, s2, r2.at[0], r, 2 * wrap(z + dz, 8) + ylo).start()

    def forward(u):
        for dz, kind, bb in FORWARDS[u]:
            n = SLOT[dz, kind, bb]
            a, b = (-dz) % 8, (bb - dz) % 8
            row = 112 * kind + 16 * (STEPS.index(dz) % 7) + 2 * b
            mine = beta == bb

            def onward(full):
                if kind == 0:
                    first, second = (0, 2), (0, 2) if full else (1 - ylo, 1)
                else:
                    first, second = (0, 2) if full else (1 - ylo, 1), (0, 2)
                src = passing.at[pl.ds(row + first[0], first[1]), pl.ds(*second)]
                at = (2 * b, 2 * a) if kind == 0 else (2 * a, 2 * b)
                dst = f_ref.at[pl.ds(at[0] + first[0], first[1]), pl.ds(at[1] + second[0], second[1])]
                copy(src, dst, s2, r2.at[group(dz, kind)], r, 2 * wrap(z + dz % 8, 8) + ylo).start()

            @pl.when(mine)
            def _():
                arrived(r1.at[n], 2)
                onward(False)

            @pl.when(jnp.logical_not(mine))
            def _():
                arrived(r1.at[n], 4)
                onward(True)

    pass_on()
    for load in smalls:
        load.wait()
    for u in range(1, 6):
        for following in AHEAD[u]:
            send_unit(following)
        if u == 2:
            factors[...] = gate_factors(angles[...], targets, order)
        if u == 3:
            share_sums()
        if u == 4:
            prepare_lanes(ylo, factors[...], right1)
        if u == 5:
            prepare_rows(z, factors[...], small, right2, left, matrix_ref)
        forward(u)

    copy(part_sums.at[pl.ds(0, 31)], part_sums.at[pl.ds(0, 31)], sa, ra, r, c).wait_recv()
    plane_sums[z] = jnp.sum(part_sums[...], axis=0)
    for k in range(1, 8):
        copy(plane_sums.at[z], plane_sums.at[z], sb, rb, r, 2 * wrap(z + k, 8) + ylo).start()

    def over_g2(g, out):
        v = jnp.concatenate([f_ref[g + n].reshape(256, 128) for n in range(2)], axis=1)
        v = dot3((right2[0], right2[1]), halves(v))
        for n in range(2):
            out[n] = v[:, 128 * n : 128 * n + 128].reshape((16,) + BLOCK)

    either(beta == 0, arrived, r1z, (59, 58))
    on_lanes(f_ref, right1, 0, 2, 0, 16)
    on_lanes(f_ref, right1, 2, 14, 0, 2)
    turned2[pl.ds(2, 2)] = jnp.zeros((2, 16) + BLOCK, jnp.float32)
    turned2[pl.ds(14, 2)] = jnp.zeros((2, 16) + BLOCK, jnp.float32)
    arrived(r2.at[0], 100)
    for n in range(5):
        on_lanes(f_ref, right1, 4 + 2 * n, 2, 4, 10)
    arrived(r2.at[1], 56)
    on_lanes(f_ref, right1, 2, 14, 2, 2)
    on_lanes(f_ref, right1, 2, 14, 14, 2)
    for g in (0, 4, 6, 8, 10, 12):
        over_g2(g, turned2.at[pl.ds(g, 2)])
    for rows in ((0, 1, 4, 5), (6, 7, 8, 9), (10, 11, 12, 13)):
        unpack(turned2, tmp, rows)
    for n in range(8):
        v = jnp.concatenate([turned2[:, 2 * n + m].reshape(256, 128) for m in range(2)], axis=1)
        early_ref[n // 2, :, 256 * (n % 2) : 256 * (n % 2) + 256] = dot3((left[0], left[1]), halves(v))
    either(beta == 0, left_all, s1, (241, 242))
    left_all(s2, 196)
    copy(plane_sums.at[pl.ds(0, 7)], plane_sums.at[pl.ds(0, 7)], sb, rb, r, c).wait()
    copy(part_sums.at[pl.ds(0, 31)], part_sums.at[pl.ds(0, 31)], sa, ra, r, c).wait_send()
    sums_ref[...] = jnp.sum(plane_sums[...], axis=0)
    arrived(r2.at[2], 40)
    on_lanes(f_ref, right1, 2, 2, 4, 10)
    on_lanes(f_ref, right1, 14, 2, 4, 10)
    over_g2(2, late_ref.at[pl.ds(0, 2)])
    over_g2(14, late_ref.at[pl.ds(2, 2)])
    unpack(late_ref, tmp, range(4))


def exchange_call(*args):
    f32, bf16 = jnp.float32, jnp.bfloat16
    dma = pltpu.SemaphoreType.DMA
    vmem, hbm = pl.BlockSpec(memory_space=pltpu.VMEM), pl.BlockSpec(memory_space=pltpu.HBM)
    blocks = lambda *n: pltpu.VMEM(n + BLOCK, f32)
    return pl.pallas_call(
        exchange_kernel,
        name="exchange",
        out_shape=(
            jax.ShapeDtypeStruct((4, 256, 512), f32),
            jax.ShapeDtypeStruct((4, 16) + BLOCK, f32),
            jax.ShapeDtypeStruct((256, 256), bf16),
            jax.ShapeDtypeStruct((1, 128), f32),
        ),
        in_specs=[hbm] * 7,
        out_specs=(vmem, vmem, vmem, vmem),
        scratch_shapes=[
            pltpu.VMEM((2, 512, 512), f32),
            pltpu.VMEM((2, 512, 512), f32),
            blocks(2, 256),
            blocks(32),
            blocks(224, 2),
            blocks(16, 16),
            pltpu.VMEM((32, 1, 128), f32),
            pltpu.VMEM((8, 1, 128), f32),
            pltpu.VMEM((2, 16, 16), f32),
            pltpu.VMEM((3, 8), f32),
            pltpu.SMEM((8,), jnp.int32),
            pltpu.SMEM((8,), jnp.int32),
            pltpu.VMEM((32, 8), f32),
            pltpu.VMEM((2, 256, 256), bf16),
            pltpu.VMEM((2, 256, 256), bf16),
            pltpu.VMEM((2, 256, 256), bf16),
            blocks(16, 16),
            pltpu.VMEM((32, 4, 8, 128), f32),
            dma((2, 4)),
            dma((5,)),
            dma,
            dma((32,)),
            dma((len(SLOT),)),
            dma,
            dma,
            dma((3,)),
            dma,
            dma,
            dma,
            dma,
        ],
        compiler_params=pltpu.CompilerParams(collective_id=0, has_side_effects=True, vmem_limit_bytes=40 * 2**20),
    )(*args)


def iota2(n, m, dim):
    return lax.broadcasted_iota(jnp.int32, (n, m), dim)


def halves(v):
    hi = v.astype(jnp.bfloat16)
    return hi, (v - hi.astype(jnp.float32)).astype(jnp.bfloat16)


def dot(a, b):
    return jnp.dot(a, b, preferred_element_type=jnp.float32)


def dot3(a, b):
    return dot(a[0], b[0]) + dot(a[0], b[1]) + dot(a[1], b[0])


def gate_factors(angles, targets, order):
    theta, alpha, beta = angles[0:1], angles[1:2], angles[2:3]
    cos, sin = jnp.cos(theta / 2), jnp.sin(theta / 2)
    both = alpha + beta
    elements = (
        (cos, cos * 0.0),
        (-jnp.cos(beta) * sin, -jnp.sin(beta) * sin),
        (jnp.cos(alpha) * sin, jnp.sin(alpha) * sin),
        (jnp.cos(both) * cos, jnp.sin(both) * cos),
    )
    i, j = iota2(32, 32, 0), iota2(32, 32, 1)
    left, right, high = i % 8, j % 8, i >= 16
    same_part, lower, same_factor = (i // 8) % 2 == (j // 8) % 2, i > j, i // 16 == j // 16
    gates = lax.broadcasted_iota(jnp.int32, (1, GATES), 1)
    total = jnp.where((iota2(32, 8, 0) % 16) == iota2(32, 8, 1), 1.0, 0.0)
    for position in range(GATES):
        gate = order[position]
        target = targets[gate]
        low_bit = jnp.where(target == 0, 1, jnp.where(target == 1, 2, jnp.where(target == 2, 4, 0)))
        high_bit = jnp.where(target == 3, 1, jnp.where(target == 4, 2, 0))
        bit = jnp.where(high, high_bit, low_bit)
        entry = [
            [jnp.sum(jnp.where(gates == gate, e, 0.0), axis=1, keepdims=True) for e in pair] for pair in elements
        ]
        left_high, right_high = (left & bit) > 0, (right & bit) > 0
        same_rest = ((left ^ right) | bit) == bit
        step = [
            jnp.where(
                left_high,
                jnp.where(right_high, entry[3][part], entry[2][part]),
                jnp.where(right_high, entry[1][part], entry[0][part]),
            )
            for part in range(2)
        ]
        step = [jnp.where(bit > 0, v, one) for v, one in zip(step, (1.0, 0.0))]
        step = jnp.where(same_part, step[0], jnp.where(lower, step[1], -step[1]))
        step = jnp.where(same_rest & same_factor, step, 0.0)
        total = jnp.dot(step, total, precision=HIGHEST, preferred_element_type=jnp.float32)
    return total


def one_hot(n, m, index):
    return jnp.where(index == iota2(n, m, 1), 1.0, 0.0)


def spread(rows, small, cols):
    wide = jnp.dot(rows, small, precision=HIGHEST, preferred_element_type=jnp.float32)
    return lax.dot_general(wide, cols, (((1,), (1,)), ((), ())), precision=HIGHEST, preferred_element_type=jnp.float32)


def times(a, b):
    return a[0] * b[0] - a[1] * b[1], a[0] * b[1] + a[1] * b[0]


def store_halves(ref, v):
    hi, lo = halves(v)
    ref[0] = hi
    ref[1] = lo


def of(factors, which):
    return [factors[16 * which + 8 * part : 16 * which + 8 * part + 8] for part in range(2)]


def by_row(n):
    return iota2(256, n, 0)


def prepare_lanes(ylo, factors, right1):
    i, j = iota2(256, 256, 0), iota2(256, 256, 1)
    low, high = of(factors, 0), of(factors, 1)
    k = (by_row(8) // 32) % 4
    on_k = one_hot(256, 8, k)
    from_k = one_hot(256, 8, jnp.where((ylo == 1) & (k % 2 == 0), 2 - k, k))
    on_top = one_hot(256, 8, (by_row(8) // 8) % 4)
    on_s = one_hot(256, 8, by_row(8) % 8)
    turn = lambda hot, m, to: spread(hot, m.T, to)
    a = [turn(from_k, m, on_k) for m in high]
    b = times([turn(on_top, m, on_top) for m in high], [turn(on_s, m, on_s) for m in low])
    value = times(a, (b[0], -b[1]))
    same, lower = i // 128 == j // 128, i > j
    store_halves(right1, jnp.where(same, value[0], jnp.where(lower, -value[1], value[1])))


def prepare_rows(z, factors, small, right2, left, late_ref):
    i, j = iota2(256, 256, 0), iota2(256, 256, 1)
    low = of(factors, 0)
    out_g = one_hot(256, 16, by_row(16) // 16)
    in_g = one_hot(256, 16, (by_row(16) // 16 + 2 * z) % 16)
    u = [spread(out_g, small[part], in_g) for part in range(2)]
    same, lower = (i // 8) % 2 == (j // 8) % 2, (i // 8) % 2 > (j // 8) % 2
    value = jnp.where(same, u[0], jnp.where(lower, -u[1], u[1]))
    store_halves(right2, jnp.where(i % 8 == j % 8, value, 0.0))
    on_s = one_hot(256, 8, by_row(8) % 8)
    low = [spread(on_s, m, on_s) for m in low]
    real = lambda value: KEEP * jnp.where(same, value[0], jnp.where(lower, value[1], -value[1]))
    store_halves(left, real(times(u, low)))
    n = (by_row(16) // 16) % 4
    in_g = one_hot(256, 16, (n + jnp.where(n < 2, 2, 12) + 2 * z) % 16)
    u = [spread(out_g, small[part], in_g) for part in range(2)]
    hi, lo = (v.astype(jnp.float32) for v in halves(real(times(u, low))))
    segment = j // 64
    late_ref[...] = jnp.where(segment == 3, 0.0, jnp.where(segment == 1, lo, hi)).astype(jnp.bfloat16)


def on_lanes(f_ref, right1, g, n, g2, n2):
    here = (pl.ds(g, n), pl.ds(g2, n2))
    v = jnp.concatenate([f_ref[(*here, part)].reshape(n * n2 * 8, 128) for part in range(2)], axis=1)
    v = dot3(halves(v), (right1[0], right1[1]))
    for part in range(2):
        f_ref[(*here, part)] = v[:, 128 * part : 128 * part + 128].reshape(n, n2, 8, 128)


def rotate_kernel(early_ref, late_ref, matrix_ref, sums_ref, re_ref, im_ref, purity_ref, purity, stage, product, sem, purity_sem):
    r, c = lax.axis_index("row"), lax.axis_index("col")
    sums = sums_ref[...]
    lane = lanes((1, 128))
    total, trace_re, trace_im = (jnp.sum(jnp.where(lane == n, sums, 0.0)) for n in range(3))
    dim = GATE * GATE * LOW
    shifts = (jnp.where(r == c, MIX * trace_re / dim, 0.0), jnp.where(r == c, MIX * trace_im / dim, 0.0))
    squared = trace_re * trace_re + trace_im * trace_im
    purity[0, 0] = (KEEP * KEEP * total + (2 * KEEP * MIX + MIX * MIX) * squared / dim) / (dim * dim)
    matrix = matrix_ref[...]
    sublane = lax.broadcasted_iota(jnp.int32, (8, 128), 0)
    v = jnp.concatenate([late_ref[:, n].reshape(64, 128) for n in range(16)], axis=1)
    hi, lo = halves(v)
    product[...] = dot(matrix, jnp.concatenate([hi, hi, lo, jnp.zeros_like(hi)], axis=0))
    copies = [pltpu.make_async_copy(purity, purity_ref, purity_sem)]
    copies[0].start()
    for q in range(4):
        for g in range(16):
            for part in range(2):
                for k in range(4):
                    row, col = 16 * g + 8 * part, 128 * k
                    tile = early_ref[q, row : row + 8, col : col + 128]
                    tile = tile + product[row : row + 8, 512 * q + col : 512 * q + col + 128]
                    if g // 4 == q:
                        tile = tile + jnp.where(lanes() == sublane + (32 * (g % 4) + 8 * k), shifts[part], 0.0)
                    stage[part, q, 32 * g + 8 * k : 32 * g + 8 * k + 8] = tile
        for part, ref in ((0, re_ref), (1, im_ref)):
            copies.append(pltpu.make_async_copy(stage.at[part, q], ref.at[:, pl.ds(128 * q, 128)], sem.at[part, q]))
            copies[-1].start()
    for copy in copies:
        copy.wait()


def rotate_call(*args):
    f32 = jnp.float32
    vmem, hbm = pl.BlockSpec(memory_space=pltpu.VMEM), pl.BlockSpec(memory_space=pltpu.HBM)
    return pl.pallas_call(
        rotate_kernel,
        name="rotate",
        out_shape=(
            jax.ShapeDtypeStruct((512, 512), f32),
            jax.ShapeDtypeStruct((512, 512), f32),
            jax.ShapeDtypeStruct((1, 1), f32),
        ),
        in_specs=[vmem] * 4,
        out_specs=(hbm, hbm, hbm),
        scratch_shapes=[
            pltpu.SMEM((1, 1), f32),
            pltpu.VMEM((2, 4, 512, 128), f32),
            pltpu.VMEM((256, 2048), f32),
            pltpu.SemaphoreType.DMA((2, 4)),
            pltpu.SemaphoreType.DMA,
        ],
        compiler_params=pltpu.CompilerParams(vmem_limit_bytes=20 * 2**20),
    )(*args)


def on_device(rho_real, rho_imag, gate_real_matrix, gate_imaginary, angles, targets, gate_order):
    args = (rho_real, rho_imag, gate_real_matrix, gate_imaginary, angles.T, targets, gate_order)
    found = exchange_call(*(pltpu.with_memory_space_constraint(v, pltpu.HBM) for v in args))
    re, im, purity = rotate_call(*found)
    return re, im, purity.reshape(())


def solution(mesh):
    return jax.shard_map(
        on_device,
        mesh=mesh,
        in_specs=(P("row", "col"), P("row", "col"), P(), P(), P(), P(), P()),
        out_specs=(P("row", "col"), P("row", "col"), P()),
        check_vma=False,
    )
```

```python
import functools

import jax
import jax.numpy as jnp
from jax import lax
from jax.experimental import pallas as pl
from jax.experimental.pallas import tpu as pltpu
from jax.sharding import PartitionSpec as P

MESH = pl.DeviceIdType.MESH
HIGHEST = lax.Precision.HIGHEST
MIX = 0.25
KEEP = 1 - MIX
GATE = 16
LOW = 32
GATES = 8
BLOCK = (2, 8, 128)


def ring(v):
    v %= 8
    return min(v, 8 - v)


STEPS = [4, 3, -3, 2, -2, 1, -1, 0]
ORDER = [(d_, k_) for d_ in STEPS[:5] for k_ in (0, 1)] + [(d_, k_) for k_ in (0, 1) for d_ in (1, -1)] + [(0, 0), (0, 1)]
UNITS = [
    [(d_, k_) for d_, k_ in ORDER if ring(b_ - d_) >= ring(d_) + k_] for b_ in range(8)
]
BESIDE = {2: (1, 0), 3: (-1, 0)}
UNITS[0] = [u_ for u_ in UNITS[0] if u_ not in BESIDE.values()] + [None, None]
CHIPS = sorted(((jx, jy) for jx in range(4) for jy in range(4) if jx or jy), key=lambda j: (min(j[0], 4 - j[0]) + min(j[1], 4 - j[1]), j))
HOPS = lambda j: min(j[0], 4 - j[0]) + min(j[1], 4 - j[1])
OTHERS = sorted(((jx, jy, jc) for jx, jy in CHIPS for jc in range(2)), key=lambda j: (HOPS(j), j[2], j))
BETAS = [7, 1, 6, 2, 5, 3, 4, 0]
FORWARDS = [
    [(*UNITS[b_][u_], b_) for b_ in BETAS if UNITS[b_][u_] and UNITS[b_][u_][0] != 0] + ([(*BESIDE[u_], 0)] if u_ in BESIDE else [])
    for u_ in range(8)
]
SLOT = {f_: i_ for i_, f_ in enumerate(f_ for fs_ in FORWARDS[1:] for f_ in fs_)}
AHEAD = {1:[2,3],2:[4],3:[5,6],4:[7],5:[]}


def group(dz, kind):
    return 1 + kind if ring(dz) == 1 else 0


def wrap(v, n):
    return jnp.where(v >= n, v - n, v)


def near(v):
    return jnp.minimum(v, 8 - v)


def pick(index, values):
    out = jnp.int32(values[0])
    for i, value in enumerate(values):
        if value != values[0]:
            out = jnp.where(index == i, value, out)
    return out


def lanes(shape=(8, 128)):
    return lax.broadcasted_iota(jnp.int32, shape, 1)


def halve(a, b, mask, shift):
    turned = pltpu.roll(jnp.where(mask, b, a), shift, 1)
    return jnp.where(mask, a, turned), jnp.where(mask, turned, b)


def pack(src, dst, tmp, i):
    low = lanes() < 64
    even = (lanes() // 32) % 2 == 0
    groups = [(4 * i + n, part, q) for n in range(4) for part in range(2) for q in range(4)]
    for n, (h, part, q) in enumerate(groups):
        tiles = [src[part, 32 * h + 8 * k : 32 * h + 8 * k + 8, 128 * q : 128 * q + 128] for k in range(4)]
        for k in range(2):
            tmp[n, k], tmp[n, k + 2] = halve(tiles[k], tiles[k + 2], low, 64)
    for n, (h, part, q) in enumerate(groups):
        for m in range(2):
            at = 16 * h + 4 * q + 2 * m
            dst[at, part], dst[at + 1, part] = halve(tmp[n, 2 * m], tmp[n, 2 * m + 1], even, 32)


def unpack(ref, tmp, rows):
    low = lanes() < 64
    even = (lanes() // 32) % 2 == 0
    groups = [(g, part, q) for g in rows for part in range(2) for q in range(4)]
    for n, (g, part, q) in enumerate(groups):
        for m in range(2):
            tmp[n, m], tmp[n, m + 2] = halve(ref[g, 4 * q + m, part], ref[g, 4 * q + m + 2, part], low, 64)
    for n, (g, part, q) in enumerate(groups):
        for m in range(2):
            a, b = tmp[n, 2 * m], tmp[n, 2 * m + 1]
            ref[g, 4 * q + 2 * m, part] = jnp.where(even, a, pltpu.roll(b, 32, 1))
            ref[g, 4 * q + 2 * m + 1, part] = jnp.where(even, pltpu.roll(a, 96, 1), b)


def exchange_kernel(
    re_hbm, im_hbm, ure_hbm, uim_hbm, angles_hbm, targets_hbm, order_hbm, early_ref, late_ref, matrix_ref, sums_ref,
    own, turned, packed, mu, passing, f_ref, part_sums, plane_sums, small, angles, targets, order, factors, right1, right2, left, turned2, tmp,
    load_sem, small_sem, s1, ru, r1, r1z, s2, r2, sa, ra, sb, rb,
):
    r, c = lax.axis_index("row"), lax.axis_index("col")
    z, ylo = c // 2, c % 2
    rho, core = r // 2, r % 2
    x, y = rho % 4, (rho // 4) * 2 + ylo
    partner = r + 1 - 2 * core
    beta = wrap(rho + 8 - z, 8)
    cores = (core, 1 - core)
    ahead = [wrap(x + jx, 4) * 2 for jx in range(4)]
    behind = [wrap(x + 4 - jx, 4) for jx in range(4)]
    halves_of = lambda yy, top: (jnp.where(yy >= 2, top, 0), jnp.where(yy >= 2, yy - 2, yy))
    up = [halves_of(wrap(y + jy, 4), 8) for jy in range(4)]
    down = [halves_of(wrap(y + 4 - jy, 4), 4) for jy in range(4)]

    def others(fn):
        for j, (jx, jy, jc) in enumerate(OTHERS):
            fn(up[jy][0] + ahead[jx] + cores[jc], up[jy][1], j)

    def copy(src, dst, send, recv, row, col):
        return pltpu.make_async_remote_copy(src, dst, send, recv, device_id=(row, col), device_id_type=MESH)

    loads = [
        [
            pltpu.make_async_copy(ref.at[pl.ds(128 * i, 128)], own.at[part, pl.ds(128 * i, 128)], load_sem.at[part, i])
            for part, ref in ((0, re_hbm), (1, im_hbm))
        ]
        for i in range(4)
    ]
    barrier = pltpu.get_barrier_semaphore()

    def greet_plane(first, last):
        for j, (jx, jy, jc) in reversed(list(enumerate(OTHERS))):
            if first <= HOPS((jx, jy)) <= last:
                pl.semaphore_signal(
                    barrier, inc=1, device_id=(up[jy][0] + ahead[jx] + cores[jc], 2 * z + up[jy][1]), device_id_type=MESH
                )

    def greet_line(*steps):
        for k in steps:
            for h in (r, partner):
                pl.semaphore_signal(barrier, inc=1, device_id=(h, 2 * wrap(z + k, 8) + ylo), device_id_type=MESH)

    for pair in loads:
        for load in pair:
            load.start()
    greet_plane(4, 4)
    greet_line(4)
    greet_plane(3, 3)
    greet_line(3, 5)
    greet_plane(2, 2)
    greet_line(2, 6)
    greet_plane(1, 1)
    greet_line(1, 7)
    pl.semaphore_signal(barrier, inc=1, device_id=(partner, 2 * z + ylo), device_id_type=MESH)
    smalls = [
        pltpu.make_async_copy(ref, dst, small_sem.at[i])
        for i, (ref, dst) in enumerate(
            (
                (ure_hbm, small.at[0]),
                (uim_hbm, small.at[1]),
                (angles_hbm, angles),
                (targets_hbm, targets),
                (order_hbm, order),
            )
        )
    ]
    for load in smalls:
        load.start()
    for i, pair in enumerate(loads):
        for load in pair:
            load.wait()
        pack(own, packed.at[0], tmp, i)

    pl.semaphore_wait(barrier, 45)

    def at_step(dz):
        zz = wrap(z + dz % 8, 8)
        b = wrap(rho + 8 - zz, 8)
        return zz, b, near(b) >= ring(dz), near(b) > ring(dz)

    def straight(kind):
        for dz in STEPS[:-1]:
            zz, b, direct, also = at_step(dz)
            if kind == 1 and ring(dz) == 4:
                continue
            a = (-dz) % 8

            @pl.when(also if kind else direct)
            def _():
                for h in (r, partner):
                    copy(
                        packed.at[kind, 16 * h + 2 * zz + ylo],
                        f_ref.at[2 * a + ylo, 2 * b + core] if kind else f_ref.at[2 * b + core, 2 * a + ylo],
                        s2,
                        r2.at[group(dz, kind)],
                        h,
                        2 * zz + ylo,
                    ).start()

    def send_unit(u):
        unit = [UNITS[b][u] or (0, 0) for b in range(8)]
        dz = pick(beta, [d % 8 for d, _ in unit])
        kind = pick(beta, [k for _, k in unit])
        zz = wrap(z + dz, 8)
        b = wrap(beta + 8 - dz, 8)
        first, second = jnp.where(kind == 0, core, ylo), jnp.where(kind == 0, ylo, core)
        if u == 0:
            others(lambda h, p, j: copy(packed.at[0, 16 * h + 2 * zz + p], mu.at[j], s1, ru.at[j], h, 2 * z + p).start())
            return

        def passed():
            row = 112 * kind + 16 * pick(beta, [STEPS.index(d) % 7 for d, _ in unit]) + 2 * b + first
            sem = r1.at[pick(beta, [SLOT.get((*unit[bb], bb), 0) for bb in range(8)])]
            others(lambda h, p, j: copy(packed.at[kind, 16 * h + 2 * zz + p], passing.at[row, second], s1, sem, h, 2 * z + p).start())

        def kept():
            row, col = jnp.where(kind == 0, 2 * b + core, ylo), jnp.where(kind == 0, ylo, 2 * b + core)

            def send(h, p, j):
                copy(packed.at[kind, 16 * h + 2 * zz + p], f_ref.at[row, col], s1, r1z, h, 2 * z + p).start()

            others(send)
            send(partner, ylo, 0)
            f_ref[row, col] = packed[kind, 16 * r + 2 * zz + ylo]

        here = [UNITS[bb][u] is not None and UNITS[bb][u][0] == 0 for bb in range(8)]
        away = [UNITS[bb][u] is not None and UNITS[bb][u][0] != 0 for bb in range(8)]
        for which, action in ((away, passed), (here, kept)):
            if all(which):
                action()
            elif any(which):
                pl.when(pick(beta, [int(v) for v in which]) == 1)(action)

        if u in BESIDE:

            @pl.when(beta == 0)
            def _():
                d, k = BESIDE[u]
                zb = wrap(z + d % 8, 8)
                row = 112 * k + 16 * STEPS.index(d) + 2 * (-d % 8) + core
                others(
                    lambda h, p, j: copy(
                        packed.at[k, 16 * h + 2 * zb + p], passing.at[row, ylo], s1, r1.at[SLOT[d, k, 0]], h, 2 * z + p
                    ).start()
                )

    send_unit(0)
    straight(0)
    for i in range(4):
        rows = pl.ds(128 * i, 128)
        for j in range(4):
            there = pl.ds(128 * j, 128)
            turned[0, there, rows] = own[0, rows, there].T
            turned[1, there, rows] = -own[1, rows, there].T
    for i in range(4):
        pack(turned, packed.at[1], tmp, i)
    straight(1)

    def arrived(sem, count):
        copy(packed.at[0, pl.ds(0, count)], packed.at[1, pl.ds(0, count)], sem, sem, r, c).wait_recv()

    def left_all(sem, count):
        copy(packed.at[0, pl.ds(0, count)], packed.at[1, pl.ds(0, count)], sem, sem, r, c).wait_send()

    def either(condition, wait, sem, counts):
        @pl.when(condition)
        def _():
            wait(sem, counts[0])

        @pl.when(jnp.logical_not(condition))
        def _():
            wait(sem, counts[1])

    def share_sums():
        def squares(i, accs):
            for n in range(2):
                rows = pl.ds(pl.multiple_of(16 * i + 8 * n, 8), 8)
                tiles = [own[part, rows, pl.ds(128 * q, 128)] for part in range(2) for q in range(4)]
                accs = [acc + v * v for acc, v in zip(accs, tiles)]
            return accs

        total = jnp.sum(sum(lax.fori_loop(0, 32, squares, [jnp.zeros((8, 128), jnp.float32)] * 8)))
        on_diagonal = lanes((128, 128)) == lax.broadcasted_iota(jnp.int32, (128, 128), 0)
        traces = []
        for part in range(2):
            v = sum(own[part, pl.ds(128 * q, 128), pl.ds(128 * q, 128)] for q in range(4))
            traces.append(jnp.where(r == c, jnp.sum(jnp.where(on_diagonal, v, 0.0)), 0.0))
        lane = lanes((1, 128))
        place = (y * 4 + x) * 2 + core
        part_sums[place] = jnp.where(lane == 0, total, jnp.where(lane == 1, traces[0], jnp.where(lane == 2, traces[1], 0.0)))

        def share(h, p, j):
            copy(part_sums.at[place], part_sums.at[place], sa, ra, h, 2 * z + p).start()

        others(share)
        share(partner, ylo, 0)

    def pass_on():
        for j, (jx, jy, jc) in enumerate(OTHERS):
            if j == 8:
                send_unit(1)
            bs = wrap(wrap(down[jy][0] + behind[jx] + 8 - z, 8), 8)
            dz = pick(bs, [UNITS[b][0][0] % 8 for b in range(8)])
            a, b = wrap(8 - dz, 8), wrap(bs + 8 - dz, 8)
            copy(mu.at[j], mu.at[j], s1, ru.at[j], r, c).wait_recv()
            dst = f_ref.at[2 * b + cores[jc], 2 * a + down[jy][1]]
            copy(mu.at[j], dst, s2, r2.at[0], r, 2 * wrap(z + dz, 8) + ylo).start()

    def forward(u):
        for dz, kind, bb in FORWARDS[u]:
            n = SLOT[dz, kind, bb]
            a, b = (-dz) % 8, (bb - dz) % 8
            row = 112 * kind + 16 * (STEPS.index(dz) % 7) + 2 * b
            mine = beta == bb

            def onward(full):
                if kind == 0:
                    first, second = (0, 2), (0, 2) if full else (1 - ylo, 1)
                else:
                    first, second = (0, 2) if full else (1 - ylo, 1), (0, 2)
                src = passing.at[pl.ds(row + first[0], first[1]), pl.ds(*second)]
                at = (2 * b, 2 * a) if kind == 0 else (2 * a, 2 * b)
                dst = f_ref.at[pl.ds(at[0] + first[0], first[1]), pl.ds(at[1] + second[0], second[1])]
                copy(src, dst, s2, r2.at[group(dz, kind)], r, 2 * wrap(z + dz % 8, 8) + ylo).start()

            @pl.when(mine)
            def _():
                arrived(r1.at[n], 2)
                onward(False)

            @pl.when(jnp.logical_not(mine))
            def _():
                arrived(r1.at[n], 4)
                onward(True)

    pass_on()
    for load in smalls:
        load.wait()
    for u in range(1, 6):
        for following in AHEAD[u]:
            send_unit(following)
        if u == 2:
            factors[...] = gate_factors(angles[...], targets, order)
        if u == 3:
            share_sums()
        if u == 4:
            prepare_lanes(ylo, factors[...], right1)
        if u == 5:
            prepare_rows(z, factors[...], small, right2, left, matrix_ref)
        forward(u)

    copy(part_sums.at[pl.ds(0, 31)], part_sums.at[pl.ds(0, 31)], sa, ra, r, c).wait_recv()
    plane_sums[z] = jnp.sum(part_sums[...], axis=0)
    for k in range(1, 8):
        copy(plane_sums.at[z], plane_sums.at[z], sb, rb, r, 2 * wrap(z + k, 8) + ylo).start()

    def over_g2(g, out):
        v = jnp.concatenate([f_ref[g + n].reshape(256, 128) for n in range(2)], axis=1)
        v = dot3((right2[0], right2[1]), halves(v))
        for n in range(2):
            out[n] = v[:, 128 * n : 128 * n + 128].reshape((16,) + BLOCK)

    either(beta == 0, arrived, r1z, (59, 58))
    on_lanes(f_ref, right1, 0, 2, 0, 16)
    on_lanes(f_ref, right1, 2, 14, 0, 2)
    turned2[pl.ds(2, 2)] = jnp.zeros((2, 16) + BLOCK, jnp.float32)
    turned2[pl.ds(14, 2)] = jnp.zeros((2, 16) + BLOCK, jnp.float32)
    arrived(r2.at[0], 100)
    for n in range(5):
        on_lanes(f_ref, right1, 4 + 2 * n, 2, 4, 10)
    arrived(r2.at[1], 56)
    on_lanes(f_ref, right1, 2, 14, 2, 2)
    on_lanes(f_ref, right1, 2, 14, 14, 2)
    for g in (0, 4, 6, 8, 10, 12):
        over_g2(g, turned2.at[pl.ds(g, 2)])
    for rows in ((0, 1, 4, 5), (6, 7, 8, 9), (10, 11, 12, 13)):
        unpack(turned2, tmp, rows)
    for n in range(8):
        v = jnp.concatenate([turned2[:, 2 * n + m].reshape(256, 128) for m in range(2)], axis=1)
        early_ref[n // 2, :, 256 * (n % 2) : 256 * (n % 2) + 256] = dot3((left[0], left[1]), halves(v))
    either(beta == 0, left_all, s1, (241, 242))
    left_all(s2, 196)
    copy(plane_sums.at[pl.ds(0, 7)], plane_sums.at[pl.ds(0, 7)], sb, rb, r, c).wait()
    copy(part_sums.at[pl.ds(0, 31)], part_sums.at[pl.ds(0, 31)], sa, ra, r, c).wait_send()
    sums_ref[...] = jnp.sum(plane_sums[...], axis=0)
    arrived(r2.at[2], 40)
    on_lanes(f_ref, right1, 2, 2, 4, 10)
    on_lanes(f_ref, right1, 14, 2, 4, 10)
    over_g2(2, late_ref.at[pl.ds(0, 2)])
    over_g2(14, late_ref.at[pl.ds(2, 2)])
    unpack(late_ref, tmp, range(4))


def exchange_call(*args):
    f32, bf16 = jnp.float32, jnp.bfloat16
    dma = pltpu.SemaphoreType.DMA
    vmem, hbm = pl.BlockSpec(memory_space=pltpu.VMEM), pl.BlockSpec(memory_space=pltpu.HBM)
    blocks = lambda *n: pltpu.VMEM(n + BLOCK, f32)
    return pl.pallas_call(
        exchange_kernel,
        name="exchange",
        out_shape=(
            jax.ShapeDtypeStruct((4, 256, 512), f32),
            jax.ShapeDtypeStruct((4, 16) + BLOCK, f32),
            jax.ShapeDtypeStruct((256, 256), bf16),
            jax.ShapeDtypeStruct((1, 128), f32),
        ),
        in_specs=[hbm] * 7,
        out_specs=(vmem, vmem, vmem, vmem),
        scratch_shapes=[
            pltpu.VMEM((2, 512, 512), f32),
            pltpu.VMEM((2, 512, 512), f32),
            blocks(2, 256),
            blocks(32),
            blocks(224, 2),
            blocks(16, 16),
            pltpu.VMEM((32, 1, 128), f32),
            pltpu.VMEM((8, 1, 128), f32),
            pltpu.VMEM((2, 16, 16), f32),
            pltpu.VMEM((3, 8), f32),
            pltpu.SMEM((8,), jnp.int32),
            pltpu.SMEM((8,), jnp.int32),
            pltpu.VMEM((32, 8), f32),
            pltpu.VMEM((2, 256, 256), bf16),
            pltpu.VMEM((2, 256, 256), bf16),
            pltpu.VMEM((2, 256, 256), bf16),
            blocks(16, 16),
            pltpu.VMEM((32, 4, 8, 128), f32),
            dma((2, 4)),
            dma((5,)),
            dma,
            dma((32,)),
            dma((len(SLOT),)),
            dma,
            dma,
            dma((3,)),
            dma,
            dma,
            dma,
            dma,
        ],
        compiler_params=pltpu.CompilerParams(collective_id=0, has_side_effects=True, vmem_limit_bytes=40 * 2**20),
    )(*args)


def iota2(n, m, dim):
    return lax.broadcasted_iota(jnp.int32, (n, m), dim)


def halves(v):
    hi = v.astype(jnp.bfloat16)
    return hi, (v - hi.astype(jnp.float32)).astype(jnp.bfloat16)


def dot(a, b):
    return jnp.dot(a, b, preferred_element_type=jnp.float32)


def dot3(a, b):
    return dot(a[0], b[0]) + dot(a[0], b[1]) + dot(a[1], b[0])


def gate_factors(angles, targets, order):
    theta, alpha, beta = angles[0:1], angles[1:2], angles[2:3]
    cos, sin = jnp.cos(theta / 2), jnp.sin(theta / 2)
    both = alpha + beta
    elements = (
        (cos, cos * 0.0),
        (-jnp.cos(beta) * sin, -jnp.sin(beta) * sin),
        (jnp.cos(alpha) * sin, jnp.sin(alpha) * sin),
        (jnp.cos(both) * cos, jnp.sin(both) * cos),
    )
    i, j = iota2(32, 32, 0), iota2(32, 32, 1)
    left, right, high = i % 8, j % 8, i >= 16
    same_part, lower, same_factor = (i // 8) % 2 == (j // 8) % 2, i > j, i // 16 == j // 16
    gates = lax.broadcasted_iota(jnp.int32, (1, GATES), 1)
    total = jnp.where((iota2(32, 8, 0) % 16) == iota2(32, 8, 1), 1.0, 0.0)
    for position in range(GATES):
        gate = order[position]
        target = targets[gate]
        low_bit = jnp.where(target == 0, 1, jnp.where(target == 1, 2, jnp.where(target == 2, 4, 0)))
        high_bit = jnp.where(target == 3, 1, jnp.where(target == 4, 2, 0))
        bit = jnp.where(high, high_bit, low_bit)
        entry = [
            [jnp.sum(jnp.where(gates == gate, e, 0.0), axis=1, keepdims=True) for e in pair] for pair in elements
        ]
        left_high, right_high = (left & bit) > 0, (right & bit) > 0
        same_rest = ((left ^ right) | bit) == bit
        step = [
            jnp.where(
                left_high,
                jnp.where(right_high, entry[3][part], entry[2][part]),
                jnp.where(right_high, entry[1][part], entry[0][part]),
            )
            for part in range(2)
        ]
        step = [jnp.where(bit > 0, v, one) for v, one in zip(step, (1.0, 0.0))]
        step = jnp.where(same_part, step[0], jnp.where(lower, step[1], -step[1]))
        step = jnp.where(same_rest & same_factor, step, 0.0)
        total = jnp.dot(step, total, precision=HIGHEST, preferred_element_type=jnp.float32)
    return total


def one_hot(n, m, index):
    return jnp.where(index == iota2(n, m, 1), 1.0, 0.0)


def spread(rows, small, cols):
    wide = jnp.dot(rows, small, precision=HIGHEST, preferred_element_type=jnp.float32)
    return lax.dot_general(wide, cols, (((1,), (1,)), ((), ())), precision=HIGHEST, preferred_element_type=jnp.float32)


def times(a, b):
    return a[0] * b[0] - a[1] * b[1], a[0] * b[1] + a[1] * b[0]


def store_halves(ref, v):
    hi, lo = halves(v)
    ref[0] = hi
    ref[1] = lo


def of(factors, which):
    return [factors[16 * which + 8 * part : 16 * which + 8 * part + 8] for part in range(2)]


def by_row(n):
    return iota2(256, n, 0)


def prepare_lanes(ylo, factors, right1):
    i, j = iota2(256, 256, 0), iota2(256, 256, 1)
    low, high = of(factors, 0), of(factors, 1)
    k = (by_row(8) // 32) % 4
    on_k = one_hot(256, 8, k)
    from_k = one_hot(256, 8, jnp.where((ylo == 1) & (k % 2 == 0), 2 - k, k))
    on_top = one_hot(256, 8, (by_row(8) // 8) % 4)
    on_s = one_hot(256, 8, by_row(8) % 8)
    turn = lambda hot, m, to: spread(hot, m.T, to)
    a = [turn(from_k, m, on_k) for m in high]
    b = times([turn(on_top, m, on_top) for m in high], [turn(on_s, m, on_s) for m in low])
    value = times(a, (b[0], -b[1]))
    same, lower = i // 128 == j // 128, i > j
    store_halves(right1, jnp.where(same, value[0], jnp.where(lower, -value[1], value[1])))


def prepare_rows(z, factors, small, right2, left, late_ref):
    i, j = iota2(256, 256, 0), iota2(256, 256, 1)
    low = of(factors, 0)
    out_g = one_hot(256, 16, by_row(16) // 16)
    in_g = one_hot(256, 16, (by_row(16) // 16 + 2 * z) % 16)
    u = [spread(out_g, small[part], in_g) for part in range(2)]
    same, lower = (i // 8) % 2 == (j // 8) % 2, (i // 8) % 2 > (j // 8) % 2
    value = jnp.where(same, u[0], jnp.where(lower, -u[1], u[1]))
    store_halves(right2, jnp.where(i % 8 == j % 8, value, 0.0))
    on_s = one_hot(256, 8, by_row(8) % 8)
    low = [spread(on_s, m, on_s) for m in low]
    real = lambda value: KEEP * jnp.where(same, value[0], jnp.where(lower, value[1], -value[1]))
    store_halves(left, real(times(u, low)))
    n = (by_row(16) // 16) % 4
    in_g = one_hot(256, 16, (n + jnp.where(n < 2, 2, 12) + 2 * z) % 16)
    u = [spread(out_g, small[part], in_g) for part in range(2)]
    hi, lo = (v.astype(jnp.float32) for v in halves(real(times(u, low))))
    segment = j // 64
    late_ref[...] = jnp.where(segment == 3, 0.0, jnp.where(segment == 1, lo, hi)).astype(jnp.bfloat16)


def on_lanes(f_ref, right1, g, n, g2, n2):
    here = (pl.ds(g, n), pl.ds(g2, n2))
    v = jnp.concatenate([f_ref[(*here, part)].reshape(n * n2 * 8, 128) for part in range(2)], axis=1)
    v = dot3(halves(v), (right1[0], right1[1]))
    for part in range(2):
        f_ref[(*here, part)] = v[:, 128 * part : 128 * part + 128].reshape(n, n2, 8, 128)


def rotate_kernel(early_ref, late_ref, matrix_ref, sums_ref, re_ref, im_ref, purity_ref, purity, stage, product, sem, purity_sem):
    r, c = lax.axis_index("row"), lax.axis_index("col")
    sums = sums_ref[...]
    lane = lanes((1, 128))
    total, trace_re, trace_im = (jnp.sum(jnp.where(lane == n, sums, 0.0)) for n in range(3))
    dim = GATE * GATE * LOW
    shifts = (jnp.where(r == c, MIX * trace_re / dim, 0.0), jnp.where(r == c, MIX * trace_im / dim, 0.0))
    squared = trace_re * trace_re + trace_im * trace_im
    purity[0, 0] = (KEEP * KEEP * total + (2 * KEEP * MIX + MIX * MIX) * squared / dim) / (dim * dim)
    matrix = matrix_ref[...]
    sublane = lax.broadcasted_iota(jnp.int32, (8, 128), 0)
    v = jnp.concatenate([late_ref[:, n].reshape(64, 128) for n in range(16)], axis=1)
    hi, lo = halves(v)
    product[...] = dot(matrix, jnp.concatenate([hi, hi, lo, jnp.zeros_like(hi)], axis=0))
    copies = [pltpu.make_async_copy(purity, purity_ref, purity_sem)]
    copies[0].start()
    for q in range(4):
        for g in range(16):
            for part in range(2):
                for k in range(4):
                    row, col = 16 * g + 8 * part, 128 * k
                    tile = early_ref[q, row : row + 8, col : col + 128]
                    tile = tile + product[row : row + 8, 512 * q + col : 512 * q + col + 128]
                    if g // 4 == q:
                        tile = tile + jnp.where(lanes() == sublane + (32 * (g % 4) + 8 * k), shifts[part], 0.0)
                    stage[part, q, 32 * g + 8 * k : 32 * g + 8 * k + 8] = tile
        for part, ref in ((0, re_ref), (1, im_ref)):
            copies.append(pltpu.make_async_copy(stage.at[part, q], ref.at[:, pl.ds(128 * q, 128)], sem.at[part, q]))
            copies[-1].start()
    for copy in copies:
        copy.wait()


def rotate_call(*args):
    f32 = jnp.float32
    vmem, hbm = pl.BlockSpec(memory_space=pltpu.VMEM), pl.BlockSpec(memory_space=pltpu.HBM)
    return pl.pallas_call(
        rotate_kernel,
        name="rotate",
        out_shape=(
            jax.ShapeDtypeStruct((512, 512), f32),
            jax.ShapeDtypeStruct((512, 512), f32),
            jax.ShapeDtypeStruct((1, 1), f32),
        ),
        in_specs=[vmem] * 4,
        out_specs=(hbm, hbm, hbm),
        scratch_shapes=[
            pltpu.SMEM((1, 1), f32),
            pltpu.VMEM((2, 4, 512, 128), f32),
            pltpu.VMEM((256, 2048), f32),
            pltpu.SemaphoreType.DMA((2, 4)),
            pltpu.SemaphoreType.DMA,
        ],
        compiler_params=pltpu.CompilerParams(vmem_limit_bytes=20 * 2**20),
    )(*args)


def on_device(rho_real, rho_imag, gate_real_matrix, gate_imaginary, angles, targets, gate_order):
    args = (rho_real, rho_imag, gate_real_matrix, gate_imaginary, angles.T, targets, gate_order)
    found = exchange_call(*(pltpu.with_memory_space_constraint(v, pltpu.HBM) for v in args))
    re, im, purity = rotate_call(*found)
    return re, im, purity.reshape(())


def solution(mesh):
    return jax.shard_map(
        on_device,
        mesh=mesh,
        in_specs=(P("row", "col"), P("row", "col"), P(), P(), P(), P(), P()),
        out_specs=(P("row", "col"), P("row", "col"), P()),
        check_vma=False,
    )
```

```python
import functools

import jax
import jax.numpy as jnp
from jax import lax
from jax.experimental import pallas as pl
from jax.experimental.pallas import tpu as pltpu
from jax.sharding import PartitionSpec as P

MESH = pl.DeviceIdType.MESH
HIGHEST = lax.Precision.HIGHEST
MIX = 0.25
KEEP = 1 - MIX
GATE = 16
LOW = 32
GATES = 8
BLOCK = (2, 8, 128)


def ring(v):
    v %= 8
    return min(v, 8 - v)


STEPS = [4, 3, -3, 2, -2, 1, -1, 0]
ORDER = [(d_, k_) for d_ in STEPS[:5] for k_ in (0, 1)] + [(d_, k_) for k_ in (0, 1) for d_ in (1, -1)] + [(0, 0), (0, 1)]
UNITS = [
    [(d_, k_) for d_, k_ in ORDER if ring(b_ - d_) >= ring(d_) + k_] for b_ in range(8)
]
BESIDE = {2: (1, 0), 3: (-1, 0)}
UNITS[0] = [u_ for u_ in UNITS[0] if u_ not in BESIDE.values()] + [None, None]
CHIPS = sorted(((jx, jy) for jx in range(4) for jy in range(4) if jx or jy), key=lambda j: (min(j[0], 4 - j[0]) + min(j[1], 4 - j[1]), j))
HOPS = lambda j: min(j[0], 4 - j[0]) + min(j[1], 4 - j[1])
OTHERS = sorted(((jx, jy, jc) for jx, jy in CHIPS for jc in range(2)), key=lambda j: (HOPS(j), j[2], j))
BETAS = [7, 1, 6, 2, 5, 3, 4, 0]
FORWARDS = [
    [(*UNITS[b_][u_], b_) for b_ in BETAS if UNITS[b_][u_] and UNITS[b_][u_][0] != 0] + ([(*BESIDE[u_], 0)] if u_ in BESIDE else [])
    for u_ in range(8)
]
SLOT = {f_: i_ for i_, f_ in enumerate(f_ for fs_ in FORWARDS[1:] for f_ in fs_)}
AHEAD = {1:[2,3],2:[4],3:[5,6],4:[7],5:[]}


def group(dz, kind):
    return 1 + kind if ring(dz) == 1 else 0


def wrap(v, n):
    return jnp.where(v >= n, v - n, v)


def near(v):
    return jnp.minimum(v, 8 - v)


def pick(index, values):
    out = jnp.int32(values[0])
    for i, value in enumerate(values):
        if value != values[0]:
            out = jnp.where(index == i, value, out)
    return out


def lanes(shape=(8, 128)):
    return lax.broadcasted_iota(jnp.int32, shape, 1)


def halve(a, b, mask, shift):
    turned = pltpu.roll(jnp.where(mask, b, a), shift, 1)
    return jnp.where(mask, a, turned), jnp.where(mask, turned, b)


def pack(src, dst, tmp, i):
    low = lanes() < 64
    even = (lanes() // 32) % 2 == 0
    groups = [(4 * i + n, part, q) for n in range(4) for part in range(2) for q in range(4)]
    for n, (h, part, q) in enumerate(groups):
        tiles = [src[part, 32 * h + 8 * k : 32 * h + 8 * k + 8, 128 * q : 128 * q + 128] for k in range(4)]
        for k in range(2):
            tmp[n, k], tmp[n, k + 2] = halve(tiles[k], tiles[k + 2], low, 64)
    for n, (h, part, q) in enumerate(groups):
        for m in range(2):
            at = 16 * h + 4 * q + 2 * m
            dst[at, part], dst[at + 1, part] = halve(tmp[n, 2 * m], tmp[n, 2 * m + 1], even, 32)


def unpack(ref, tmp, rows):
    low = lanes() < 64
    even = (lanes() // 32) % 2 == 0
    groups = [(g, part, q) for g in rows for part in range(2) for q in range(4)]
    for n, (g, part, q) in enumerate(groups):
        for m in range(2):
            tmp[n, m], tmp[n, m + 2] = halve(ref[g, 4 * q + m, part], ref[g, 4 * q + m + 2, part], low, 64)
    for n, (g, part, q) in enumerate(groups):
        for m in range(2):
            a, b = tmp[n, 2 * m], tmp[n, 2 * m + 1]
            ref[g, 4 * q + 2 * m, part] = jnp.where(even, a, pltpu.roll(b, 32, 1))
            ref[g, 4 * q + 2 * m + 1, part] = jnp.where(even, pltpu.roll(a, 96, 1), b)


def exchange_kernel(
    re_hbm, im_hbm, ure_hbm, uim_hbm, angles_hbm, targets_hbm, order_hbm, early_ref, late_ref, matrix_ref, sums_ref,
    own, turned, packed, mu, passing, f_ref, part_sums, plane_sums, small, angles, targets, order, factors, right1, right2, left, turned2, tmp,
    load_sem, small_sem, s1, ru, r1, r1z, s2, r2, sa, ra, sb, rb,
):
    r, c = lax.axis_index("row"), lax.axis_index("col")
    z, ylo = c // 2, c % 2
    rho, core = r // 2, r % 2
    x, y = rho % 4, (rho // 4) * 2 + ylo
    partner = r + 1 - 2 * core
    beta = wrap(rho + 8 - z, 8)
    cores = (core, 1 - core)
    ahead = [wrap(x + jx, 4) * 2 for jx in range(4)]
    behind = [wrap(x + 4 - jx, 4) for jx in range(4)]
    halves_of = lambda yy, top: (jnp.where(yy >= 2, top, 0), jnp.where(yy >= 2, yy - 2, yy))
    up = [halves_of(wrap(y + jy, 4), 8) for jy in range(4)]
    down = [halves_of(wrap(y + 4 - jy, 4), 4) for jy in range(4)]

    def others(fn):
        for j, (jx, jy, jc) in enumerate(OTHERS):
            fn(up[jy][0] + ahead[jx] + 1 - jc, up[jy][1], jnp.where(core == 1, OTHERS.index((jx, jy, 0)), OTHERS.index((jx, jy, 1))))

    def copy(src, dst, send, recv, row, col):
        return pltpu.make_async_remote_copy(src, dst, send, recv, device_id=(row, col), device_id_type=MESH)

    loads = [
        [
            pltpu.make_async_copy(ref.at[pl.ds(128 * i, 128)], own.at[part, pl.ds(128 * i, 128)], load_sem.at[part, i])
            for part, ref in ((0, re_hbm), (1, im_hbm))
        ]
        for i in range(4)
    ]
    barrier = pltpu.get_barrier_semaphore()

    def greet_plane(first, last):
        for j, (jx, jy, jc) in reversed(list(enumerate(OTHERS))):
            if first <= HOPS((jx, jy)) <= last:
                pl.semaphore_signal(
                    barrier, inc=1, device_id=(up[jy][0] + ahead[jx] + cores[jc], 2 * z + up[jy][1]), device_id_type=MESH
                )

    def greet_line(*steps):
        for k in steps:
            for h in (r, partner):
                pl.semaphore_signal(barrier, inc=1, device_id=(h, 2 * wrap(z + k, 8) + ylo), device_id_type=MESH)

    for pair in loads:
        for load in pair:
            load.start()
    greet_plane(4, 4)
    greet_line(4)
    greet_plane(3, 3)
    greet_line(3, 5)
    greet_plane(2, 2)
    greet_line(2, 6)
    greet_plane(1, 1)
    greet_line(1, 7)
    pl.semaphore_signal(barrier, inc=1, device_id=(partner, 2 * z + ylo), device_id_type=MESH)
    smalls = [
        pltpu.make_async_copy(ref, dst, small_sem.at[i])
        for i, (ref, dst) in enumerate(
            (
                (ure_hbm, small.at[0]),
                (uim_hbm, small.at[1]),
                (angles_hbm, angles),
                (targets_hbm, targets),
                (order_hbm, order),
            )
        )
    ]
    for load in smalls:
        load.start()
    for i, pair in enumerate(loads):
        for load in pair:
            load.wait()
        pack(own, packed.at[0], tmp, i)

    pl.semaphore_wait(barrier, 45)

    def at_step(dz):
        zz = wrap(z + dz % 8, 8)
        b = wrap(rho + 8 - zz, 8)
        return zz, b, near(b) >= ring(dz), near(b) > ring(dz)

    def straight(kind):
        for dz in STEPS[:-1]:
            zz, b, direct, also = at_step(dz)
            if kind == 1 and ring(dz) == 4:
                continue
            a = (-dz) % 8

            @pl.when(also if kind else direct)
            def _():
                for h in (r, partner):
                    copy(
                        packed.at[kind, 16 * h + 2 * zz + ylo],
                        f_ref.at[2 * a + ylo, 2 * b + core] if kind else f_ref.at[2 * b + core, 2 * a + ylo],
                        s2,
                        r2.at[group(dz, kind)],
                        h,
                        2 * zz + ylo,
                    ).start()

    def send_unit(u):
        unit = [UNITS[b][u] or (0, 0) for b in range(8)]
        dz = pick(beta, [d % 8 for d, _ in unit])
        kind = pick(beta, [k for _, k in unit])
        zz = wrap(z + dz, 8)
        b = wrap(beta + 8 - dz, 8)
        first, second = jnp.where(kind == 0, core, ylo), jnp.where(kind == 0, ylo, core)
        if u == 0:
            others(lambda h, p, j: copy(packed.at[0, 16 * h + 2 * zz + p], mu.at[j], s1, ru.at[j], h, 2 * z + p).start())
            return

        def passed():
            row = 112 * kind + 16 * pick(beta, [STEPS.index(d) % 7 for d, _ in unit]) + 2 * b + first
            sem = r1.at[pick(beta, [SLOT.get((*unit[bb], bb), 0) for bb in range(8)])]
            others(lambda h, p, j: copy(packed.at[kind, 16 * h + 2 * zz + p], passing.at[row, second], s1, sem, h, 2 * z + p).start())

        def kept():
            row, col = jnp.where(kind == 0, 2 * b + core, ylo), jnp.where(kind == 0, ylo, 2 * b + core)

            def send(h, p, j):
                copy(packed.at[kind, 16 * h + 2 * zz + p], f_ref.at[row, col], s1, r1z, h, 2 * z + p).start()

            others(send)
            send(partner, ylo, 0)
            f_ref[row, col] = packed[kind, 16 * r + 2 * zz + ylo]

        here = [UNITS[bb][u] is not None and UNITS[bb][u][0] == 0 for bb in range(8)]
        away = [UNITS[bb][u] is not None and UNITS[bb][u][0] != 0 for bb in range(8)]
        for which, action in ((away, passed), (here, kept)):
            if all(which):
                action()
            elif any(which):
                pl.when(pick(beta, [int(v) for v in which]) == 1)(action)

        if u in BESIDE:

            @pl.when(beta == 0)
            def _():
                d, k = BESIDE[u]
                zb = wrap(z + d % 8, 8)
                row = 112 * k + 16 * STEPS.index(d) + 2 * (-d % 8) + core
                others(
                    lambda h, p, j: copy(
                        packed.at[k, 16 * h + 2 * zb + p], passing.at[row, ylo], s1, r1.at[SLOT[d, k, 0]], h, 2 * z + p
                    ).start()
                )

    send_unit(0)
    straight(0)
    for i in range(4):
        rows = pl.ds(128 * i, 128)
        for j in range(4):
            there = pl.ds(128 * j, 128)
            turned[0, there, rows] = own[0, rows, there].T
            turned[1, there, rows] = -own[1, rows, there].T
    for i in range(4):
        pack(turned, packed.at[1], tmp, i)
    straight(1)

    def arrived(sem, count):
        copy(packed.at[0, pl.ds(0, count)], packed.at[1, pl.ds(0, count)], sem, sem, r, c).wait_recv()

    def left_all(sem, count):
        copy(packed.at[0, pl.ds(0, count)], packed.at[1, pl.ds(0, count)], sem, sem, r, c).wait_send()

    def either(condition, wait, sem, counts):
        @pl.when(condition)
        def _():
            wait(sem, counts[0])

        @pl.when(jnp.logical_not(condition))
        def _():
            wait(sem, counts[1])

    def share_sums():
        def squares(i, accs):
            for n in range(2):
                rows = pl.ds(pl.multiple_of(16 * i + 8 * n, 8), 8)
                tiles = [own[part, rows, pl.ds(128 * q, 128)] for part in range(2) for q in range(4)]
                accs = [acc + v * v for acc, v in zip(accs, tiles)]
            return accs

        total = jnp.sum(sum(lax.fori_loop(0, 32, squares, [jnp.zeros((8, 128), jnp.float32)] * 8)))
        on_diagonal = lanes((128, 128)) == lax.broadcasted_iota(jnp.int32, (128, 128), 0)
        traces = []
        for part in range(2):
            v = sum(own[part, pl.ds(128 * q, 128), pl.ds(128 * q, 128)] for q in range(4))
            traces.append(jnp.where(r == c, jnp.sum(jnp.where(on_diagonal, v, 0.0)), 0.0))
        lane = lanes((1, 128))
        place = (y * 4 + x) * 2 + core
        part_sums[place] = jnp.where(lane == 0, total, jnp.where(lane == 1, traces[0], jnp.where(lane == 2, traces[1], 0.0)))

        def share(h, p, j):
            copy(part_sums.at[place], part_sums.at[place], sa, ra, h, 2 * z + p).start()

        others(share)
        share(partner, ylo, 0)

    def pass_on():
        for j, (jx, jy, jc) in enumerate(OTHERS):
            if j == 4:
                send_unit(1)
            bs = wrap(wrap(down[jy][0] + behind[jx] + 8 - z, 8), 8)
            dz = pick(bs, [UNITS[b][0][0] % 8 for b in range(8)])
            a, b = wrap(8 - dz, 8), wrap(bs + 8 - dz, 8)
            copy(mu.at[j], mu.at[j], s1, ru.at[j], r, c).wait_recv()
            dst = f_ref.at[2 * b + 1 - jc, 2 * a + down[jy][1]]
            copy(mu.at[j], dst, s2, r2.at[0], r, 2 * wrap(z + dz, 8) + ylo).start()

    def forward(u):
        for dz, kind, bb in FORWARDS[u]:
            n = SLOT[dz, kind, bb]
            a, b = (-dz) % 8, (bb - dz) % 8
            row = 112 * kind + 16 * (STEPS.index(dz) % 7) + 2 * b
            mine = beta == bb

            def onward(full):
                if kind == 0:
                    first, second = (0, 2), (0, 2) if full else (1 - ylo, 1)
                else:
                    first, second = (0, 2) if full else (1 - ylo, 1), (0, 2)
                src = passing.at[pl.ds(row + first[0], first[1]), pl.ds(*second)]
                at = (2 * b, 2 * a) if kind == 0 else (2 * a, 2 * b)
                dst = f_ref.at[pl.ds(at[0] + first[0], first[1]), pl.ds(at[1] + second[0], second[1])]
                copy(src, dst, s2, r2.at[group(dz, kind)], r, 2 * wrap(z + dz % 8, 8) + ylo).start()

            @pl.when(mine)
            def _():
                arrived(r1.at[n], 2)
                onward(False)

            @pl.when(jnp.logical_not(mine))
            def _():
                arrived(r1.at[n], 4)
                onward(True)

    pass_on()
    for load in smalls:
        load.wait()
    for u in range(1, 6):
        for following in AHEAD[u]:
            send_unit(following)
        if u == 2:
            factors[...] = gate_factors(angles[...], targets, order)
        if u == 3:
            share_sums()
        if u == 4:
            prepare_lanes(ylo, factors[...], right1)
        if u == 5:
            prepare_rows(z, factors[...], small, right2, left, matrix_ref)
        forward(u)

    copy(part_sums.at[pl.ds(0, 31)], part_sums.at[pl.ds(0, 31)], sa, ra, r, c).wait_recv()
    plane_sums[z] = jnp.sum(part_sums[...], axis=0)
    for k in range(1, 8):
        copy(plane_sums.at[z], plane_sums.at[z], sb, rb, r, 2 * wrap(z + k, 8) + ylo).start()

    def over_g2(g, out):
        v = jnp.concatenate([f_ref[g + n].reshape(256, 128) for n in range(2)], axis=1)
        v = dot3((right2[0], right2[1]), halves(v))
        for n in range(2):
            out[n] = v[:, 128 * n : 128 * n + 128].reshape((16,) + BLOCK)

    either(beta == 0, arrived, r1z, (59, 58))
    on_lanes(f_ref, right1, 0, 2, 0, 16)
    on_lanes(f_ref, right1, 2, 14, 0, 2)
    turned2[pl.ds(2, 2)] = jnp.zeros((2, 16) + BLOCK, jnp.float32)
    turned2[pl.ds(14, 2)] = jnp.zeros((2, 16) + BLOCK, jnp.float32)
    arrived(r2.at[0], 100)
    for n in range(5):
        on_lanes(f_ref, right1, 4 + 2 * n, 2, 4, 10)
    arrived(r2.at[1], 56)
    on_lanes(f_ref, right1, 2, 14, 2, 2)
    on_lanes(f_ref, right1, 2, 14, 14, 2)
    for g in (0, 4, 6, 8, 10, 12):
        over_g2(g, turned2.at[pl.ds(g, 2)])
    for rows in ((0, 1, 4, 5), (6, 7, 8, 9), (10, 11, 12, 13)):
        unpack(turned2, tmp, rows)
    for n in range(8):
        v = jnp.concatenate([turned2[:, 2 * n + m].reshape(256, 128) for m in range(2)], axis=1)
        early_ref[n // 2, :, 256 * (n % 2) : 256 * (n % 2) + 256] = dot3((left[0], left[1]), halves(v))
    either(beta == 0, left_all, s1, (241, 242))
    left_all(s2, 196)
    copy(plane_sums.at[pl.ds(0, 7)], plane_sums.at[pl.ds(0, 7)], sb, rb, r, c).wait()
    copy(part_sums.at[pl.ds(0, 31)], part_sums.at[pl.ds(0, 31)], sa, ra, r, c).wait_send()
    sums_ref[...] = jnp.sum(plane_sums[...], axis=0)
    arrived(r2.at[2], 40)
    on_lanes(f_ref, right1, 2, 2, 4, 10)
    on_lanes(f_ref, right1, 14, 2, 4, 10)
    over_g2(2, late_ref.at[pl.ds(0, 2)])
    over_g2(14, late_ref.at[pl.ds(2, 2)])
    unpack(late_ref, tmp, range(4))


def exchange_call(*args):
    f32, bf16 = jnp.float32, jnp.bfloat16
    dma = pltpu.SemaphoreType.DMA
    vmem, hbm = pl.BlockSpec(memory_space=pltpu.VMEM), pl.BlockSpec(memory_space=pltpu.HBM)
    blocks = lambda *n: pltpu.VMEM(n + BLOCK, f32)
    return pl.pallas_call(
        exchange_kernel,
        name="exchange",
        out_shape=(
            jax.ShapeDtypeStruct((4, 256, 512), f32),
            jax.ShapeDtypeStruct((4, 16) + BLOCK, f32),
            jax.ShapeDtypeStruct((256, 256), bf16),
            jax.ShapeDtypeStruct((1, 128), f32),
        ),
        in_specs=[hbm] * 7,
        out_specs=(vmem, vmem, vmem, vmem),
        scratch_shapes=[
            pltpu.VMEM((2, 512, 512), f32),
            pltpu.VMEM((2, 512, 512), f32),
            blocks(2, 256),
            blocks(32),
            blocks(224, 2),
            blocks(16, 16),
            pltpu.VMEM((32, 1, 128), f32),
            pltpu.VMEM((8, 1, 128), f32),
            pltpu.VMEM((2, 16, 16), f32),
            pltpu.VMEM((3, 8), f32),
            pltpu.SMEM((8,), jnp.int32),
            pltpu.SMEM((8,), jnp.int32),
            pltpu.VMEM((32, 8), f32),
            pltpu.VMEM((2, 256, 256), bf16),
            pltpu.VMEM((2, 256, 256), bf16),
            pltpu.VMEM((2, 256, 256), bf16),
            blocks(16, 16),
            pltpu.VMEM((32, 4, 8, 128), f32),
            dma((2, 4)),
            dma((5,)),
            dma,
            dma((32,)),
            dma((len(SLOT),)),
            dma,
            dma,
            dma((3,)),
            dma,
            dma,
            dma,
            dma,
        ],
        compiler_params=pltpu.CompilerParams(collective_id=0, has_side_effects=True, vmem_limit_bytes=40 * 2**20),
    )(*args)


def iota2(n, m, dim):
    return lax.broadcasted_iota(jnp.int32, (n, m), dim)


def halves(v):
    hi = v.astype(jnp.bfloat16)
    return hi, (v - hi.astype(jnp.float32)).astype(jnp.bfloat16)


def dot(a, b):
    return jnp.dot(a, b, preferred_element_type=jnp.float32)


def dot3(a, b):
    return dot(a[0], b[0]) + dot(a[0], b[1]) + dot(a[1], b[0])


def gate_factors(angles, targets, order):
    theta, alpha, beta = angles[0:1], angles[1:2], angles[2:3]
    cos, sin = jnp.cos(theta / 2), jnp.sin(theta / 2)
    both = alpha + beta
    elements = (
        (cos, cos * 0.0),
        (-jnp.cos(beta) * sin, -jnp.sin(beta) * sin),
        (jnp.cos(alpha) * sin, jnp.sin(alpha) * sin),
        (jnp.cos(both) * cos, jnp.sin(both) * cos),
    )
    i, j = iota2(32, 32, 0), iota2(32, 32, 1)
    left, right, high = i % 8, j % 8, i >= 16
    same_part, lower, same_factor = (i // 8) % 2 == (j // 8) % 2, i > j, i // 16 == j // 16
    gates = lax.broadcasted_iota(jnp.int32, (1, GATES), 1)
    total = jnp.where((iota2(32, 8, 0) % 16) == iota2(32, 8, 1), 1.0, 0.0)
    for position in range(GATES):
        gate = order[position]
        target = targets[gate]
        low_bit = jnp.where(target == 0, 1, jnp.where(target == 1, 2, jnp.where(target == 2, 4, 0)))
        high_bit = jnp.where(target == 3, 1, jnp.where(target == 4, 2, 0))
        bit = jnp.where(high, high_bit, low_bit)
        entry = [
            [jnp.sum(jnp.where(gates == gate, e, 0.0), axis=1, keepdims=True) for e in pair] for pair in elements
        ]
        left_high, right_high = (left & bit) > 0, (right & bit) > 0
        same_rest = ((left ^ right) | bit) == bit
        step = [
            jnp.where(
                left_high,
                jnp.where(right_high, entry[3][part], entry[2][part]),
                jnp.where(right_high, entry[1][part], entry[0][part]),
            )
            for part in range(2)
        ]
        step = [jnp.where(bit > 0, v, one) for v, one in zip(step, (1.0, 0.0))]
        step = jnp.where(same_part, step[0], jnp.where(lower, step[1], -step[1]))
        step = jnp.where(same_rest & same_factor, step, 0.0)
        total = jnp.dot(step, total, precision=HIGHEST, preferred_element_type=jnp.float32)
    return total


def one_hot(n, m, index):
    return jnp.where(index == iota2(n, m, 1), 1.0, 0.0)


def spread(rows, small, cols):
    wide = jnp.dot(rows, small, precision=HIGHEST, preferred_element_type=jnp.float32)
    return lax.dot_general(wide, cols, (((1,), (1,)), ((), ())), precision=HIGHEST, preferred_element_type=jnp.float32)


def times(a, b):
    return a[0] * b[0] - a[1] * b[1], a[0] * b[1] + a[1] * b[0]


def store_halves(ref, v):
    hi, lo = halves(v)
    ref[0] = hi
    ref[1] = lo


def of(factors, which):
    return [factors[16 * which + 8 * part : 16 * which + 8 * part + 8] for part in range(2)]


def by_row(n):
    return iota2(256, n, 0)


def prepare_lanes(ylo, factors, right1):
    i, j = iota2(256, 256, 0), iota2(256, 256, 1)
    low, high = of(factors, 0), of(factors, 1)
    k = (by_row(8) // 32) % 4
    on_k = one_hot(256, 8, k)
    from_k = one_hot(256, 8, jnp.where((ylo == 1) & (k % 2 == 0), 2 - k, k))
    on_top = one_hot(256, 8, (by_row(8) // 8) % 4)
    on_s = one_hot(256, 8, by_row(8) % 8)
    turn = lambda hot, m, to: spread(hot, m.T, to)
    a = [turn(from_k, m, on_k) for m in high]
    b = times([turn(on_top, m, on_top) for m in high], [turn(on_s, m, on_s) for m in low])
    value = times(a, (b[0], -b[1]))
    same, lower = i // 128 == j // 128, i > j
    store_halves(right1, jnp.where(same, value[0], jnp.where(lower, -value[1], value[1])))


def prepare_rows(z, factors, small, right2, left, late_ref):
    i, j = iota2(256, 256, 0), iota2(256, 256, 1)
    low = of(factors, 0)
    out_g = one_hot(256, 16, by_row(16) // 16)
    in_g = one_hot(256, 16, (by_row(16) // 16 + 2 * z) % 16)
    u = [spread(out_g, small[part], in_g) for part in range(2)]
    same, lower = (i // 8) % 2 == (j // 8) % 2, (i // 8) % 2 > (j // 8) % 2
    value = jnp.where(same, u[0], jnp.where(lower, -u[1], u[1]))
    store_halves(right2, jnp.where(i % 8 == j % 8, value, 0.0))
    on_s = one_hot(256, 8, by_row(8) % 8)
    low = [spread(on_s, m, on_s) for m in low]
    real = lambda value: KEEP * jnp.where(same, value[0], jnp.where(lower, value[1], -value[1]))
    store_halves(left, real(times(u, low)))
    n = (by_row(16) // 16) % 4
    in_g = one_hot(256, 16, (n + jnp.where(n < 2, 2, 12) + 2 * z) % 16)
    u = [spread(out_g, small[part], in_g) for part in range(2)]
    hi, lo = (v.astype(jnp.float32) for v in halves(real(times(u, low))))
    segment = j // 64
    late_ref[...] = jnp.where(segment == 3, 0.0, jnp.where(segment == 1, lo, hi)).astype(jnp.bfloat16)


def on_lanes(f_ref, right1, g, n, g2, n2):
    here = (pl.ds(g, n), pl.ds(g2, n2))
    v = jnp.concatenate([f_ref[(*here, part)].reshape(n * n2 * 8, 128) for part in range(2)], axis=1)
    v = dot3(halves(v), (right1[0], right1[1]))
    for part in range(2):
        f_ref[(*here, part)] = v[:, 128 * part : 128 * part + 128].reshape(n, n2, 8, 128)


def rotate_kernel(early_ref, late_ref, matrix_ref, sums_ref, re_ref, im_ref, purity_ref, purity, stage, product, sem, purity_sem):
    r, c = lax.axis_index("row"), lax.axis_index("col")
    sums = sums_ref[...]
    lane = lanes((1, 128))
    total, trace_re, trace_im = (jnp.sum(jnp.where(lane == n, sums, 0.0)) for n in range(3))
    dim = GATE * GATE * LOW
    shifts = (jnp.where(r == c, MIX * trace_re / dim, 0.0), jnp.where(r == c, MIX * trace_im / dim, 0.0))
    squared = trace_re * trace_re + trace_im * trace_im
    purity[0, 0] = (KEEP * KEEP * total + (2 * KEEP * MIX + MIX * MIX) * squared / dim) / (dim * dim)
    matrix = matrix_ref[...]
    sublane = lax.broadcasted_iota(jnp.int32, (8, 128), 0)
    v = jnp.concatenate([late_ref[:, n].reshape(64, 128) for n in range(16)], axis=1)
    hi, lo = halves(v)
    product[...] = dot(matrix, jnp.concatenate([hi, hi, lo, jnp.zeros_like(hi)], axis=0))
    copies = [pltpu.make_async_copy(purity, purity_ref, purity_sem)]
    copies[0].start()
    for q in range(4):
        for g in range(16):
            for part in range(2):
                for k in range(4):
                    row, col = 16 * g + 8 * part, 128 * k
                    tile = early_ref[q, row : row + 8, col : col + 128]
                    tile = tile + product[row : row + 8, 512 * q + col : 512 * q + col + 128]
                    if g // 4 == q:
                        tile = tile + jnp.where(lanes() == sublane + (32 * (g % 4) + 8 * k), shifts[part], 0.0)
                    stage[part, q, 32 * g + 8 * k : 32 * g + 8 * k + 8] = tile
        for part, ref in ((0, re_ref), (1, im_ref)):
            copies.append(pltpu.make_async_copy(stage.at[part, q], ref.at[:, pl.ds(128 * q, 128)], sem.at[part, q]))
            copies[-1].start()
    for copy in copies:
        copy.wait()


def rotate_call(*args):
    f32 = jnp.float32
    vmem, hbm = pl.BlockSpec(memory_space=pltpu.VMEM), pl.BlockSpec(memory_space=pltpu.HBM)
    return pl.pallas_call(
        rotate_kernel,
        name="rotate",
        out_shape=(
            jax.ShapeDtypeStruct((512, 512), f32),
            jax.ShapeDtypeStruct((512, 512), f32),
            jax.ShapeDtypeStruct((1, 1), f32),
        ),
        in_specs=[vmem] * 4,
        out_specs=(hbm, hbm, hbm),
        scratch_shapes=[
            pltpu.SMEM((1, 1), f32),
            pltpu.VMEM((2, 4, 512, 128), f32),
            pltpu.VMEM((256, 2048), f32),
            pltpu.SemaphoreType.DMA((2, 4)),
            pltpu.SemaphoreType.DMA,
        ],
        compiler_params=pltpu.CompilerParams(vmem_limit_bytes=20 * 2**20),
    )(*args)


def on_device(rho_real, rho_imag, gate_real_matrix, gate_imaginary, angles, targets, gate_order):
    args = (rho_real, rho_imag, gate_real_matrix, gate_imaginary, angles.T, targets, gate_order)
    found = exchange_call(*(pltpu.with_memory_space_constraint(v, pltpu.HBM) for v in args))
    re, im, purity = rotate_call(*found)
    return re, im, purity.reshape(())


def solution(mesh):
    return jax.shard_map(
        on_device,
        mesh=mesh,
        in_specs=(P("row", "col"), P("row", "col"), P(), P(), P(), P(), P()),
        out_specs=(P("row", "col"), P("row", "col"), P()),
        check_vma=False,
    )
```

```python
import functools

import jax
import jax.numpy as jnp
from jax import lax
from jax.experimental import pallas as pl
from jax.experimental.pallas import tpu as pltpu
from jax.sharding import PartitionSpec as P

MESH = pl.DeviceIdType.MESH
HIGHEST = lax.Precision.HIGHEST
MIX = 0.25
KEEP = 1 - MIX
GATE = 16
LOW = 32
GATES = 8
BLOCK = (2, 8, 128)


def ring(v):
    v %= 8
    return min(v, 8 - v)


STEPS = [4, 3, -3, 2, -2, 1, -1, 0]
ORDER = [(d_, k_) for d_ in STEPS[:5] for k_ in (0, 1)] + [(d_, k_) for k_ in (0, 1) for d_ in (1, -1)] + [(0, 0), (0, 1)]
UNITS = [
    [(d_, k_) for d_, k_ in ORDER if ring(b_ - d_) >= ring(d_) + k_] for b_ in range(8)
]
BESIDE = {2: (1, 0), 3: (-1, 0)}
UNITS[0] = [u_ for u_ in UNITS[0] if u_ not in BESIDE.values()] + [None, None]
CHIPS = sorted(((jx, jy) for jx in range(4) for jy in range(4) if jx or jy), key=lambda j: (min(j[0], 4 - j[0]) + min(j[1], 4 - j[1]), j))
HOPS = lambda j: min(j[0], 4 - j[0]) + min(j[1], 4 - j[1])
OTHERS = sorted(((jx, jy, jc) for jx, jy in CHIPS for jc in range(2)), key=lambda j: (HOPS(j), j[2], j))
BETAS = [7, 1, 6, 2, 5, 3, 4, 0]
FORWARDS = [
    [(*UNITS[b_][u_], b_) for b_ in BETAS if UNITS[b_][u_] and UNITS[b_][u_][0] != 0] + ([(*BESIDE[u_], 0)] if u_ in BESIDE else [])
    for u_ in range(8)
]
SLOT = {f_: i_ for i_, f_ in enumerate(f_ for fs_ in FORWARDS[1:] for f_ in fs_)}
AHEAD = {1:[2,3],2:[4],3:[5,6],4:[7],5:[]}


def group(dz, kind):
    return 1 + kind if ring(dz) == 1 else 0


def wrap(v, n):
    return jnp.where(v >= n, v - n, v)


def near(v):
    return jnp.minimum(v, 8 - v)


def pick(index, values):
    out = jnp.int32(values[0])
    for i, value in enumerate(values):
        if value != values[0]:
            out = jnp.where(index == i, value, out)
    return out


def lanes(shape=(8, 128)):
    return lax.broadcasted_iota(jnp.int32, shape, 1)


def halve(a, b, mask, shift):
    turned = pltpu.roll(jnp.where(mask, b, a), shift, 1)
    return jnp.where(mask, a, turned), jnp.where(mask, turned, b)


def pack(src, dst, tmp, i):
    low = lanes() < 64
    even = (lanes() // 32) % 2 == 0
    groups = [(4 * i + n, part, q) for n in range(4) for part in range(2) for q in range(4)]
    for n, (h, part, q) in enumerate(groups):
        tiles = [src[part, 32 * h + 8 * k : 32 * h + 8 * k + 8, 128 * q : 128 * q + 128] for k in range(4)]
        for k in range(2):
            tmp[n, k], tmp[n, k + 2] = halve(tiles[k], tiles[k + 2], low, 64)
    for n, (h, part, q) in enumerate(groups):
        for m in range(2):
            at = 16 * h + 4 * q + 2 * m
            dst[at, part], dst[at + 1, part] = halve(tmp[n, 2 * m], tmp[n, 2 * m + 1], even, 32)


def unpack(ref, tmp, rows):
    low = lanes() < 64
    even = (lanes() // 32) % 2 == 0
    groups = [(g, part, q) for g in rows for part in range(2) for q in range(4)]
    for n, (g, part, q) in enumerate(groups):
        for m in range(2):
            tmp[n, m], tmp[n, m + 2] = halve(ref[g, 4 * q + m, part], ref[g, 4 * q + m + 2, part], low, 64)
    for n, (g, part, q) in enumerate(groups):
        for m in range(2):
            a, b = tmp[n, 2 * m], tmp[n, 2 * m + 1]
            ref[g, 4 * q + 2 * m, part] = jnp.where(even, a, pltpu.roll(b, 32, 1))
            ref[g, 4 * q + 2 * m + 1, part] = jnp.where(even, pltpu.roll(a, 96, 1), b)


def exchange_kernel(
    re_hbm, im_hbm, ure_hbm, uim_hbm, angles_hbm, targets_hbm, order_hbm, early_ref, late_ref, matrix_ref, sums_ref,
    own, turned, packed, mu, passing, f_ref, part_sums, plane_sums, small, angles, targets, order, factors, right1, right2, left, turned2, tmp,
    load_sem, small_sem, s1, ru, r1, r1z, s2, r2, sa, ra, sb, rb,
):
    r, c = lax.axis_index("row"), lax.axis_index("col")
    z, ylo = c // 2, c % 2
    rho, core = r // 2, r % 2
    x, y = rho % 4, (rho // 4) * 2 + ylo
    partner = r + 1 - 2 * core
    beta = wrap(rho + 8 - z, 8)
    cores = (core, 1 - core)
    ahead = [wrap(x + jx, 4) * 2 for jx in range(4)]
    behind = [wrap(x + 4 - jx, 4) for jx in range(4)]
    halves_of = lambda yy, top: (jnp.where(yy >= 2, top, 0), jnp.where(yy >= 2, yy - 2, yy))
    up = [halves_of(wrap(y + jy, 4), 8) for jy in range(4)]
    down = [halves_of(wrap(y + 4 - jy, 4), 4) for jy in range(4)]

    def others(fn):
        for j, (jx, jy, jc) in enumerate(OTHERS):
            fn(up[jy][0] + ahead[jx] + 1 - jc, up[jy][1], jnp.where(core == 1, OTHERS.index((jx, jy, 0)), OTHERS.index((jx, jy, 1))))

    def copy(src, dst, send, recv, row, col):
        return pltpu.make_async_remote_copy(src, dst, send, recv, device_id=(row, col), device_id_type=MESH)

    loads = [
        [
            pltpu.make_async_copy(ref.at[pl.ds(128 * i, 128)], own.at[part, pl.ds(128 * i, 128)], load_sem.at[part, i])
            for part, ref in ((0, re_hbm), (1, im_hbm))
        ]
        for i in range(4)
    ]
    barrier = pltpu.get_barrier_semaphore()

    def greet_plane(first, last):
        for j, (jx, jy, jc) in reversed(list(enumerate(OTHERS))):
            if first <= HOPS((jx, jy)) <= last:
                pl.semaphore_signal(
                    barrier, inc=1, device_id=(up[jy][0] + ahead[jx] + cores[jc], 2 * z + up[jy][1]), device_id_type=MESH
                )

    def greet_line(*steps):
        for k in steps:
            for h in (r, partner):
                pl.semaphore_signal(barrier, inc=1, device_id=(h, 2 * wrap(z + k, 8) + ylo), device_id_type=MESH)

    for pair in loads:
        for load in pair:
            load.start()
    greet_plane(4, 4)
    greet_line(4)
    greet_plane(3, 3)
    greet_line(3, 5)
    greet_plane(2, 2)
    greet_line(2, 6)
    greet_plane(1, 1)
    greet_line(1, 7)
    pl.semaphore_signal(barrier, inc=1, device_id=(partner, 2 * z + ylo), device_id_type=MESH)
    smalls = [
        pltpu.make_async_copy(ref, dst, small_sem.at[i])
        for i, (ref, dst) in enumerate(
            (
                (ure_hbm, small.at[0]),
                (uim_hbm, small.at[1]),
                (angles_hbm, angles),
                (targets_hbm, targets),
                (order_hbm, order),
            )
        )
    ]
    for load in smalls:
        load.start()
    for i, pair in enumerate(loads):
        for load in pair:
            load.wait()
        pack(own, packed.at[0], tmp, i)

    pl.semaphore_wait(barrier, 45)

    def at_step(dz):
        zz = wrap(z + dz % 8, 8)
        b = wrap(rho + 8 - zz, 8)
        return zz, b, near(b) >= ring(dz), near(b) > ring(dz)

    def straight(kind):
        for dz in STEPS[:-1]:
            zz, b, direct, also = at_step(dz)
            if kind == 1 and ring(dz) == 4:
                continue
            a = (-dz) % 8

            @pl.when(also if kind else direct)
            def _():
                for h in (r, partner):
                    copy(
                        packed.at[kind, 16 * h + 2 * zz + ylo],
                        f_ref.at[2 * a + ylo, 2 * b + core] if kind else f_ref.at[2 * b + core, 2 * a + ylo],
                        s2,
                        r2.at[group(dz, kind)],
                        h,
                        2 * zz + ylo,
                    ).start()

    def send_unit(u):
        unit = [UNITS[b][u] or (0, 0) for b in range(8)]
        dz = pick(beta, [d % 8 for d, _ in unit])
        kind = pick(beta, [k for _, k in unit])
        zz = wrap(z + dz, 8)
        b = wrap(beta + 8 - dz, 8)
        first, second = jnp.where(kind == 0, core, ylo), jnp.where(kind == 0, ylo, core)
        if u == 0:
            others(lambda h, p, j: copy(packed.at[0, 16 * h + 2 * zz + p], mu.at[j], s1, ru.at[j], h, 2 * z + p).start())
            return

        def passed():
            row = 112 * kind + 16 * pick(beta, [STEPS.index(d) % 7 for d, _ in unit]) + 2 * b + first
            sem = r1.at[pick(beta, [SLOT.get((*unit[bb], bb), 0) for bb in range(8)])]
            others(lambda h, p, j: copy(packed.at[kind, 16 * h + 2 * zz + p], passing.at[row, second], s1, sem, h, 2 * z + p).start())

        def kept():
            row, col = jnp.where(kind == 0, 2 * b + core, ylo), jnp.where(kind == 0, ylo, 2 * b + core)

            def send(h, p, j):
                copy(packed.at[kind, 16 * h + 2 * zz + p], f_ref.at[row, col], s1, r1z, h, 2 * z + p).start()

            others(send)
            send(partner, ylo, 0)
            f_ref[row, col] = packed[kind, 16 * r + 2 * zz + ylo]

        here = [UNITS[bb][u] is not None and UNITS[bb][u][0] == 0 for bb in range(8)]
        away = [UNITS[bb][u] is not None and UNITS[bb][u][0] != 0 for bb in range(8)]
        for which, action in ((away, passed), (here, kept)):
            if all(which):
                action()
            elif any(which):
                pl.when(pick(beta, [int(v) for v in which]) == 1)(action)

        if u in BESIDE:

            @pl.when(beta == 0)
            def _():
                d, k = BESIDE[u]
                zb = wrap(z + d % 8, 8)
                row = 112 * k + 16 * STEPS.index(d) + 2 * (-d % 8) + core
                others(
                    lambda h, p, j: copy(
                        packed.at[k, 16 * h + 2 * zb + p], passing.at[row, ylo], s1, r1.at[SLOT[d, k, 0]], h, 2 * z + p
                    ).start()
                )

    send_unit(0)
    straight(0)
    for i in range(4):
        rows = pl.ds(128 * i, 128)
        for j in range(4):
            there = pl.ds(128 * j, 128)
            turned[0, there, rows] = own[0, rows, there].T
            turned[1, there, rows] = -own[1, rows, there].T
    for i in range(4):
        pack(turned, packed.at[1], tmp, i)
    straight(1)

    def arrived(sem, count):
        copy(packed.at[0, pl.ds(0, count)], packed.at[1, pl.ds(0, count)], sem, sem, r, c).wait_recv()

    def left_all(sem, count):
        copy(packed.at[0, pl.ds(0, count)], packed.at[1, pl.ds(0, count)], sem, sem, r, c).wait_send()

    def either(condition, wait, sem, counts):
        @pl.when(condition)
        def _():
            wait(sem, counts[0])

        @pl.when(jnp.logical_not(condition))
        def _():
            wait(sem, counts[1])

    def share_sums():
        def squares(i, accs):
            for n in range(2):
                rows = pl.ds(pl.multiple_of(16 * i + 8 * n, 8), 8)
                tiles = [own[part, rows, pl.ds(128 * q, 128)] for part in range(2) for q in range(4)]
                accs = [acc + v * v for acc, v in zip(accs, tiles)]
            return accs

        total = jnp.sum(sum(lax.fori_loop(0, 32, squares, [jnp.zeros((8, 128), jnp.float32)] * 8)))
        on_diagonal = lanes((128, 128)) == lax.broadcasted_iota(jnp.int32, (128, 128), 0)
        traces = []
        for part in range(2):
            v = sum(own[part, pl.ds(128 * q, 128), pl.ds(128 * q, 128)] for q in range(4))
            traces.append(jnp.where(r == c, jnp.sum(jnp.where(on_diagonal, v, 0.0)), 0.0))
        lane = lanes((1, 128))
        place = (y * 4 + x) * 2 + core
        part_sums[place] = jnp.where(lane == 0, total, jnp.where(lane == 1, traces[0], jnp.where(lane == 2, traces[1], 0.0)))

        def share(h, p, j):
            copy(part_sums.at[place], part_sums.at[place], sa, ra, h, 2 * z + p).start()

        others(share)
        share(partner, ylo, 0)

    def pass_on():
        for j, (jx, jy, jc) in enumerate(OTHERS):
            if j == 8:
                send_unit(1)
            bs = wrap(wrap(down[jy][0] + behind[jx] + 8 - z, 8), 8)
            dz = pick(bs, [UNITS[b][0][0] % 8 for b in range(8)])
            a, b = wrap(8 - dz, 8), wrap(bs + 8 - dz, 8)
            copy(mu.at[j], mu.at[j], s1, ru.at[j], r, c).wait_recv()
            dst = f_ref.at[2 * b + 1 - jc, 2 * a + down[jy][1]]
            copy(mu.at[j], dst, s2, r2.at[0], r, 2 * wrap(z + dz, 8) + ylo).start()

    def forward(u):
        for dz, kind, bb in FORWARDS[u]:
            n = SLOT[dz, kind, bb]
            a, b = (-dz) % 8, (bb - dz) % 8
            row = 112 * kind + 16 * (STEPS.index(dz) % 7) + 2 * b
            mine = beta == bb

            def onward(full):
                if kind == 0:
                    first, second = (0, 2), (0, 2) if full else (1 - ylo, 1)
                else:
                    first, second = (0, 2) if full else (1 - ylo, 1), (0, 2)
                src = passing.at[pl.ds(row + first[0], first[1]), pl.ds(*second)]
                at = (2 * b, 2 * a) if kind == 0 else (2 * a, 2 * b)
                dst = f_ref.at[pl.ds(at[0] + first[0], first[1]), pl.ds(at[1] + second[0], second[1])]
                copy(src, dst, s2, r2.at[group(dz, kind)], r, 2 * wrap(z + dz % 8, 8) + ylo).start()

            @pl.when(mine)
            def _():
                arrived(r1.at[n], 2)
                onward(False)

            @pl.when(jnp.logical_not(mine))
            def _():
                arrived(r1.at[n], 4)
                onward(True)

    pass_on()
    for load in smalls:
        load.wait()
    for u in range(1, 6):
        for following in AHEAD[u]:
            send_unit(following)
        if u == 2:
            factors[...] = gate_factors(angles[...], targets, order)
        if u == 3:
            share_sums()
        if u == 4:
            prepare_lanes(ylo, factors[...], right1)
        if u == 5:
            prepare_rows(z, factors[...], small, right2, left, matrix_ref)
        forward(u)

    copy(part_sums.at[pl.ds(0, 31)], part_sums.at[pl.ds(0, 31)], sa, ra, r, c).wait_recv()
    plane_sums[z] = jnp.sum(part_sums[...], axis=0)
    for k in range(1, 8):
        copy(plane_sums.at[z], plane_sums.at[z], sb, rb, r, 2 * wrap(z + k, 8) + ylo).start()

    def over_g2(g, out):
        v = jnp.concatenate([f_ref[g + n].reshape(256, 128) for n in range(2)], axis=1)
        v = dot3((right2[0], right2[1]), halves(v))
        for n in range(2):
            out[n] = v[:, 128 * n : 128 * n + 128].reshape((16,) + BLOCK)

    either(beta == 0, arrived, r1z, (59, 58))
    on_lanes(f_ref, right1, 0, 2, 0, 16)
    on_lanes(f_ref, right1, 2, 14, 0, 2)
    turned2[pl.ds(2, 2)] = jnp.zeros((2, 16) + BLOCK, jnp.float32)
    turned2[pl.ds(14, 2)] = jnp.zeros((2, 16) + BLOCK, jnp.float32)
    arrived(r2.at[0], 100)
    for n in range(5):
        on_lanes(f_ref, right1, 4 + 2 * n, 2, 4, 10)
    arrived(r2.at[1], 56)
    on_lanes(f_ref, right1, 2, 14, 2, 2)
    on_lanes(f_ref, right1, 2, 14, 14, 2)
    for g in (0, 4, 6, 8, 10, 12):
        over_g2(g, turned2.at[pl.ds(g, 2)])
    for rows in ((0, 1, 4, 5), (6, 7, 8, 9), (10, 11, 12, 13)):
        unpack(turned2, tmp, rows)
    for n in range(8):
        v = jnp.concatenate([turned2[:, 2 * n + m].reshape(256, 128) for m in range(2)], axis=1)
        early_ref[n // 2, :, 256 * (n % 2) : 256 * (n % 2) + 256] = dot3((left[0], left[1]), halves(v))
    either(beta == 0, left_all, s1, (241, 242))
    left_all(s2, 196)
    copy(plane_sums.at[pl.ds(0, 7)], plane_sums.at[pl.ds(0, 7)], sb, rb, r, c).wait()
    copy(part_sums.at[pl.ds(0, 31)], part_sums.at[pl.ds(0, 31)], sa, ra, r, c).wait_send()
    sums_ref[...] = jnp.sum(plane_sums[...], axis=0)
    arrived(r2.at[2], 40)
    on_lanes(f_ref, right1, 2, 2, 4, 10)
    on_lanes(f_ref, right1, 14, 2, 4, 10)
    over_g2(2, late_ref.at[pl.ds(0, 2)])
    over_g2(14, late_ref.at[pl.ds(2, 2)])
    unpack(late_ref, tmp, range(4))


def exchange_call(*args):
    f32, bf16 = jnp.float32, jnp.bfloat16
    dma = pltpu.SemaphoreType.DMA
    vmem, hbm = pl.BlockSpec(memory_space=pltpu.VMEM), pl.BlockSpec(memory_space=pltpu.HBM)
    blocks = lambda *n: pltpu.VMEM(n + BLOCK, f32)
    return pl.pallas_call(
        exchange_kernel,
        name="exchange",
        out_shape=(
            jax.ShapeDtypeStruct((4, 256, 512), f32),
            jax.ShapeDtypeStruct((4, 16) + BLOCK, f32),
            jax.ShapeDtypeStruct((256, 256), bf16),
            jax.ShapeDtypeStruct((1, 128), f32),
        ),
        in_specs=[hbm] * 7,
        out_specs=(vmem, vmem, vmem, vmem),
        scratch_shapes=[
            pltpu.VMEM((2, 512, 512), f32),
            pltpu.VMEM((2, 512, 512), f32),
            blocks(2, 256),
            blocks(32),
            blocks(224, 2),
            blocks(16, 16),
            pltpu.VMEM((32, 1, 128), f32),
            pltpu.VMEM((8, 1, 128), f32),
            pltpu.VMEM((2, 16, 16), f32),
            pltpu.VMEM((3, 8), f32),
            pltpu.SMEM((8,), jnp.int32),
            pltpu.SMEM((8,), jnp.int32),
            pltpu.VMEM((32, 8), f32),
            pltpu.VMEM((2, 256, 256), bf16),
            pltpu.VMEM((2, 256, 256), bf16),
            pltpu.VMEM((2, 256, 256), bf16),
            blocks(16, 16),
            pltpu.VMEM((32, 4, 8, 128), f32),
            dma((2, 4)),
            dma((5,)),
            dma,
            dma((32,)),
            dma((len(SLOT),)),
            dma,
            dma,
            dma((3,)),
            dma,
            dma,
            dma,
            dma,
        ],
        compiler_params=pltpu.CompilerParams(collective_id=0, has_side_effects=True, vmem_limit_bytes=40 * 2**20),
    )(*args)


def iota2(n, m, dim):
    return lax.broadcasted_iota(jnp.int32, (n, m), dim)


def halves(v):
    hi = v.astype(jnp.bfloat16)
    return hi, (v - hi.astype(jnp.float32)).astype(jnp.bfloat16)


def dot(a, b):
    return jnp.dot(a, b, preferred_element_type=jnp.float32)


def dot3(a, b):
    return dot(a[0], b[0]) + dot(a[0], b[1]) + dot(a[1], b[0])


def gate_factors(angles, targets, order):
    theta, alpha, beta = angles[0:1], angles[1:2], angles[2:3]
    cos, sin = jnp.cos(theta / 2), jnp.sin(theta / 2)
    both = alpha + beta
    elements = (
        (cos, cos * 0.0),
        (-jnp.cos(beta) * sin, -jnp.sin(beta) * sin),
        (jnp.cos(alpha) * sin, jnp.sin(alpha) * sin),
        (jnp.cos(both) * cos, jnp.sin(both) * cos),
    )
    i, j = iota2(32, 32, 0), iota2(32, 32, 1)
    left, right, high = i % 8, j % 8, i >= 16
    same_part, lower, same_factor = (i // 8) % 2 == (j // 8) % 2, i > j, i // 16 == j // 16
    gates = lax.broadcasted_iota(jnp.int32, (1, GATES), 1)
    total = jnp.where((iota2(32, 8, 0) % 16) == iota2(32, 8, 1), 1.0, 0.0)
    for position in range(GATES):
        gate = order[position]
        target = targets[gate]
        low_bit = jnp.where(target == 0, 1, jnp.where(target == 1, 2, jnp.where(target == 2, 4, 0)))
        high_bit = jnp.where(target == 3, 1, jnp.where(target == 4, 2, 0))
        bit = jnp.where(high, high_bit, low_bit)
        entry = [
            [jnp.sum(jnp.where(gates == gate, e, 0.0), axis=1, keepdims=True) for e in pair] for pair in elements
        ]
        left_high, right_high = (left & bit) > 0, (right & bit) > 0
        same_rest = ((left ^ right) | bit) == bit
        step = [
            jnp.where(
                left_high,
                jnp.where(right_high, entry[3][part], entry[2][part]),
                jnp.where(right_high, entry[1][part], entry[0][part]),
            )
            for part in range(2)
        ]
        step = [jnp.where(bit > 0, v, one) for v, one in zip(step, (1.0, 0.0))]
        step = jnp.where(same_part, step[0], jnp.where(lower, step[1], -step[1]))
        step = jnp.where(same_rest & same_factor, step, 0.0)
        total = jnp.dot(step, total, precision=HIGHEST, preferred_element_type=jnp.float32)
    return total


def one_hot(n, m, index):
    return jnp.where(index == iota2(n, m, 1), 1.0, 0.0)


def spread(rows, small, cols):
    wide = jnp.dot(rows, small, precision=HIGHEST, preferred_element_type=jnp.float32)
    return lax.dot_general(wide, cols, (((1,), (1,)), ((), ())), precision=HIGHEST, preferred_element_type=jnp.float32)


def times(a, b):
    return a[0] * b[0] - a[1] * b[1], a[0] * b[1] + a[1] * b[0]


def store_halves(ref, v):
    hi, lo = halves(v)
    ref[0] = hi
    ref[1] = lo


def of(factors, which):
    return [factors[16 * which + 8 * part : 16 * which + 8 * part + 8] for part in range(2)]


def by_row(n):
    return iota2(256, n, 0)


def prepare_lanes(ylo, factors, right1):
    i, j = iota2(256, 256, 0), iota2(256, 256, 1)
    low, high = of(factors, 0), of(factors, 1)
    k = (by_row(8) // 32) % 4
    on_k = one_hot(256, 8, k)
    from_k = one_hot(256, 8, jnp.where((ylo == 1) & (k % 2 == 0), 2 - k, k))
    on_top = one_hot(256, 8, (by_row(8) // 8) % 4)
    on_s = one_hot(256, 8, by_row(8) % 8)
    turn = lambda hot, m, to: spread(hot, m.T, to)
    a = [turn(from_k, m, on_k) for m in high]
    b = times([turn(on_top, m, on_top) for m in high], [turn(on_s, m, on_s) for m in low])
    value = times(a, (b[0], -b[1]))
    same, lower = i // 128 == j // 128, i > j
    store_halves(right1, jnp.where(same, value[0], jnp.where(lower, -value[1], value[1])))


def prepare_rows(z, factors, small, right2, left, late_ref):
    i, j = iota2(256, 256, 0), iota2(256, 256, 1)
    low = of(factors, 0)
    out_g = one_hot(256, 16, by_row(16) // 16)
    in_g = one_hot(256, 16, (by_row(16) // 16 + 2 * z) % 16)
    u = [spread(out_g, small[part], in_g) for part in range(2)]
    same, lower = (i // 8) % 2 == (j // 8) % 2, (i // 8) % 2 > (j // 8) % 2
    value = jnp.where(same, u[0], jnp.where(lower, -u[1], u[1]))
    store_halves(right2, jnp.where(i % 8 == j % 8, value, 0.0))
    on_s = one_hot(256, 8, by_row(8) % 8)
    low = [spread(on_s, m, on_s) for m in low]
    real = lambda value: KEEP * jnp.where(same, value[0], jnp.where(lower, value[1], -value[1]))
    store_halves(left, real(times(u, low)))
    n = (by_row(16) // 16) % 4
    in_g = one_hot(256, 16, (n + jnp.where(n < 2, 2, 12) + 2 * z) % 16)
    u = [spread(out_g, small[part], in_g) for part in range(2)]
    hi, lo = (v.astype(jnp.float32) for v in halves(real(times(u, low))))
    segment = j // 64
    late_ref[...] = jnp.where(segment == 3, 0.0, jnp.where(segment == 1, lo, hi)).astype(jnp.bfloat16)


def on_lanes(f_ref, right1, g, n, g2, n2):
    here = (pl.ds(g, n), pl.ds(g2, n2))
    v = jnp.concatenate([f_ref[(*here, part)].reshape(n * n2 * 8, 128) for part in range(2)], axis=1)
    v = dot3(halves(v), (right1[0], right1[1]))
    for part in range(2):
        f_ref[(*here, part)] = v[:, 128 * part : 128 * part + 128].reshape(n, n2, 8, 128)


def rotate_kernel(early_ref, late_ref, matrix_ref, sums_ref, re_ref, im_ref, purity_ref, purity, stage, product, sem, purity_sem):
    r, c = lax.axis_index("row"), lax.axis_index("col")
    sums = sums_ref[...]
    lane = lanes((1, 128))
    total, trace_re, trace_im = (jnp.sum(jnp.where(lane == n, sums, 0.0)) for n in range(3))
    dim = GATE * GATE * LOW
    shifts = (jnp.where(r == c, MIX * trace_re / dim, 0.0), jnp.where(r == c, MIX * trace_im / dim, 0.0))
    squared = trace_re * trace_re + trace_im * trace_im
    purity[0, 0] = (KEEP * KEEP * total + (2 * KEEP * MIX + MIX * MIX) * squared / dim) / (dim * dim)
    matrix = matrix_ref[...]
    sublane = lax.broadcasted_iota(jnp.int32, (8, 128), 0)
    v = jnp.concatenate([late_ref[:, n].reshape(64, 128) for n in range(16)], axis=1)
    hi, lo = halves(v)
    product[...] = dot(matrix, jnp.concatenate([hi, hi, lo, jnp.zeros_like(hi)], axis=0))
    copies = [pltpu.make_async_copy(purity, purity_ref, purity_sem)]
    copies[0].start()
    for q in range(4):
        for g in range(16):
            for part in range(2):
                for k in range(4):
                    row, col = 16 * g + 8 * part, 128 * k
                    tile = early_ref[q, row : row + 8, col : col + 128]
                    tile = tile + product[row : row + 8, 512 * q + col : 512 * q + col + 128]
                    if g // 4 == q:
                        tile = tile + jnp.where(lanes() == sublane + (32 * (g % 4) + 8 * k), shifts[part], 0.0)
                    stage[part, q, 32 * g + 8 * k : 32 * g + 8 * k + 8] = tile
        for part, ref in ((0, re_ref), (1, im_ref)):
            copies.append(pltpu.make_async_copy(stage.at[part, q], ref.at[:, pl.ds(128 * q, 128)], sem.at[part, q]))
            copies[-1].start()
    for copy in copies:
        copy.wait()


def rotate_call(*args):
    f32 = jnp.float32
    vmem, hbm = pl.BlockSpec(memory_space=pltpu.VMEM), pl.BlockSpec(memory_space=pltpu.HBM)
    return pl.pallas_call(
        rotate_kernel,
        name="rotate",
        out_shape=(
            jax.ShapeDtypeStruct((512, 512), f32),
            jax.ShapeDtypeStruct((512, 512), f32),
            jax.ShapeDtypeStruct((1, 1), f32),
        ),
        in_specs=[vmem] * 4,
        out_specs=(hbm, hbm, hbm),
        scratch_shapes=[
            pltpu.SMEM((1, 1), f32),
            pltpu.VMEM((2, 4, 512, 128), f32),
            pltpu.VMEM((256, 2048), f32),
            pltpu.SemaphoreType.DMA((2, 4)),
            pltpu.SemaphoreType.DMA,
        ],
        compiler_params=pltpu.CompilerParams(vmem_limit_bytes=20 * 2**20),
    )(*args)


def on_device(rho_real, rho_imag, gate_real_matrix, gate_imaginary, angles, targets, gate_order):
    args = (rho_real, rho_imag, gate_real_matrix, gate_imaginary, angles.T, targets, gate_order)
    found = exchange_call(*(pltpu.with_memory_space_constraint(v, pltpu.HBM) for v in args))
    re, im, purity = rotate_call(*found)
    return re, im, purity.reshape(())


def solution(mesh):
    return jax.shard_map(
        on_device,
        mesh=mesh,
        in_specs=(P("row", "col"), P("row", "col"), P(), P(), P(), P(), P()),
        out_specs=(P("row", "col"), P("row", "col"), P()),
        check_vma=False,
    )
```

```python
import functools

import jax
import jax.numpy as jnp
from jax import lax
from jax.experimental import pallas as pl
from jax.experimental.pallas import tpu as pltpu
from jax.sharding import PartitionSpec as P

MESH = pl.DeviceIdType.MESH
HIGHEST = lax.Precision.HIGHEST
MIX = 0.25
KEEP = 1 - MIX
GATE = 16
LOW = 32
GATES = 8
BLOCK = (2, 8, 128)


def ring(v):
    v %= 8
    return min(v, 8 - v)


STEPS = [4, 3, -3, 2, -2, 1, -1, 0]
ORDER = [(d_, k_) for d_ in STEPS[:5] for k_ in (0, 1)] + [(d_, k_) for k_ in (0, 1) for d_ in (1, -1)] + [(0, 0), (0, 1)]
UNITS = [
    [(d_, k_) for d_, k_ in ORDER if ring(b_ - d_) >= ring(d_) + k_] for b_ in range(8)
]
BESIDE = {2: (1, 0), 3: (-1, 0)}
UNITS[0] = [u_ for u_ in UNITS[0] if u_ not in BESIDE.values()] + [None, None]
CHIPS = sorted(((jx, jy) for jx in range(4) for jy in range(4) if jx or jy), key=lambda j: (min(j[0], 4 - j[0]) + min(j[1], 4 - j[1]), j))
HOPS = lambda j: min(j[0], 4 - j[0]) + min(j[1], 4 - j[1])
OTHERS = sorted(((jx, jy, jc) for jx, jy in CHIPS for jc in range(2)), key=lambda j: (HOPS(j), j[2], j))
BETAS = [7, 1, 6, 2, 5, 3, 4, 0]
FORWARDS = [
    [(*UNITS[b_][u_], b_) for b_ in BETAS if UNITS[b_][u_] and UNITS[b_][u_][0] != 0] + ([(*BESIDE[u_], 0)] if u_ in BESIDE else [])
    for u_ in range(8)
]
SLOT = {f_: i_ for i_, f_ in enumerate(f_ for fs_ in FORWARDS[1:] for f_ in fs_)}
AHEAD = {1:[2,3],2:[4,5],3:[6],4:[7],5:[]}


def group(dz, kind):
    return 1 + kind if ring(dz) == 1 else 0


def wrap(v, n):
    return jnp.where(v >= n, v - n, v)


def near(v):
    return jnp.minimum(v, 8 - v)


def pick(index, values):
    out = jnp.int32(values[0])
    for i, value in enumerate(values):
        if value != values[0]:
            out = jnp.where(index == i, value, out)
    return out


def lanes(shape=(8, 128)):
    return lax.broadcasted_iota(jnp.int32, shape, 1)


def halve(a, b, mask, shift):
    turned = pltpu.roll(jnp.where(mask, b, a), shift, 1)
    return jnp.where(mask, a, turned), jnp.where(mask, turned, b)


def pack(src, dst, tmp, i):
    low = lanes() < 64
    even = (lanes() // 32) % 2 == 0
    groups = [(4 * i + n, part, q) for n in range(4) for part in range(2) for q in range(4)]
    for n, (h, part, q) in enumerate(groups):
        tiles = [src[part, 32 * h + 8 * k : 32 * h + 8 * k + 8, 128 * q : 128 * q + 128] for k in range(4)]
        for k in range(2):
            tmp[n, k], tmp[n, k + 2] = halve(tiles[k], tiles[k + 2], low, 64)
    for n, (h, part, q) in enumerate(groups):
        for m in range(2):
            at = 16 * h + 4 * q + 2 * m
            dst[at, part], dst[at + 1, part] = halve(tmp[n, 2 * m], tmp[n, 2 * m + 1], even, 32)


def unpack(ref, tmp, rows):
    low = lanes() < 64
    even = (lanes() // 32) % 2 == 0
    groups = [(g, part, q) for g in rows for part in range(2) for q in range(4)]
    for n, (g, part, q) in enumerate(groups):
        for m in range(2):
            tmp[n, m], tmp[n, m + 2] = halve(ref[g, 4 * q + m, part], ref[g, 4 * q + m + 2, part], low, 64)
    for n, (g, part, q) in enumerate(groups):
        for m in range(2):
            a, b = tmp[n, 2 * m], tmp[n, 2 * m + 1]
            ref[g, 4 * q + 2 * m, part] = jnp.where(even, a, pltpu.roll(b, 32, 1))
            ref[g, 4 * q + 2 * m + 1, part] = jnp.where(even, pltpu.roll(a, 96, 1), b)


def exchange_kernel(
    re_hbm, im_hbm, ure_hbm, uim_hbm, angles_hbm, targets_hbm, order_hbm, early_ref, late_ref, matrix_ref, sums_ref,
    own, turned, packed, mu, passing, f_ref, part_sums, plane_sums, small, angles, targets, order, factors, right1, right2, left, turned2, tmp,
    load_sem, small_sem, s1, ru, r1, r1z, s2, r2, sa, ra, sb, rb,
):
    r, c = lax.axis_index("row"), lax.axis_index("col")
    z, ylo = c // 2, c % 2
    rho, core = r // 2, r % 2
    x, y = rho % 4, (rho // 4) * 2 + ylo
    partner = r + 1 - 2 * core
    beta = wrap(rho + 8 - z, 8)
    cores = (core, 1 - core)
    ahead = [wrap(x + jx, 4) * 2 for jx in range(4)]
    behind = [wrap(x + 4 - jx, 4) for jx in range(4)]
    halves_of = lambda yy, top: (jnp.where(yy >= 2, top, 0), jnp.where(yy >= 2, yy - 2, yy))
    up = [halves_of(wrap(y + jy, 4), 8) for jy in range(4)]
    down = [halves_of(wrap(y + 4 - jy, 4), 4) for jy in range(4)]

    def others(fn):
        for j, (jx, jy, jc) in enumerate(OTHERS):
            fn(up[jy][0] + ahead[jx] + 1 - jc, up[jy][1], jnp.where(core == 1, OTHERS.index((jx, jy, 0)), OTHERS.index((jx, jy, 1))))

    def copy(src, dst, send, recv, row, col):
        return pltpu.make_async_remote_copy(src, dst, send, recv, device_id=(row, col), device_id_type=MESH)

    loads = [
        [
            pltpu.make_async_copy(ref.at[pl.ds(128 * i, 128)], own.at[part, pl.ds(128 * i, 128)], load_sem.at[part, i])
            for part, ref in ((0, re_hbm), (1, im_hbm))
        ]
        for i in range(4)
    ]
    barrier = pltpu.get_barrier_semaphore()

    def greet_plane(first, last):
        for j, (jx, jy, jc) in reversed(list(enumerate(OTHERS))):
            if first <= HOPS((jx, jy)) <= last:
                pl.semaphore_signal(
                    barrier, inc=1, device_id=(up[jy][0] + ahead[jx] + cores[jc], 2 * z + up[jy][1]), device_id_type=MESH
                )

    def greet_line(*steps):
        for k in steps:
            for h in (r, partner):
                pl.semaphore_signal(barrier, inc=1, device_id=(h, 2 * wrap(z + k, 8) + ylo), device_id_type=MESH)

    for pair in loads:
        for load in pair:
            load.start()
    greet_plane(4, 4)
    greet_line(4)
    greet_plane(3, 3)
    greet_line(3, 5)
    greet_plane(2, 2)
    greet_line(2, 6)
    greet_plane(1, 1)
    greet_line(1, 7)
    pl.semaphore_signal(barrier, inc=1, device_id=(partner, 2 * z + ylo), device_id_type=MESH)
    smalls = [
        pltpu.make_async_copy(ref, dst, small_sem.at[i])
        for i, (ref, dst) in enumerate(
            (
                (ure_hbm, small.at[0]),
                (uim_hbm, small.at[1]),
                (angles_hbm, angles),
                (targets_hbm, targets),
                (order_hbm, order),
            )
        )
    ]
    for load in smalls:
        load.start()
    for i, pair in enumerate(loads):
        for load in pair:
            load.wait()
        pack(own, packed.at[0], tmp, i)

    pl.semaphore_wait(barrier, 45)

    def at_step(dz):
        zz = wrap(z + dz % 8, 8)
        b = wrap(rho + 8 - zz, 8)
        return zz, b, near(b) >= ring(dz), near(b) > ring(dz)

    def straight(kind):
        for dz in STEPS[:-1]:
            zz, b, direct, also = at_step(dz)
            if kind == 1 and ring(dz) == 4:
                continue
            a = (-dz) % 8

            @pl.when(also if kind else direct)
            def _():
                for h in (r, partner):
                    copy(
                        packed.at[kind, 16 * h + 2 * zz + ylo],
                        f_ref.at[2 * a + ylo, 2 * b + core] if kind else f_ref.at[2 * b + core, 2 * a + ylo],
                        s2,
                        r2.at[group(dz, kind)],
                        h,
                        2 * zz + ylo,
                    ).start()

    def send_unit(u):
        unit = [UNITS[b][u] or (0, 0) for b in range(8)]
        dz = pick(beta, [d % 8 for d, _ in unit])
        kind = pick(beta, [k for _, k in unit])
        zz = wrap(z + dz, 8)
        b = wrap(beta + 8 - dz, 8)
        first, second = jnp.where(kind == 0, core, ylo), jnp.where(kind == 0, ylo, core)
        if u == 0:
            others(lambda h, p, j: copy(packed.at[0, 16 * h + 2 * zz + p], mu.at[j], s1, ru.at[j], h, 2 * z + p).start())
            return

        def passed():
            row = 112 * kind + 16 * pick(beta, [STEPS.index(d) % 7 for d, _ in unit]) + 2 * b + first
            sem = r1.at[pick(beta, [SLOT.get((*unit[bb], bb), 0) for bb in range(8)])]
            others(lambda h, p, j: copy(packed.at[kind, 16 * h + 2 * zz + p], passing.at[row, second], s1, sem, h, 2 * z + p).start())

        def kept():
            row, col = jnp.where(kind == 0, 2 * b + core, ylo), jnp.where(kind == 0, ylo, 2 * b + core)

            def send(h, p, j):
                copy(packed.at[kind, 16 * h + 2 * zz + p], f_ref.at[row, col], s1, r1z, h, 2 * z + p).start()

            others(send)
            send(partner, ylo, 0)
            f_ref[row, col] = packed[kind, 16 * r + 2 * zz + ylo]

        here = [UNITS[bb][u] is not None and UNITS[bb][u][0] == 0 for bb in range(8)]
        away = [UNITS[bb][u] is not None and UNITS[bb][u][0] != 0 for bb in range(8)]
        for which, action in ((away, passed), (here, kept)):
            if all(which):
                action()
            elif any(which):
                pl.when(pick(beta, [int(v) for v in which]) == 1)(action)

        if u in BESIDE:

            @pl.when(beta == 0)
            def _():
                d, k = BESIDE[u]
                zb = wrap(z + d % 8, 8)
                row = 112 * k + 16 * STEPS.index(d) + 2 * (-d % 8) + core
                others(
                    lambda h, p, j: copy(
                        packed.at[k, 16 * h + 2 * zb + p], passing.at[row, ylo], s1, r1.at[SLOT[d, k, 0]], h, 2 * z + p
                    ).start()
                )

    send_unit(0)
    straight(0)
    for i in range(4):
        rows = pl.ds(128 * i, 128)
        for j in range(4):
            there = pl.ds(128 * j, 128)
            turned[0, there, rows] = own[0, rows, there].T
            turned[1, there, rows] = -own[1, rows, there].T
    for i in range(4):
        pack(turned, packed.at[1], tmp, i)
    straight(1)

    def arrived(sem, count):
        copy(packed.at[0, pl.ds(0, count)], packed.at[1, pl.ds(0, count)], sem, sem, r, c).wait_recv()

    def left_all(sem, count):
        copy(packed.at[0, pl.ds(0, count)], packed.at[1, pl.ds(0, count)], sem, sem, r, c).wait_send()

    def either(condition, wait, sem, counts):
        @pl.when(condition)
        def _():
            wait(sem, counts[0])

        @pl.when(jnp.logical_not(condition))
        def _():
            wait(sem, counts[1])

    def share_sums():
        def squares(i, accs):
            for n in range(2):
                rows = pl.ds(pl.multiple_of(16 * i + 8 * n, 8), 8)
                tiles = [own[part, rows, pl.ds(128 * q, 128)] for part in range(2) for q in range(4)]
                accs = [acc + v * v for acc, v in zip(accs, tiles)]
            return accs

        total = jnp.sum(sum(lax.fori_loop(0, 32, squares, [jnp.zeros((8, 128), jnp.float32)] * 8)))
        on_diagonal = lanes((128, 128)) == lax.broadcasted_iota(jnp.int32, (128, 128), 0)
        traces = []
        for part in range(2):
            v = sum(own[part, pl.ds(128 * q, 128), pl.ds(128 * q, 128)] for q in range(4))
            traces.append(jnp.where(r == c, jnp.sum(jnp.where(on_diagonal, v, 0.0)), 0.0))
        lane = lanes((1, 128))
        place = (y * 4 + x) * 2 + core
        part_sums[place] = jnp.where(lane == 0, total, jnp.where(lane == 1, traces[0], jnp.where(lane == 2, traces[1], 0.0)))

        def share(h, p, j):
            copy(part_sums.at[place], part_sums.at[place], sa, ra, h, 2 * z + p).start()

        others(share)
        share(partner, ylo, 0)

    def pass_on():
        for j, (jx, jy, jc) in enumerate(OTHERS):
            if j == 8:
                send_unit(1)
            bs = wrap(wrap(down[jy][0] + behind[jx] + 8 - z, 8), 8)
            dz = pick(bs, [UNITS[b][0][0] % 8 for b in range(8)])
            a, b = wrap(8 - dz, 8), wrap(bs + 8 - dz, 8)
            copy(mu.at[j], mu.at[j], s1, ru.at[j], r, c).wait_recv()
            dst = f_ref.at[2 * b + 1 - jc, 2 * a + down[jy][1]]
            copy(mu.at[j], dst, s2, r2.at[0], r, 2 * wrap(z + dz, 8) + ylo).start()

    def forward(u):
        for dz, kind, bb in FORWARDS[u]:
            n = SLOT[dz, kind, bb]
            a, b = (-dz) % 8, (bb - dz) % 8
            row = 112 * kind + 16 * (STEPS.index(dz) % 7) + 2 * b
            mine = beta == bb

            def onward(full):
                if kind == 0:
                    first, second = (0, 2), (0, 2) if full else (1 - ylo, 1)
                else:
                    first, second = (0, 2) if full else (1 - ylo, 1), (0, 2)
                src = passing.at[pl.ds(row + first[0], first[1]), pl.ds(*second)]
                at = (2 * b, 2 * a) if kind == 0 else (2 * a, 2 * b)
                dst = f_ref.at[pl.ds(at[0] + first[0], first[1]), pl.ds(at[1] + second[0], second[1])]
                copy(src, dst, s2, r2.at[group(dz, kind)], r, 2 * wrap(z + dz % 8, 8) + ylo).start()

            @pl.when(mine)
            def _():
                arrived(r1.at[n], 2)
                onward(False)

            @pl.when(jnp.logical_not(mine))
            def _():
                arrived(r1.at[n], 4)
                onward(True)

    pass_on()
    for load in smalls:
        load.wait()
    for u in range(1, 6):
        for following in AHEAD[u]:
            send_unit(following)
        if u == 2:
            factors[...] = gate_factors(angles[...], targets, order)
        if u == 3:
            share_sums()
        if u == 4:
            prepare_lanes(ylo, factors[...], right1)
        if u == 5:
            prepare_rows(z, factors[...], small, right2, left, matrix_ref)
        forward(u)

    copy(part_sums.at[pl.ds(0, 31)], part_sums.at[pl.ds(0, 31)], sa, ra, r, c).wait_recv()
    plane_sums[z] = jnp.sum(part_sums[...], axis=0)
    for k in range(1, 8):
        copy(plane_sums.at[z], plane_sums.at[z], sb, rb, r, 2 * wrap(z + k, 8) + ylo).start()

    def over_g2(g, out):
        v = jnp.concatenate([f_ref[g + n].reshape(256, 128) for n in range(2)], axis=1)
        v = dot3((right2[0], right2[1]), halves(v))
        for n in range(2):
            out[n] = v[:, 128 * n : 128 * n + 128].reshape((16,) + BLOCK)

    either(beta == 0, arrived, r1z, (59, 58))
    on_lanes(f_ref, right1, 0, 2, 0, 16)
    on_lanes(f_ref, right1, 2, 14, 0, 2)
    turned2[pl.ds(2, 2)] = jnp.zeros((2, 16) + BLOCK, jnp.float32)
    turned2[pl.ds(14, 2)] = jnp.zeros((2, 16) + BLOCK, jnp.float32)
    arrived(r2.at[0], 100)
    for n in range(5):
        on_lanes(f_ref, right1, 4 + 2 * n, 2, 4, 10)
    arrived(r2.at[1], 56)
    on_lanes(f_ref, right1, 2, 14, 2, 2)
    on_lanes(f_ref, right1, 2, 14, 14, 2)
    for g in (0, 4, 6, 8, 10, 12):
        over_g2(g, turned2.at[pl.ds(g, 2)])
    for rows in ((0, 1, 4, 5), (6, 7, 8, 9), (10, 11, 12, 13)):
        unpack(turned2, tmp, rows)
    for n in range(8):
        v = jnp.concatenate([turned2[:, 2 * n + m].reshape(256, 128) for m in range(2)], axis=1)
        early_ref[n // 2, :, 256 * (n % 2) : 256 * (n % 2) + 256] = dot3((left[0], left[1]), halves(v))
    either(beta == 0, left_all, s1, (241, 242))
    left_all(s2, 196)
    copy(plane_sums.at[pl.ds(0, 7)], plane_sums.at[pl.ds(0, 7)], sb, rb, r, c).wait()
    copy(part_sums.at[pl.ds(0, 31)], part_sums.at[pl.ds(0, 31)], sa, ra, r, c).wait_send()
    sums_ref[...] = jnp.sum(plane_sums[...], axis=0)
    arrived(r2.at[2], 40)
    on_lanes(f_ref, right1, 2, 2, 4, 10)
    on_lanes(f_ref, right1, 14, 2, 4, 10)
    over_g2(2, late_ref.at[pl.ds(0, 2)])
    over_g2(14, late_ref.at[pl.ds(2, 2)])
    unpack(late_ref, tmp, range(4))


def exchange_call(*args):
    f32, bf16 = jnp.float32, jnp.bfloat16
    dma = pltpu.SemaphoreType.DMA
    vmem, hbm = pl.BlockSpec(memory_space=pltpu.VMEM), pl.BlockSpec(memory_space=pltpu.HBM)
    blocks = lambda *n: pltpu.VMEM(n + BLOCK, f32)
    return pl.pallas_call(
        exchange_kernel,
        name="exchange",
        out_shape=(
            jax.ShapeDtypeStruct((4, 256, 512), f32),
            jax.ShapeDtypeStruct((4, 16) + BLOCK, f32),
            jax.ShapeDtypeStruct((256, 256), bf16),
            jax.ShapeDtypeStruct((1, 128), f32),
        ),
        in_specs=[hbm] * 7,
        out_specs=(vmem, vmem, vmem, vmem),
        scratch_shapes=[
            pltpu.VMEM((2, 512, 512), f32),
            pltpu.VMEM((2, 512, 512), f32),
            blocks(2, 256),
            blocks(32),
            blocks(224, 2),
            blocks(16, 16),
            pltpu.VMEM((32, 1, 128), f32),
            pltpu.VMEM((8, 1, 128), f32),
            pltpu.VMEM((2, 16, 16), f32),
            pltpu.VMEM((3, 8), f32),
            pltpu.SMEM((8,), jnp.int32),
            pltpu.SMEM((8,), jnp.int32),
            pltpu.VMEM((32, 8), f32),
            pltpu.VMEM((2, 256, 256), bf16),
            pltpu.VMEM((2, 256, 256), bf16),
            pltpu.VMEM((2, 256, 256), bf16),
            blocks(16, 16),
            pltpu.VMEM((32, 4, 8, 128), f32),
            dma((2, 4)),
            dma((5,)),
            dma,
            dma((32,)),
            dma((len(SLOT),)),
            dma,
            dma,
            dma((3,)),
            dma,
            dma,
            dma,
            dma,
        ],
        compiler_params=pltpu.CompilerParams(collective_id=0, has_side_effects=True, vmem_limit_bytes=40 * 2**20),
    )(*args)


def iota2(n, m, dim):
    return lax.broadcasted_iota(jnp.int32, (n, m), dim)


def halves(v):
    hi = v.astype(jnp.bfloat16)
    return hi, (v - hi.astype(jnp.float32)).astype(jnp.bfloat16)


def dot(a, b):
    return jnp.dot(a, b, preferred_element_type=jnp.float32)


def dot3(a, b):
    return dot(a[0], b[0]) + dot(a[0], b[1]) + dot(a[1], b[0])


def gate_factors(angles, targets, order):
    theta, alpha, beta = angles[0:1], angles[1:2], angles[2:3]
    cos, sin = jnp.cos(theta / 2), jnp.sin(theta / 2)
    both = alpha + beta
    elements = (
        (cos, cos * 0.0),
        (-jnp.cos(beta) * sin, -jnp.sin(beta) * sin),
        (jnp.cos(alpha) * sin, jnp.sin(alpha) * sin),
        (jnp.cos(both) * cos, jnp.sin(both) * cos),
    )
    i, j = iota2(32, 32, 0), iota2(32, 32, 1)
    left, right, high = i % 8, j % 8, i >= 16
    same_part, lower, same_factor = (i // 8) % 2 == (j // 8) % 2, i > j, i // 16 == j // 16
    gates = lax.broadcasted_iota(jnp.int32, (1, GATES), 1)
    total = jnp.where((iota2(32, 8, 0) % 16) == iota2(32, 8, 1), 1.0, 0.0)
    for position in range(GATES):
        gate = order[position]
        target = targets[gate]
        low_bit = jnp.where(target == 0, 1, jnp.where(target == 1, 2, jnp.where(target == 2, 4, 0)))
        high_bit = jnp.where(target == 3, 1, jnp.where(target == 4, 2, 0))
        bit = jnp.where(high, high_bit, low_bit)
        entry = [
            [jnp.sum(jnp.where(gates == gate, e, 0.0), axis=1, keepdims=True) for e in pair] for pair in elements
        ]
        left_high, right_high = (left & bit) > 0, (right & bit) > 0
        same_rest = ((left ^ right) | bit) == bit
        step = [
            jnp.where(
                left_high,
                jnp.where(right_high, entry[3][part], entry[2][part]),
                jnp.where(right_high, entry[1][part], entry[0][part]),
            )
            for part in range(2)
        ]
        step = [jnp.where(bit > 0, v, one) for v, one in zip(step, (1.0, 0.0))]
        step = jnp.where(same_part, step[0], jnp.where(lower, step[1], -step[1]))
        step = jnp.where(same_rest & same_factor, step, 0.0)
        total = jnp.dot(step, total, precision=HIGHEST, preferred_element_type=jnp.float32)
    return total


def one_hot(n, m, index):
    return jnp.where(index == iota2(n, m, 1), 1.0, 0.0)


def spread(rows, small, cols):
    wide = jnp.dot(rows, small, precision=HIGHEST, preferred_element_type=jnp.float32)
    return lax.dot_general(wide, cols, (((1,), (1,)), ((), ())), precision=HIGHEST, preferred_element_type=jnp.float32)


def times(a, b):
    return a[0] * b[0] - a[1] * b[1], a[0] * b[1] + a[1] * b[0]


def store_halves(ref, v):
    hi, lo = halves(v)
    ref[0] = hi
    ref[1] = lo


def of(factors, which):
    return [factors[16 * which + 8 * part : 16 * which + 8 * part + 8] for part in range(2)]


def by_row(n):
    return iota2(256, n, 0)


def prepare_lanes(ylo, factors, right1):
    i, j = iota2(256, 256, 0), iota2(256, 256, 1)
    low, high = of(factors, 0), of(factors, 1)
    k = (by_row(8) // 32) % 4
    on_k = one_hot(256, 8, k)
    from_k = one_hot(256, 8, jnp.where((ylo == 1) & (k % 2 == 0), 2 - k, k))
    on_top = one_hot(256, 8, (by_row(8) // 8) % 4)
    on_s = one_hot(256, 8, by_row(8) % 8)
    turn = lambda hot, m, to: spread(hot, m.T, to)
    a = [turn(from_k, m, on_k) for m in high]
    b = times([turn(on_top, m, on_top) for m in high], [turn(on_s, m, on_s) for m in low])
    value = times(a, (b[0], -b[1]))
    same, lower = i // 128 == j // 128, i > j
    store_halves(right1, jnp.where(same, value[0], jnp.where(lower, -value[1], value[1])))


def prepare_rows(z, factors, small, right2, left, late_ref):
    i, j = iota2(256, 256, 0), iota2(256, 256, 1)
    low = of(factors, 0)
    out_g = one_hot(256, 16, by_row(16) // 16)
    in_g = one_hot(256, 16, (by_row(16) // 16 + 2 * z) % 16)
    u = [spread(out_g, small[part], in_g) for part in range(2)]
    same, lower = (i // 8) % 2 == (j // 8) % 2, (i // 8) % 2 > (j // 8) % 2
    value = jnp.where(same, u[0], jnp.where(lower, -u[1], u[1]))
    store_halves(right2, jnp.where(i % 8 == j % 8, value, 0.0))
    on_s = one_hot(256, 8, by_row(8) % 8)
    low = [spread(on_s, m, on_s) for m in low]
    real = lambda value: KEEP * jnp.where(same, value[0], jnp.where(lower, value[1], -value[1]))
    store_halves(left, real(times(u, low)))
    n = (by_row(16) // 16) % 4
    in_g = one_hot(256, 16, (n + jnp.where(n < 2, 2, 12) + 2 * z) % 16)
    u = [spread(out_g, small[part], in_g) for part in range(2)]
    hi, lo = (v.astype(jnp.float32) for v in halves(real(times(u, low))))
    segment = j // 64
    late_ref[...] = jnp.where(segment == 3, 0.0, jnp.where(segment == 1, lo, hi)).astype(jnp.bfloat16)


def on_lanes(f_ref, right1, g, n, g2, n2):
    here = (pl.ds(g, n), pl.ds(g2, n2))
    v = jnp.concatenate([f_ref[(*here, part)].reshape(n * n2 * 8, 128) for part in range(2)], axis=1)
    v = dot3(halves(v), (right1[0], right1[1]))
    for part in range(2):
        f_ref[(*here, part)] = v[:, 128 * part : 128 * part + 128].reshape(n, n2, 8, 128)


def rotate_kernel(early_ref, late_ref, matrix_ref, sums_ref, re_ref, im_ref, purity_ref, purity, stage, product, sem, purity_sem):
    r, c = lax.axis_index("row"), lax.axis_index("col")
    sums = sums_ref[...]
    lane = lanes((1, 128))
    total, trace_re, trace_im = (jnp.sum(jnp.where(lane == n, sums, 0.0)) for n in range(3))
    dim = GATE * GATE * LOW
    shifts = (jnp.where(r == c, MIX * trace_re / dim, 0.0), jnp.where(r == c, MIX * trace_im / dim, 0.0))
    squared = trace_re * trace_re + trace_im * trace_im
    purity[0, 0] = (KEEP * KEEP * total + (2 * KEEP * MIX + MIX * MIX) * squared / dim) / (dim * dim)
    matrix = matrix_ref[...]
    sublane = lax.broadcasted_iota(jnp.int32, (8, 128), 0)
    v = jnp.concatenate([late_ref[:, n].reshape(64, 128) for n in range(16)], axis=1)
    hi, lo = halves(v)
    product[...] = dot(matrix, jnp.concatenate([hi, hi, lo, jnp.zeros_like(hi)], axis=0))
    copies = [pltpu.make_async_copy(purity, purity_ref, purity_sem)]
    copies[0].start()
    for q in range(4):
        for g in range(16):
            for part in range(2):
                for k in range(4):
                    row, col = 16 * g + 8 * part, 128 * k
                    tile = early_ref[q, row : row + 8, col : col + 128]
                    tile = tile + product[row : row + 8, 512 * q + col : 512 * q + col + 128]
                    if g // 4 == q:
                        tile = tile + jnp.where(lanes() == sublane + (32 * (g % 4) + 8 * k), shifts[part], 0.0)
                    stage[part, q, 32 * g + 8 * k : 32 * g + 8 * k + 8] = tile
        for part, ref in ((0, re_ref), (1, im_ref)):
            copies.append(pltpu.make_async_copy(stage.at[part, q], ref.at[:, pl.ds(128 * q, 128)], sem.at[part, q]))
            copies[-1].start()
    for copy in copies:
        copy.wait()


def rotate_call(*args):
    f32 = jnp.float32
    vmem, hbm = pl.BlockSpec(memory_space=pltpu.VMEM), pl.BlockSpec(memory_space=pltpu.HBM)
    return pl.pallas_call(
        rotate_kernel,
        name="rotate",
        out_shape=(
            jax.ShapeDtypeStruct((512, 512), f32),
            jax.ShapeDtypeStruct((512, 512), f32),
            jax.ShapeDtypeStruct((1, 1), f32),
        ),
        in_specs=[vmem] * 4,
        out_specs=(hbm, hbm, hbm),
        scratch_shapes=[
            pltpu.SMEM((1, 1), f32),
            pltpu.VMEM((2, 4, 512, 128), f32),
            pltpu.VMEM((256, 2048), f32),
            pltpu.SemaphoreType.DMA((2, 4)),
            pltpu.SemaphoreType.DMA,
        ],
        compiler_params=pltpu.CompilerParams(vmem_limit_bytes=20 * 2**20),
    )(*args)


def on_device(rho_real, rho_imag, gate_real_matrix, gate_imaginary, angles, targets, gate_order):
    args = (rho_real, rho_imag, gate_real_matrix, gate_imaginary, angles.T, targets, gate_order)
    found = exchange_call(*(pltpu.with_memory_space_constraint(v, pltpu.HBM) for v in args))
    re, im, purity = rotate_call(*found)
    return re, im, purity.reshape(())


def solution(mesh):
    return jax.shard_map(
        on_device,
        mesh=mesh,
        in_specs=(P("row", "col"), P("row", "col"), P(), P(), P(), P(), P()),
        out_specs=(P("row", "col"), P("row", "col"), P()),
        check_vma=False,
    )
```

```python
import functools

import jax
import jax.numpy as jnp
from jax import lax
from jax.experimental import pallas as pl
from jax.experimental.pallas import tpu as pltpu
from jax.sharding import PartitionSpec as P

MESH = pl.DeviceIdType.MESH
HIGHEST = lax.Precision.HIGHEST
MIX = 0.25
KEEP = 1 - MIX
GATE = 16
LOW = 32
GATES = 8
BLOCK = (2, 8, 128)


def ring(v):
    v %= 8
    return min(v, 8 - v)


STEPS = [4, 3, -3, 2, -2, 1, -1, 0]
ORDER = [(d_, k_) for d_ in STEPS[:5] for k_ in (0, 1)] + [(d_, k_) for k_ in (0, 1) for d_ in (1, -1)] + [(0, 0), (0, 1)]
UNITS = [
    [(d_, k_) for d_, k_ in ORDER if ring(b_ - d_) >= ring(d_) + k_] for b_ in range(8)
]
BESIDE = {2: (1, 0), 3: (-1, 0)}
UNITS[0] = [u_ for u_ in UNITS[0] if u_ not in BESIDE.values()] + [None, None]
CHIPS = sorted(((jx, jy) for jx in range(4) for jy in range(4) if jx or jy), key=lambda j: (min(j[0], 4 - j[0]) + min(j[1], 4 - j[1]), j))
HOPS = lambda j: min(j[0], 4 - j[0]) + min(j[1], 4 - j[1])
OTHERS = sorted(((jx, jy, jc) for jx, jy in CHIPS for jc in range(2)), key=lambda j: (HOPS(j), j[2], j))
BETAS = [7, 1, 6, 2, 5, 3, 4, 0]
FORWARDS = [
    [(*UNITS[b_][u_], b_) for b_ in BETAS if UNITS[b_][u_] and UNITS[b_][u_][0] != 0] + ([(*BESIDE[u_], 0)] if u_ in BESIDE else [])
    for u_ in range(8)
]
SLOT = {f_: i_ for i_, f_ in enumerate(f_ for fs_ in FORWARDS[1:] for f_ in fs_)}
AHEAD = {1:[2,3],2:[4],3:[5,6],4:[7],5:[]}


def group(dz, kind):
    return 1 + kind if ring(dz) == 1 else 0


def wrap(v, n):
    return jnp.where(v >= n, v - n, v)


def near(v):
    return jnp.minimum(v, 8 - v)


def pick(index, values):
    out = jnp.int32(values[0])
    for i, value in enumerate(values):
        if value != values[0]:
            out = jnp.where(index == i, value, out)
    return out


def lanes(shape=(8, 128)):
    return lax.broadcasted_iota(jnp.int32, shape, 1)


def halve(a, b, mask, shift):
    turned = pltpu.roll(jnp.where(mask, b, a), shift, 1)
    return jnp.where(mask, a, turned), jnp.where(mask, turned, b)


def pack(src, dst, tmp, i):
    low = lanes() < 64
    even = (lanes() // 32) % 2 == 0
    groups = [(4 * i + n, part, q) for n in range(4) for part in range(2) for q in range(4)]
    for n, (h, part, q) in enumerate(groups):
        tiles = [src[part, 32 * h + 8 * k : 32 * h + 8 * k + 8, 128 * q : 128 * q + 128] for k in range(4)]
        for k in range(2):
            tmp[n, k], tmp[n, k + 2] = halve(tiles[k], tiles[k + 2], low, 64)
    for n, (h, part, q) in enumerate(groups):
        for m in range(2):
            at = 16 * h + 4 * q + 2 * m
            dst[at, part], dst[at + 1, part] = halve(tmp[n, 2 * m], tmp[n, 2 * m + 1], even, 32)


def unpack(ref, tmp, rows):
    low = lanes() < 64
    even = (lanes() // 32) % 2 == 0
    groups = [(g, part, q) for g in rows for part in range(2) for q in range(4)]
    for n, (g, part, q) in enumerate(groups):
        for m in range(2):
            tmp[n, m], tmp[n, m + 2] = halve(ref[g, 4 * q + m, part], ref[g, 4 * q + m + 2, part], low, 64)
    for n, (g, part, q) in enumerate(groups):
        for m in range(2):
            a, b = tmp[n, 2 * m], tmp[n, 2 * m + 1]
            ref[g, 4 * q + 2 * m, part] = jnp.where(even, a, pltpu.roll(b, 32, 1))
            ref[g, 4 * q + 2 * m + 1, part] = jnp.where(even, pltpu.roll(a, 96, 1), b)


def exchange_kernel(
    re_hbm, im_hbm, ure_hbm, uim_hbm, angles_hbm, targets_hbm, order_hbm, early_ref, late_ref, matrix_ref, sums_ref,
    own, turned, packed, mu, passing, f_ref, part_sums, plane_sums, small, angles, targets, order, factors, right1, right2, left, turned2, tmp,
    load_sem, small_sem, s1, ru, r1, r1z, s2, r2, sa, ra, sb, rb,
):
    r, c = lax.axis_index("row"), lax.axis_index("col")
    z, ylo = c // 2, c % 2
    rho, core = r // 2, r % 2
    x, y = rho % 4, (rho // 4) * 2 + ylo
    partner = r + 1 - 2 * core
    beta = wrap(rho + 8 - z, 8)
    cores = (core, 1 - core)
    ahead = [wrap(x + jx, 4) * 2 for jx in range(4)]
    behind = [wrap(x + 4 - jx, 4) for jx in range(4)]
    halves_of = lambda yy, top: (jnp.where(yy >= 2, top, 0), jnp.where(yy >= 2, yy - 2, yy))
    up = [halves_of(wrap(y + jy, 4), 8) for jy in range(4)]
    down = [halves_of(wrap(y + 4 - jy, 4), 4) for jy in range(4)]

    def others(fn):
        for j, (jx, jy, jc) in enumerate(OTHERS):
            fn(up[jy][0] + ahead[jx] + 1 - jc, up[jy][1], jnp.where(core == 1, OTHERS.index((jx, jy, 0)), OTHERS.index((jx, jy, 1))))

    def copy(src, dst, send, recv, row, col):
        return pltpu.make_async_remote_copy(src, dst, send, recv, device_id=(row, col), device_id_type=MESH)

    loads = [
        [
            pltpu.make_async_copy(ref.at[pl.ds(128 * i, 128)], own.at[part, pl.ds(128 * i, 128)], load_sem.at[part, i])
            for part, ref in ((0, re_hbm), (1, im_hbm))
        ]
        for i in range(4)
    ]
    barrier = pltpu.get_barrier_semaphore()

    def greet_plane(first, last):
        for j, (jx, jy, jc) in reversed(list(enumerate(OTHERS))):
            if first <= HOPS((jx, jy)) <= last:
                pl.semaphore_signal(
                    barrier, inc=1, device_id=(up[jy][0] + ahead[jx] + cores[jc], 2 * z + up[jy][1]), device_id_type=MESH
                )

    def greet_line(*steps):
        for k in steps:
            for h in (r, partner):
                pl.semaphore_signal(barrier, inc=1, device_id=(h, 2 * wrap(z + k, 8) + ylo), device_id_type=MESH)

    for pair in loads:
        for load in pair:
            load.start()
    greet_plane(4, 4)
    greet_line(4)
    greet_plane(3, 3)
    greet_line(3, 5)
    greet_plane(2, 2)
    greet_line(2, 6)
    greet_plane(1, 1)
    greet_line(1, 7)
    pl.semaphore_signal(barrier, inc=1, device_id=(partner, 2 * z + ylo), device_id_type=MESH)
    smalls = [
        pltpu.make_async_copy(ref, dst, small_sem.at[i])
        for i, (ref, dst) in enumerate(
            (
                (ure_hbm, small.at[0]),
                (uim_hbm, small.at[1]),
                (angles_hbm, angles),
                (targets_hbm, targets),
                (order_hbm, order),
            )
        )
    ]
    for load in smalls:
        load.start()
    for i, pair in enumerate(loads):
        for load in pair:
            load.wait()
        pack(own, packed.at[0], tmp, i)

    pl.semaphore_wait(barrier, 45)

    def at_step(dz):
        zz = wrap(z + dz % 8, 8)
        b = wrap(rho + 8 - zz, 8)
        return zz, b, near(b) >= ring(dz), near(b) > ring(dz)

    def straight(kind):
        for dz in STEPS[:-1]:
            zz, b, direct, also = at_step(dz)
            if kind == 1 and ring(dz) == 4:
                continue
            a = (-dz) % 8

            @pl.when(also if kind else direct)
            def _():
                for h in (r, partner):
                    copy(
                        packed.at[kind, 16 * h + 2 * zz + ylo],
                        f_ref.at[2 * a + ylo, 2 * b + core] if kind else f_ref.at[2 * b + core, 2 * a + ylo],
                        s2,
                        r2.at[group(dz, kind)],
                        h,
                        2 * zz + ylo,
                    ).start()

    def send_unit(u):
        unit = [UNITS[b][u] or (0, 0) for b in range(8)]
        dz = pick(beta, [d % 8 for d, _ in unit])
        kind = pick(beta, [k for _, k in unit])
        zz = wrap(z + dz, 8)
        b = wrap(beta + 8 - dz, 8)
        first, second = jnp.where(kind == 0, core, ylo), jnp.where(kind == 0, ylo, core)
        if u == 0:
            others(lambda h, p, j: copy(packed.at[0, 16 * h + 2 * zz + p], mu.at[j], s1, ru.at[j], h, 2 * z + p).start())
            return

        def passed():
            row = 112 * kind + 16 * pick(beta, [STEPS.index(d) % 7 for d, _ in unit]) + 2 * b + first
            sem = r1.at[pick(beta, [SLOT.get((*unit[bb], bb), 0) for bb in range(8)])]
            others(lambda h, p, j: copy(packed.at[kind, 16 * h + 2 * zz + p], passing.at[row, second], s1, sem, h, 2 * z + p).start())

        def kept():
            row, col = jnp.where(kind == 0, 2 * b + core, ylo), jnp.where(kind == 0, ylo, 2 * b + core)

            def send(h, p, j):
                copy(packed.at[kind, 16 * h + 2 * zz + p], f_ref.at[row, col], s1, r1z, h, 2 * z + p).start()

            others(send)
            send(partner, ylo, 0)
            f_ref[row, col] = packed[kind, 16 * r + 2 * zz + ylo]

        here = [UNITS[bb][u] is not None and UNITS[bb][u][0] == 0 for bb in range(8)]
        away = [UNITS[bb][u] is not None and UNITS[bb][u][0] != 0 for bb in range(8)]
        for which, action in ((away, passed), (here, kept)):
            if all(which):
                action()
            elif any(which):
                pl.when(pick(beta, [int(v) for v in which]) == 1)(action)

        if u in BESIDE:

            @pl.when(beta == 0)
            def _():
                d, k = BESIDE[u]
                zb = wrap(z + d % 8, 8)
                row = 112 * k + 16 * STEPS.index(d) + 2 * (-d % 8) + core
                others(
                    lambda h, p, j: copy(
                        packed.at[k, 16 * h + 2 * zb + p], passing.at[row, ylo], s1, r1.at[SLOT[d, k, 0]], h, 2 * z + p
                    ).start()
                )

    send_unit(0)
    straight(0)
    for i in range(4):
        rows = pl.ds(128 * i, 128)
        for j in range(4):
            there = pl.ds(128 * j, 128)
            turned[0, there, rows] = own[0, rows, there].T
            turned[1, there, rows] = -own[1, rows, there].T
    for i in range(4):
        pack(turned, packed.at[1], tmp, i)
    straight(1)

    def arrived(sem, count):
        copy(packed.at[0, pl.ds(0, count)], packed.at[1, pl.ds(0, count)], sem, sem, r, c).wait_recv()

    def left_all(sem, count):
        copy(packed.at[0, pl.ds(0, count)], packed.at[1, pl.ds(0, count)], sem, sem, r, c).wait_send()

    def either(condition, wait, sem, counts):
        @pl.when(condition)
        def _():
            wait(sem, counts[0])

        @pl.when(jnp.logical_not(condition))
        def _():
            wait(sem, counts[1])

    def share_sums():
        def squares(i, accs):
            for n in range(2):
                rows = pl.ds(pl.multiple_of(16 * i + 8 * n, 8), 8)
                tiles = [own[part, rows, pl.ds(128 * q, 128)] for part in range(2) for q in range(4)]
                accs = [acc + v * v for acc, v in zip(accs, tiles)]
            return accs

        total = jnp.sum(sum(lax.fori_loop(0, 32, squares, [jnp.zeros((8, 128), jnp.float32)] * 8)))
        on_diagonal = lanes((128, 128)) == lax.broadcasted_iota(jnp.int32, (128, 128), 0)
        traces = []
        for part in range(2):
            v = sum(own[part, pl.ds(128 * q, 128), pl.ds(128 * q, 128)] for q in range(4))
            traces.append(jnp.where(r == c, jnp.sum(jnp.where(on_diagonal, v, 0.0)), 0.0))
        lane = lanes((1, 128))
        place = (y * 4 + x) * 2 + core
        part_sums[place] = jnp.where(lane == 0, total, jnp.where(lane == 1, traces[0], jnp.where(lane == 2, traces[1], 0.0)))

        def share(h, p, j):
            copy(part_sums.at[place], part_sums.at[place], sa, ra, h, 2 * z + p).start()

        others(share)
        share(partner, ylo, 0)

    def pass_on():
        for j, (jx, jy, jc) in enumerate(OTHERS):
            if j == 6:
                send_unit(1)
            bs = wrap(wrap(down[jy][0] + behind[jx] + 8 - z, 8), 8)
            dz = pick(bs, [UNITS[b][0][0] % 8 for b in range(8)])
            a, b = wrap(8 - dz, 8), wrap(bs + 8 - dz, 8)
            copy(mu.at[j], mu.at[j], s1, ru.at[j], r, c).wait_recv()
            dst = f_ref.at[2 * b + 1 - jc, 2 * a + down[jy][1]]
            copy(mu.at[j], dst, s2, r2.at[0], r, 2 * wrap(z + dz, 8) + ylo).start()

    def forward(u):
        for dz, kind, bb in FORWARDS[u]:
            n = SLOT[dz, kind, bb]
            a, b = (-dz) % 8, (bb - dz) % 8
            row = 112 * kind + 16 * (STEPS.index(dz) % 7) + 2 * b
            mine = beta == bb

            def onward(full):
                if kind == 0:
                    first, second = (0, 2), (0, 2) if full else (1 - ylo, 1)
                else:
                    first, second = (0, 2) if full else (1 - ylo, 1), (0, 2)
                src = passing.at[pl.ds(row + first[0], first[1]), pl.ds(*second)]
                at = (2 * b, 2 * a) if kind == 0 else (2 * a, 2 * b)
                dst = f_ref.at[pl.ds(at[0] + first[0], first[1]), pl.ds(at[1] + second[0], second[1])]
                copy(src, dst, s2, r2.at[group(dz, kind)], r, 2 * wrap(z + dz % 8, 8) + ylo).start()

            @pl.when(mine)
            def _():
                arrived(r1.at[n], 2)
                onward(False)

            @pl.when(jnp.logical_not(mine))
            def _():
                arrived(r1.at[n], 4)
                onward(True)

    pass_on()
    for load in smalls:
        load.wait()
    for u in range(1, 6):
        for following in AHEAD[u]:
            send_unit(following)
        if u == 2:
            factors[...] = gate_factors(angles[...], targets, order)
        if u == 3:
            share_sums()
        if u == 4:
            prepare_lanes(ylo, factors[...], right1)
        if u == 5:
            prepare_rows(z, factors[...], small, right2, left, matrix_ref)
        forward(u)

    copy(part_sums.at[pl.ds(0, 31)], part_sums.at[pl.ds(0, 31)], sa, ra, r, c).wait_recv()
    plane_sums[z] = jnp.sum(part_sums[...], axis=0)
    for k in range(1, 8):
        copy(plane_sums.at[z], plane_sums.at[z], sb, rb, r, 2 * wrap(z + k, 8) + ylo).start()

    def over_g2(g, out):
        v = jnp.concatenate([f_ref[g + n].reshape(256, 128) for n in range(2)], axis=1)
        v = dot3((right2[0], right2[1]), halves(v))
        for n in range(2):
            out[n] = v[:, 128 * n : 128 * n + 128].reshape((16,) + BLOCK)

    either(beta == 0, arrived, r1z, (59, 58))
    on_lanes(f_ref, right1, 0, 2, 0, 16)
    on_lanes(f_ref, right1, 2, 14, 0, 2)
    turned2[pl.ds(2, 2)] = jnp.zeros((2, 16) + BLOCK, jnp.float32)
    turned2[pl.ds(14, 2)] = jnp.zeros((2, 16) + BLOCK, jnp.float32)
    arrived(r2.at[0], 100)
    for n in range(5):
        on_lanes(f_ref, right1, 4 + 2 * n, 2, 4, 10)
    arrived(r2.at[1], 56)
    on_lanes(f_ref, right1, 2, 14, 2, 2)
    on_lanes(f_ref, right1, 2, 14, 14, 2)
    for g in (0, 4, 6, 8, 10, 12):
        over_g2(g, turned2.at[pl.ds(g, 2)])
    for rows in ((0, 1, 4, 5), (6, 7, 8, 9), (10, 11, 12, 13)):
        unpack(turned2, tmp, rows)
    for n in range(8):
        v = jnp.concatenate([turned2[:, 2 * n + m].reshape(256, 128) for m in range(2)], axis=1)
        early_ref[n // 2, :, 256 * (n % 2) : 256 * (n % 2) + 256] = dot3((left[0], left[1]), halves(v))
    either(beta == 0, left_all, s1, (241, 242))
    left_all(s2, 196)
    copy(plane_sums.at[pl.ds(0, 7)], plane_sums.at[pl.ds(0, 7)], sb, rb, r, c).wait()
    copy(part_sums.at[pl.ds(0, 31)], part_sums.at[pl.ds(0, 31)], sa, ra, r, c).wait_send()
    sums_ref[...] = jnp.sum(plane_sums[...], axis=0)
    arrived(r2.at[2], 40)
    on_lanes(f_ref, right1, 2, 2, 4, 10)
    on_lanes(f_ref, right1, 14, 2, 4, 10)
    over_g2(2, late_ref.at[pl.ds(0, 2)])
    over_g2(14, late_ref.at[pl.ds(2, 2)])
    unpack(late_ref, tmp, range(4))


def exchange_call(*args):
    f32, bf16 = jnp.float32, jnp.bfloat16
    dma = pltpu.SemaphoreType.DMA
    vmem, hbm = pl.BlockSpec(memory_space=pltpu.VMEM), pl.BlockSpec(memory_space=pltpu.HBM)
    blocks = lambda *n: pltpu.VMEM(n + BLOCK, f32)
    return pl.pallas_call(
        exchange_kernel,
        name="exchange",
        out_shape=(
            jax.ShapeDtypeStruct((4, 256, 512), f32),
            jax.ShapeDtypeStruct((4, 16) + BLOCK, f32),
            jax.ShapeDtypeStruct((256, 256), bf16),
            jax.ShapeDtypeStruct((1, 128), f32),
        ),
        in_specs=[hbm] * 7,
        out_specs=(vmem, vmem, vmem, vmem),
        scratch_shapes=[
            pltpu.VMEM((2, 512, 512), f32),
            pltpu.VMEM((2, 512, 512), f32),
            blocks(2, 256),
            blocks(32),
            blocks(224, 2),
            blocks(16, 16),
            pltpu.VMEM((32, 1, 128), f32),
            pltpu.VMEM((8, 1, 128), f32),
            pltpu.VMEM((2, 16, 16), f32),
            pltpu.VMEM((3, 8), f32),
            pltpu.SMEM((8,), jnp.int32),
            pltpu.SMEM((8,), jnp.int32),
            pltpu.VMEM((32, 8), f32),
            pltpu.VMEM((2, 256, 256), bf16),
            pltpu.VMEM((2, 256, 256), bf16),
            pltpu.VMEM((2, 256, 256), bf16),
            blocks(16, 16),
            pltpu.VMEM((32, 4, 8, 128), f32),
            dma((2, 4)),
            dma((5,)),
            dma,
            dma((32,)),
            dma((len(SLOT),)),
            dma,
            dma,
            dma((3,)),
            dma,
            dma,
            dma,
            dma,
        ],
        compiler_params=pltpu.CompilerParams(collective_id=0, has_side_effects=True, vmem_limit_bytes=40 * 2**20),
    )(*args)


def iota2(n, m, dim):
    return lax.broadcasted_iota(jnp.int32, (n, m), dim)


def halves(v):
    hi = v.astype(jnp.bfloat16)
    return hi, (v - hi.astype(jnp.float32)).astype(jnp.bfloat16)


def dot(a, b):
    return jnp.dot(a, b, preferred_element_type=jnp.float32)


def dot3(a, b):
    return dot(a[0], b[0]) + dot(a[0], b[1]) + dot(a[1], b[0])


def gate_factors(angles, targets, order):
    theta, alpha, beta = angles[0:1], angles[1:2], angles[2:3]
    cos, sin = jnp.cos(theta / 2), jnp.sin(theta / 2)
    both = alpha + beta
    elements = (
        (cos, cos * 0.0),
        (-jnp.cos(beta) * sin, -jnp.sin(beta) * sin),
        (jnp.cos(alpha) * sin, jnp.sin(alpha) * sin),
        (jnp.cos(both) * cos, jnp.sin(both) * cos),
    )
    i, j = iota2(32, 32, 0), iota2(32, 32, 1)
    left, right, high = i % 8, j % 8, i >= 16
    same_part, lower, same_factor = (i // 8) % 2 == (j // 8) % 2, i > j, i // 16 == j // 16
    gates = lax.broadcasted_iota(jnp.int32, (1, GATES), 1)
    total = jnp.where((iota2(32, 8, 0) % 16) == iota2(32, 8, 1), 1.0, 0.0)
    for position in range(GATES):
        gate = order[position]
        target = targets[gate]
        low_bit = jnp.where(target == 0, 1, jnp.where(target == 1, 2, jnp.where(target == 2, 4, 0)))
        high_bit = jnp.where(target == 3, 1, jnp.where(target == 4, 2, 0))
        bit = jnp.where(high, high_bit, low_bit)
        entry = [
            [jnp.sum(jnp.where(gates == gate, e, 0.0), axis=1, keepdims=True) for e in pair] for pair in elements
        ]
        left_high, right_high = (left & bit) > 0, (right & bit) > 0
        same_rest = ((left ^ right) | bit) == bit
        step = [
            jnp.where(
                left_high,
                jnp.where(right_high, entry[3][part], entry[2][part]),
                jnp.where(right_high, entry[1][part], entry[0][part]),
            )
            for part in range(2)
        ]
        step = [jnp.where(bit > 0, v, one) for v, one in zip(step, (1.0, 0.0))]
        step = jnp.where(same_part, step[0], jnp.where(lower, step[1], -step[1]))
        step = jnp.where(same_rest & same_factor, step, 0.0)
        total = jnp.dot(step, total, precision=HIGHEST, preferred_element_type=jnp.float32)
    return total


def one_hot(n, m, index):
    return jnp.where(index == iota2(n, m, 1), 1.0, 0.0)


def spread(rows, small, cols):
    wide = jnp.dot(rows, small, precision=HIGHEST, preferred_element_type=jnp.float32)
    return lax.dot_general(wide, cols, (((1,), (1,)), ((), ())), precision=HIGHEST, preferred_element_type=jnp.float32)


def times(a, b):
    return a[0] * b[0] - a[1] * b[1], a[0] * b[1] + a[1] * b[0]


def store_halves(ref, v):
    hi, lo = halves(v)
    ref[0] = hi
    ref[1] = lo


def of(factors, which):
    return [factors[16 * which + 8 * part : 16 * which + 8 * part + 8] for part in range(2)]


def by_row(n):
    return iota2(256, n, 0)


def prepare_lanes(ylo, factors, right1):
    i, j = iota2(256, 256, 0), iota2(256, 256, 1)
    low, high = of(factors, 0), of(factors, 1)
    k = (by_row(8) // 32) % 4
    on_k = one_hot(256, 8, k)
    from_k = one_hot(256, 8, jnp.where((ylo == 1) & (k % 2 == 0), 2 - k, k))
    on_top = one_hot(256, 8, (by_row(8) // 8) % 4)
    on_s = one_hot(256, 8, by_row(8) % 8)
    turn = lambda hot, m, to: spread(hot, m.T, to)
    a = [turn(from_k, m, on_k) for m in high]
    b = times([turn(on_top, m, on_top) for m in high], [turn(on_s, m, on_s) for m in low])
    value = times(a, (b[0], -b[1]))
    same, lower = i // 128 == j // 128, i > j
    store_halves(right1, jnp.where(same, value[0], jnp.where(lower, -value[1], value[1])))


def prepare_rows(z, factors, small, right2, left, late_ref):
    i, j = iota2(256, 256, 0), iota2(256, 256, 1)
    low = of(factors, 0)
    out_g = one_hot(256, 16, by_row(16) // 16)
    in_g = one_hot(256, 16, (by_row(16) // 16 + 2 * z) % 16)
    u = [spread(out_g, small[part], in_g) for part in range(2)]
    same, lower = (i // 8) % 2 == (j // 8) % 2, (i // 8) % 2 > (j // 8) % 2
    value = jnp.where(same, u[0], jnp.where(lower, -u[1], u[1]))
    store_halves(right2, jnp.where(i % 8 == j % 8, value, 0.0))
    on_s = one_hot(256, 8, by_row(8) % 8)
    low = [spread(on_s, m, on_s) for m in low]
    real = lambda value: KEEP * jnp.where(same, value[0], jnp.where(lower, value[1], -value[1]))
    store_halves(left, real(times(u, low)))
    n = (by_row(16) // 16) % 4
    in_g = one_hot(256, 16, (n + jnp.where(n < 2, 2, 12) + 2 * z) % 16)
    u = [spread(out_g, small[part], in_g) for part in range(2)]
    hi, lo = (v.astype(jnp.float32) for v in halves(real(times(u, low))))
    segment = j // 64
    late_ref[...] = jnp.where(segment == 3, 0.0, jnp.where(segment == 1, lo, hi)).astype(jnp.bfloat16)


def on_lanes(f_ref, right1, g, n, g2, n2):
    here = (pl.ds(g, n), pl.ds(g2, n2))
    v = jnp.concatenate([f_ref[(*here, part)].reshape(n * n2 * 8, 128) for part in range(2)], axis=1)
    v = dot3(halves(v), (right1[0], right1[1]))
    for part in range(2):
        f_ref[(*here, part)] = v[:, 128 * part : 128 * part + 128].reshape(n, n2, 8, 128)


def rotate_kernel(early_ref, late_ref, matrix_ref, sums_ref, re_ref, im_ref, purity_ref, purity, stage, product, sem, purity_sem):
    r, c = lax.axis_index("row"), lax.axis_index("col")
    sums = sums_ref[...]
    lane = lanes((1, 128))
    total, trace_re, trace_im = (jnp.sum(jnp.where(lane == n, sums, 0.0)) for n in range(3))
    dim = GATE * GATE * LOW
    shifts = (jnp.where(r == c, MIX * trace_re / dim, 0.0), jnp.where(r == c, MIX * trace_im / dim, 0.0))
    squared = trace_re * trace_re + trace_im * trace_im
    purity[0, 0] = (KEEP * KEEP * total + (2 * KEEP * MIX + MIX * MIX) * squared / dim) / (dim * dim)
    matrix = matrix_ref[...]
    sublane = lax.broadcasted_iota(jnp.int32, (8, 128), 0)
    v = jnp.concatenate([late_ref[:, n].reshape(64, 128) for n in range(16)], axis=1)
    hi, lo = halves(v)
    product[...] = dot(matrix, jnp.concatenate([hi, hi, lo, jnp.zeros_like(hi)], axis=0))
    copies = [pltpu.make_async_copy(purity, purity_ref, purity_sem)]
    copies[0].start()
    for q in range(4):
        for g in range(16):
            for part in range(2):
                for k in range(4):
                    row, col = 16 * g + 8 * part, 128 * k
                    tile = early_ref[q, row : row + 8, col : col + 128]
                    tile = tile + product[row : row + 8, 512 * q + col : 512 * q + col + 128]
                    if g // 4 == q:
                        tile = tile + jnp.where(lanes() == sublane + (32 * (g % 4) + 8 * k), shifts[part], 0.0)
                    stage[part, q, 32 * g + 8 * k : 32 * g + 8 * k + 8] = tile
        for part, ref in ((0, re_ref), (1, im_ref)):
            copies.append(pltpu.make_async_copy(stage.at[part, q], ref.at[:, pl.ds(128 * q, 128)], sem.at[part, q]))
            copies[-1].start()
    for copy in copies:
        copy.wait()


def rotate_call(*args):
    f32 = jnp.float32
    vmem, hbm = pl.BlockSpec(memory_space=pltpu.VMEM), pl.BlockSpec(memory_space=pltpu.HBM)
    return pl.pallas_call(
        rotate_kernel,
        name="rotate",
        out_shape=(
            jax.ShapeDtypeStruct((512, 512), f32),
            jax.ShapeDtypeStruct((512, 512), f32),
            jax.ShapeDtypeStruct((1, 1), f32),
        ),
        in_specs=[vmem] * 4,
        out_specs=(hbm, hbm, hbm),
        scratch_shapes=[
            pltpu.SMEM((1, 1), f32),
            pltpu.VMEM((2, 4, 512, 128), f32),
            pltpu.VMEM((256, 2048), f32),
            pltpu.SemaphoreType.DMA((2, 4)),
            pltpu.SemaphoreType.DMA,
        ],
        compiler_params=pltpu.CompilerParams(vmem_limit_bytes=20 * 2**20),
    )(*args)


def on_device(rho_real, rho_imag, gate_real_matrix, gate_imaginary, angles, targets, gate_order):
    args = (rho_real, rho_imag, gate_real_matrix, gate_imaginary, angles.T, targets, gate_order)
    found = exchange_call(*(pltpu.with_memory_space_constraint(v, pltpu.HBM) for v in args))
    re, im, purity = rotate_call(*found)
    return re, im, purity.reshape(())


def solution(mesh):
    return jax.shard_map(
        on_device,
        mesh=mesh,
        in_specs=(P("row", "col"), P("row", "col"), P(), P(), P(), P(), P()),
        out_specs=(P("row", "col"), P("row", "col"), P()),
        check_vma=False,
    )
```
